32 devices in a mesh: gx: 8 (over y, x, core), gy: 4 (over z).
Axes of the slice: x: 2, y: 2, z: 4, core: 2. Of those that a mesh axis runs over, the one named last changes fastest.
Arguments:
- u_old: float32 [3, 256, 128, 256], P(None, 'gx', 'gy'), may hold values from -0.6 to 0.6
- density: float32 [256, 128, 256], P('gx', 'gy'), may hold values from 0.5 to 2
- offsets: float32 [3, 512, 128], P(None, ('gx', 'gy')), may hold values from 0 to 1
- forces: float32 [3, 512, 128], P(None, ('gx', 'gy')), may hold values from -60 to 60
- base_x: int32 [512, 128], P(('gx', 'gy')), may hold values from 0 to 31
- base_y: int32 [512, 128], P(('gx', 'gy')), may hold values from 0 to 31
- base_z: int32 [512, 128], P(('gx', 'gy')), may hold values from 0 to 255
- tile_count: int32 [32], P(('gx', 'gy')), may hold values from 1 to 16, as said below
Outputs:
- u_new: float32 [3, 256, 128, 256], P(None, 'gx', 'gy')
- marker_velocity: float32 [3, 512, 128], P(None, ('gx', 'gy'))
The draws below stay inside these ranges and needn't reach their ends.
Inputs may be any that keep to these rules, and one draw needn't show every extreme that they name: `tile_count`: every draw has a device with exactly 16 live tiles; loads are skewed, with a mean near a quarter of that.
All inputs are finite; a program needn't handle non-finite values.
Results may differ from the reference program's by a relative error of at most 0.000075.
Values sent between devices are 32-bit elements; how exact they have to be, the bound alone decides.
A program may use at most 64 MiB of HBM per device.

```python
import math
import jax
import jax.numpy as jnp

CX = 32
CY = 32
NZ = 256
TILE = 128
MAXT = 16
NX = 256
NY = 128
TILES = 512
N_GY = 4
DEVICES = 32


def draw_tile_count(key, part):
    first, second, third = jax.random.split(jax.random.fold_in(key, 17), 3)
    upper = jax.random.randint(first, (DEVICES,), 0, MAXT)
    lower = jax.random.randint(second, (DEVICES,), 0, MAXT)
    counts = 1 + upper * lower // MAXT
    busiest = jax.random.randint(third, (), 0, DEVICES)
    return jnp.where(jnp.arange(DEVICES) == busiest, MAXT, counts).astype(jnp.int32)


def plant(drawn, key, least, top_value):
    index_at = [jax.random.randint(jax.random.fold_in(key, axis), (), 0, length) for axis, length in enumerate(drawn.shape)]
    widest = drawn.shape.index(max(drawn.shape))
    next_to = index_at[:widest] + [(index_at[widest] + 1) % drawn.shape[widest]] + index_at[widest + 1:]
    return drawn.at[tuple(index_at)].set(least).at[tuple(next_to)].set(top_value)


def block_levels(stream_key, dims, shards, least, largest):
    level, own = 1.0, jax.random.fold_in(stream_key, 6)
    for dim, shards_of in shards:
        steps = jnp.exp(jax.random.uniform(jax.random.fold_in(own, dim), (shards_of,), jnp.float32, least / len(shards), largest / len(shards)))
        level = level * jnp.repeat(steps, dims[dim] // shards_of).reshape([-1 if axis == dim else 1 for axis in range(len(dims))])
    return level


def noise(own_key, dims, scale, most, cuts=(), kind=jnp.bfloat16):
    drawn = jax.random.normal(own_key, dims, jnp.float32) * scale
    if len(cuts) > 0:
        drawn = block_levels(own_key, dims, cuts, -0.22, 0.18) * drawn
    return jnp.clip(drawn, min=-most, max=most).astype(kind)


def setup_inputs(seed: int = 0) -> dict:
    key_list = jax.random.split(jax.random.key(seed), 9)
    return {
        "u_old": noise(key_list[0], (3, NX, NY, NZ), 0.1, 0.6, ((1, 8), (2, 4)), jnp.float32),
        "density": jnp.clip(jnp.exp(math.log(2.0) - 1.3862944 * jax.random.uniform(key_list[1], (NX, NY, NZ), jnp.float32) ** block_levels(key_list[1], (NX, NY, NZ), ((0, 8), (1, 4)), -0.2, 0.2)), 0.5, 2.0),
        "offsets": jnp.clip(1.0 * jax.random.uniform(key_list[2], (3, TILES, TILE), jnp.float32) ** block_levels(key_list[2], (3, TILES, TILE), ((1, 32),), -0.2, 0.2), 0.0, 1.0),
        "forces": noise(key_list[3], (3, TILES, TILE), 10.0, 60.0, ((1, 32),), jnp.float32),
        "base_x": plant(jax.random.randint(key_list[4], (TILES, TILE), 0, CX), jax.random.fold_in(key_list[4], 1), 0, CX - 1).astype(jnp.int32),
        "base_y": plant(jax.random.randint(key_list[5], (TILES, TILE), 0, CY), jax.random.fold_in(key_list[5], 1), 0, CY - 1).astype(jnp.int32),
        "base_z": plant(jax.random.randint(key_list[6], (TILES, TILE), 0, NZ), jax.random.fold_in(key_list[6], 1), 0, NZ - 1).astype(jnp.int32),
        "tile_count": draw_tile_count(jax.random.fold_in(key_list[8], 71), 0),
    }


def stencil(frac):
    root = jnp.sqrt(1.0 + 4.0 * frac - 4.0 * frac * frac)
    return [(3.0 - 2.0 * frac - root) / 8.0, (3.0 - 2.0 * frac + root) / 8.0, (1.0 + 2.0 * frac + root) / 8.0, (1.0 + 2.0 * frac - root) / 8.0]

def reference(u_old, density, offsets, forces, base_x, base_y, base_z, tile_count):
    time_step = 0.5
    tiles, width = base_x.shape
    nx, ny, nz = density.shape
    slot = jnp.arange(tiles).astype(jnp.int32)
    device = slot // MAXT
    anchor_x = (device // N_GY * CX)[:, None]
    anchor_y = (device % N_GY * CY)[:, None]
    live = (slot % MAXT < tile_count[device]).astype(jnp.float32)[:, None] * jnp.ones((tiles, width), jnp.float32)
    weight_x = stencil(offsets[0])
    weight_y = stencil(offsets[1])
    weight_z = stencil(offsets[2])
    load = forces * live[None]
    grid = jnp.zeros((3, nx * ny * nz), jnp.float32)
    places = []
    for shift_a in range(4):
        cell_x = (anchor_x + base_x + shift_a - 1) % nx
        for shift_b in range(4):
            cell_y = (anchor_y + base_y + shift_b - 1) % ny
            for shift_c in range(4):
                cell_z = (base_z + shift_c - 1) % nz
                index = ((cell_x * ny + cell_y) * nz + cell_z).astype(jnp.int32)
                weight = weight_x[shift_a] * weight_y[shift_b] * weight_z[shift_c]
                grid = grid.at[:, index.reshape(-1)].add((load * weight[None]).reshape(3, -1))
                places.append((index, weight))
    force_grid = grid.reshape(3, nx, ny, nz)
    u_new = u_old + time_step * force_grid / density[None]
    table = u_new.reshape(3, -1)
    velocity = jnp.zeros((3, tiles, width), jnp.float32)
    for index, weight in places:
        velocity = velocity + table[:, index.reshape(-1)].reshape(3, tiles, width) * weight[None]
    return (u_new, velocity * live[None])
```

```python
import functools

import jax
import jax.numpy as jnp
from jax import lax
from jax.experimental import pallas as pl
from jax.experimental.pallas import tpu as pltpu
from jax.sharding import PartitionSpec as P

VMEM_LIMIT = 60 * 1024 * 1024


def divisor(count, most):
    return max(d for d in range(1, most + 1) if count % d == 0)


def moved(value, step_x, step_y):
    if step_y == 0:
        n = lax.axis_size("gx")
        return lax.ppermute(value, "gx", [(i, (i + step_x) % n) for i in range(n)])
    if step_x == 0:
        n = lax.axis_size("gy")
        return lax.ppermute(value, "gy", [(i, (i + step_y) % n) for i in range(n)])
    nx, ny = lax.axis_size("gx"), lax.axis_size("gy")
    pairs = [
        (i * ny + j, ((i + step_x) % nx) * ny + (j + step_y) % ny)
        for i in range(nx)
        for j in range(ny)
    ]
    return lax.ppermute(value, ("gx", "gy"), pairs)


def stencil(frac):
    root = jnp.sqrt(1.0 + 4.0 * frac - 4.0 * frac * frac)
    return [
        (3.0 - 2.0 * frac - root) / 8.0,
        (3.0 - 2.0 * frac + root) / 8.0,
        (1.0 + 2.0 * frac + root) / 8.0,
        (1.0 + 2.0 * frac - root) / 8.0,
    ]


def pick(delta, four):
    total = jnp.where(delta == 0, four[0], 0.0)
    for k in range(1, 4):
        total = jnp.where(delta == k, four[k], total)
    return total


def wrapped(delta, length):
    delta = jnp.where(delta < 0, delta + length, delta)
    return jnp.where(delta >= length, delta - length, delta)


def edge_weights(frac, base, rows, size):
    row = lax.broadcasted_iota(jnp.int32, (rows, base.shape[1]), 0)
    cell = jnp.where(row == size + 2, -1, row)
    cell = jnp.where(row > size + 2, -8, cell)
    return pick(cell - base + 1, stencil(frac))


def halves(value):
    high = value.astype(jnp.bfloat16)
    low = (value - high.astype(jnp.float32)).astype(jnp.bfloat16)
    return high, low


def edges(size):
    return (size - 1, size, size + 1), (size + 2, 0, 1)


def spread_kernel(size_x, size_y, feat, base, grid, *refs):
    slabs, (wx_s, wy_s, high_s, low_s) = refs[:8], refs[8:]
    planes, rows, depth = grid.shape[1], grid.shape[2], grid.shape[3]
    markers = feat.shape[1]
    wx_s[...] = edge_weights(feat[0:1, :], base[0:1, :], wx_s.shape[0], size_x)
    wy_s[...] = edge_weights(feat[1:2, :], base[1:2, :], rows, size_y)
    four = stencil(feat[2:3, :])
    column = jnp.concatenate(
        four + [base[2:3, :].astype(jnp.float32)] + [feat[3 + c : 4 + c, :] for c in range(3)], axis=0
    ).T
    cut = 256 if markers % 256 == 0 else 128
    for start in range(0, markers, cut):
        part = column[start : start + cut]
        lane = lax.broadcasted_iota(jnp.int32, (cut, depth), 1)
        delta = wrapped(lane - part[:, 4:5].astype(jnp.int32) + 1, depth)
        wz = pick(delta, [part[:, k : k + 1] for k in range(4)])
        for c in range(3):
            high, low = halves(wz * part[:, 5 + c : 6 + c])
            high_s[start : start + cut, c * depth : (c + 1) * depth] = high
            low_s[start : start + cut, c * depth : (c + 1) * depth] = low
    group = divisor(planes, 8)

    def turn(g, carry):
        first = g * group
        left = jnp.concatenate(
            [wy_s[...] * wx_s[pl.ds(first + j, 1), :] for j in range(group)], axis=0
        )
        high, low = halves(left)
        dot = functools.partial(jnp.dot, preferred_element_type=jnp.float32)
        total = dot(high, high_s[...]) + dot(low, high_s[...]) + dot(high, low_s[...])
        for j in range(group):
            for c in range(3):
                grid[c, first + j] = total[j * rows : (j + 1) * rows, c * depth : (c + 1) * depth]
        return carry

    lax.fori_loop(0, planes // group, turn, 0)
    sides_x, sides_y = edges(size_x), edges(size_y)
    for side in range(2):
        for c in range(3):
            for j, p in enumerate(sides_x[side]):
                slabs[side][c, j] = grid[c, p]
                for other in range(2):
                    for i, r in enumerate(sides_y[other]):
                        slabs[4 + 2 * side + other][c, j, i : i + 1] = grid[c, p, r : r + 1]
            for i, r in enumerate(sides_y[side]):
                for p in range(planes):
                    slabs[2 + side][c, i, p : p + 1] = grid[c, p, r : r + 1]


def read_kernel(size_x, size_y, time_step, *refs):
    feat, base, grid, u_old, density, low_x, high_x, low_y, high_y = refs[:9]
    slabs, (u_new, velocity) = refs[9:17], refs[17:19]
    total, wx_s, wy_s, wz3, table = refs[19:]
    planes, rows, depth = grid.shape[1], grid.shape[2], grid.shape[3]
    markers = feat.shape[1]
    wx_s[...] = edge_weights(feat[0:1, :], base[0:1, :], wx_s.shape[0], size_x)
    wy_s[...] = edge_weights(feat[1:2, :], base[1:2, :], rows, size_y)
    cut = 256 if markers % 256 == 0 else 128
    for start in range(0, markers, cut):
        at = slice(start, start + cut)
        row = lax.broadcasted_iota(jnp.int32, (depth, cut), 0)
        delta = wrapped(row - base[2:3, at] + 1, depth)
        high, low = halves(pick(delta, stencil(feat[2:3, at])))
        wz3[0:depth, at] = high
        wz3[depth : 2 * depth, at] = high
        wz3[2 * depth :, at] = low
    total[...] = grid[...]
    near_x, near_y = edges(size_x)[::-1], edges(size_y)[::-1]
    for side in range(2):
        for c in range(3):
            for j, p in enumerate(near_x[side]):
                total[c, p] = total[c, p] + slabs[side][c, j]
                for other in range(2):
                    for i, r in enumerate(near_y[other]):
                        total[c, p, r : r + 1] = (
                            total[c, p, r : r + 1] + slabs[4 + 2 * side + other][c, j, i : i + 1]
                        )
            for i, r in enumerate(near_y[side]):
                for p in range(planes):
                    total[c, p, r : r + 1] = total[c, p, r : r + 1] + slabs[2 + side][c, i, p : p + 1]
    group = divisor(planes, 6)
    spare = jnp.ones((rows - size_y - 3, depth), jnp.float32)

    def plane_state(k, p):
        if p < size_x:
            main = density[p] if k == 3 else u_old[k, p]
        elif p < size_x + 2:
            main = high_x[k, p - size_x]
        else:
            main = low_x[k, 0]
        edge = [high_y[k, 0, p : p + 1], high_y[k, 1, p : p + 1], low_y[k, 0, p : p + 1], spare]
        return jnp.concatenate([main] + edge, axis=0)

    for g in range(planes // group):
        pieces = []
        for p in range(g * group, (g + 1) * group):
            scale = time_step / plane_state(3, p)
            for c in range(3):
                value = plane_state(c, p) + total[c, p] * scale
                if p < size_x:
                    u_new[c, p] = value[:size_y]
                pieces.append(value)
        high, low = halves(jnp.concatenate(pieces, axis=0))
        table[g, :, 0:depth] = high
        table[g, :, depth : 2 * depth] = low
        table[g, :, 2 * depth :] = high

    def turn(step, carry):
        at = pl.ds(pl.multiple_of(step * cut, cut), cut)
        right = wz3[:, at]
        wy = wy_s[:, at]
        sums = [jnp.zeros((8, cut), jnp.float32) for _ in range(3)]
        for g in range(planes // group):
            found = jnp.dot(table[g], right, preferred_element_type=jnp.float32)
            for j in range(group):
                p = g * group + j
                weight = wy * wx_s[p : p + 1, at]
                for c in range(3):
                    first = (j * 3 + c) * rows
                    product = found[first : first + rows] * weight
                    for r in range(0, rows, 8):
                        sums[c] = sums[c] + product[r : r + 8]
        velocity[:, at] = (
            jnp.concatenate([jnp.sum(s, axis=0, keepdims=True) for s in sums], axis=0) * feat[6:7, at]
        )
        return carry

    lax.fori_loop(0, markers // cut, turn, 0)


def dense_device(u_old, density, offsets, forces, base_x, base_y, base_z, tile_count):
    time_step = 0.5
    _, size_x, size_y, depth = u_old.shape
    slots, width = base_x.shape
    markers = slots * width
    planes = size_x + 3
    rows = -(-(size_y + 3) // 8) * 8
    lines = -(-planes // 8) * 8
    f32, bf16 = jnp.float32, jnp.bfloat16
    live = (lax.broadcasted_iota(jnp.int32, (slots, width), 0) < tile_count[0]).astype(f32)
    feat = jnp.concatenate([offsets, forces * live[None], live[None]], axis=0).reshape(7, markers)
    base = jnp.stack([base_x, base_y, base_z], axis=0).reshape(3, markers)

    up = jnp.concatenate([u_old[:, size_x - 1 :], density[None, size_x - 1 :]], axis=0)
    down = jnp.concatenate([u_old[:, :2], density[None, :2]], axis=0)
    low_x, high_x = moved(up, 1, 0), moved(down, -1, 0)

    def strip(r):
        inner = jnp.concatenate([u_old[:, :, r], density[None, :, r]], axis=0)
        return jnp.concatenate([inner, high_x[:, :, r], low_x[:, :, r]], axis=1)

    low_y = moved(strip(size_y - 1)[:, None], 0, 1)
    high_y = moved(jnp.stack([strip(0), strip(1)], axis=1), 0, -1)

    params = pltpu.CompilerParams(vmem_limit_bytes=VMEM_LIMIT)
    slab_x = jax.ShapeDtypeStruct((3, 3, rows, depth), f32)
    slab_y = jax.ShapeDtypeStruct((3, 3, planes, depth), f32)
    corner = jax.ShapeDtypeStruct((3, 3, 3, depth), f32)
    whole = pl.BlockSpec(memory_space=pltpu.VMEM)
    flops = 6 * planes * rows * 3 * depth * markers
    cost = pl.CostEstimate(flops=flops, transcendentals=0, bytes_accessed=8 * planes * rows * depth)
    grid, *slabs = pl.pallas_call(
        functools.partial(spread_kernel, size_x, size_y),
        out_shape=[jax.ShapeDtypeStruct((3, planes, rows, depth), f32)]
        + [slab_x] * 2
        + [slab_y] * 2
        + [corner] * 4,
        in_specs=[whole] * 2,
        out_specs=[whole] * 9,
        scratch_shapes=[
            pltpu.VMEM((lines, markers), f32),
            pltpu.VMEM((rows, markers), f32),
            pltpu.VMEM((markers, 3 * depth), bf16),
            pltpu.VMEM((markers, 3 * depth), bf16),
        ],
        compiler_params=params,
        cost_estimate=cost,
        name="spread",
    )(feat, base)
    ways = [(1, 0), (-1, 0), (0, 1), (0, -1), (1, 1), (1, -1), (-1, 1), (-1, -1)]
    slabs = [moved(slab, *way) for slab, way in zip(slabs, ways)]
    group = divisor(planes, 6)
    u_new, velocity = pl.pallas_call(
        functools.partial(read_kernel, size_x, size_y, time_step),
        out_shape=[
            jax.ShapeDtypeStruct(u_old.shape, f32),
            jax.ShapeDtypeStruct((3, markers), f32),
        ],
        in_specs=[whole] * 17,
        out_specs=[whole] * 2,
        scratch_shapes=[
            pltpu.VMEM((3, planes, rows, depth), f32),
            pltpu.VMEM((lines, markers), f32),
            pltpu.VMEM((rows, markers), f32),
            pltpu.VMEM((3 * depth, markers), bf16),
            pltpu.VMEM((planes // group, group * 3 * rows, 3 * depth), bf16),
        ],
        compiler_params=params,
        cost_estimate=cost,
        name="read",
    )(feat, base, grid, u_old, density, low_x, high_x, low_y, high_y, *slabs)
    return (u_new, velocity.reshape(3, slots, width))


MESH = pl.DeviceIdType.MESH
WAYS = [(1, 0), (-1, 0), (0, 1), (0, -1), (1, 1), (1, -1), (-1, 1), (-1, -1)]
BATCH = 8


def thirds(value):
    high = value.astype(jnp.bfloat16).astype(jnp.float32)
    rest = value - high
    middle = rest.astype(jnp.bfloat16).astype(jnp.float32)
    return [high, middle, rest - middle]


class Plan:
    def __init__(self, size_x, size_y, depth, slots, width):
        self.size_x, self.size_y, self.depth = size_x, size_y, depth
        self.slots, self.width = slots, width
        self.markers = slots * width

        def cap(reach, size):
            return -(-2 * reach * self.markers // size // width) * width

        corner = width // 4
        self.caps = [cap(2, size_x), cap(1, size_x), cap(2, size_y), cap(1, size_y)] + [corner] * 4
        self.starts = [sum(self.caps[:d]) for d in range(8)]
        self.listed = sum(self.caps)
        self.faces = self.starts[4]
        self.tiles = slots + self.listed // width
        self.total = self.tiles * width
        self.tile_rows = -(-self.tiles // 8) * 8
        self.outers = (size_x + 2) // 2 + 2
        self.outer_rows = 2 * (depth + 4)
        self.grid_rows = self.outers * self.outer_rows

    def span(self, d):
        if d < 4:
            return self.starts[d], self.caps[d]
        return self.faces, self.width


def row_mask(shape, value):
    return lax.broadcasted_iota(jnp.int32, shape, 0) == value


def prepare(plan, data, first, count, weights, own, plain, places):
    width, size_y = plan.width, plan.size_y
    f32, bf16 = jnp.float32, jnp.bfloat16
    k_row = lax.broadcasted_iota(jnp.int32, (32, 6 * width), 0)
    n_lane = lax.broadcasted_iota(jnp.int32, (32, 6 * width), 1)
    kind = k_row % 8
    part, inside = n_lane // width, n_lane % width
    hit = ((kind < 5) & (part == kind)) | ((kind > 4) & (part == 5) & (inside // size_y == kind - 5))
    select = jnp.where(hit & (k_row < 24), 1.0, 0.0).astype(bf16)
    step = 4
    for t0 in range(0, count, step):
        n = min(step, count - t0) * width
        d = data[:, t0 * width : t0 * width + n]
        at = slice((first + t0) * width, (first + t0) * width + n)
        rows = lax.broadcasted_iota(jnp.int32, (8, n), 0)
        w = stencil(jnp.where(rows < 3, d[0:8], 0.5))
        z = [jnp.broadcast_to(v[2:3], (8, n)) for v in w]
        x = [jnp.broadcast_to(v[0:1], (8, n)) for v in w]
        along = jnp.where(rows < 2, z[0], jnp.where(rows < 4, z[1], jnp.where(rows < 6, z[2], z[3])))
        even = rows % 2 == 0
        weights[0:8, at] = along * jnp.where(even, x[0], x[1])
        weights[8:16, at] = along * jnp.where(even, x[2], x[3])
        block = jnp.concatenate([v[1:2] for v in w] + [d[7:8], d[3:6]], axis=0)
        stack = jnp.concatenate(thirds(block) + [jnp.zeros((8, n), f32)], axis=0).astype(bf16)
        wide = lax.dot_general(
            stack, select, (((0,), (0,)), ((), ())), preferred_element_type=f32
        )
        cols = [wide[:, i * width : (i + 1) * width] for i in range(6)]
        lane = lax.broadcasted_iota(jnp.int32, (n, width), 1)
        y = jnp.where(lane < 3 * size_y, lane % size_y, -1000).astype(f32)
        pattern = pick(y - cols[4] + 1.0, cols[:4])
        plain[at, :] = pattern
        own[at, :] = pattern * cols[5]
    keys, zs, bases = [], [], []
    for t in range(count):
        at = slice(t * width, (t + 1) * width)
        bx = data[6:7, at].astype(jnp.int32)
        bz = data[8:9, at].astype(jnp.int32)
        good = data[9:10, at] > 0.0
        lane = lax.broadcasted_iota(jnp.int32, (1, width), 1)
        step_in = lane % BATCH
        across = bx + 2
        side, outer = across % 2, across // 2
        spare = plan.grid_rows + ((plan.size_x + 2) // 2) * plan.outer_rows + 8 * step_in
        base = side * plan.grid_rows + outer * plan.outer_rows + 2 * bz
        bases.append(jnp.where(good, base, spare))
        keys.append(jnp.where(good, side * (plan.outers + 8) + outer, -100 - 10 * step_in))
        zs.append(bz)
    rows = -(-count // 8) * 8
    fill = [jnp.zeros((rows - count, width), jnp.int32)] if rows > count else []
    key, z = jnp.concatenate(keys + fill, axis=0), jnp.concatenate(zs + fill, axis=0)
    base = jnp.concatenate(bases + fill, axis=0)
    lane = lax.broadcasted_iota(jnp.int32, (rows, width), 1) % BATCH

    def near(a, b, most):
        return (a - b <= most) & (b - a <= most)

    clashes = [
        (lane >= d) & near(key, pltpu.roll(key, d, 1), 1) & near(z, pltpu.roll(z, d, 1), 3)
        for d in range(1, BATCH)
    ]
    second = clashes[0]
    for clash in clashes[1:]:
        second = second | clash
    second = jnp.where(second, 1, 0)
    bad = jnp.zeros((rows, width), jnp.int32)
    for d, clash in enumerate(clashes):
        both = second * pltpu.roll(second, d + 1, 1)
        bad = jnp.maximum(bad, jnp.where(clash, both, 0))
    places[first : first + rows, :] = base + second * (2 * plan.grid_rows)
    bad = jnp.max(bad, axis=1, keepdims=True)
    goods = [jnp.max(data[9:10, t * width : (t + 1) * width], axis=1, keepdims=True) for t in range(count)]
    goods = goods + [jnp.zeros((rows - count, 1), jnp.float32)] * (1 if rows > count else 0)
    good = jnp.concatenate(goods, axis=0)
    state = jnp.where(good > 0.0, 1 + bad, 0)
    below = plan.tile_rows + first
    places[below : below + rows, :] = jnp.broadcast_to(state, (rows, width))


def place():
    nx, ny = lax.axis_size("gx"), lax.axis_size("gy")
    return nx, ny, lax.axis_index("gx"), lax.axis_index("gy")


def send_kernel(plan, *refs):
    (offsets, forces, base_x, base_y, base_z, tile_count) = refs[:6]
    (own, plain, weights, places, slot_map, any_over) = refs[6:12]
    data, one_hot, lists, inbox, corners, got, note, notes = refs[12:20]
    send_sem, recv_sem, note_send, note_recv = refs[20:]
    f32, bf16 = jnp.float32, jnp.bfloat16
    slots, width, markers = plan.slots, plan.width, plan.markers
    nx, ny, mx, my = place()
    devices = nx * ny
    me = mx * ny + my

    def other(i):
        to = lax.rem(me + i, devices)
        return to // ny, lax.rem(to, ny)

    barrier = pltpu.get_barrier_semaphore()

    def greet(i, carry):
        pl.semaphore_signal(barrier, inc=1, device_id=other(i), device_id_type=MESH)
        return carry

    lax.fori_loop(1, devices, greet, 0)

    live = jnp.where(lax.broadcasted_iota(jnp.int32, (slots, width), 0) < tile_count[0], 1.0, 0.0)
    bx, by, bz = base_x[...], base_y[...], base_z[...]
    values = [offsets[c] for c in range(3)] + [forces[c] * live for c in range(3)]
    values = values + [bx.astype(f32), by.astype(f32), bz.astype(f32), live]
    data[10:16, :] = jnp.zeros((6, markers), f32)
    for k, value in enumerate(values):
        for t in range(slots):
            data[k : k + 1, t * width : (t + 1) * width] = value[t : t + 1, :]
    ahead_x = jnp.where(bx >= plan.size_x - 2, live, 0.0)
    back_x = jnp.where(bx < 1, live, 0.0)
    ahead_y = jnp.where(by >= plan.size_y - 2, 1.0, 0.0)
    back_y = jnp.where(by < 1, 1.0, 0.0)
    flags = []
    for step_x, step_y in WAYS:
        flag = {1: ahead_x, -1: back_x, 0: live}[step_x]
        flags.append(flag if step_y == 0 else flag * (ahead_y if step_y > 0 else back_y))
    flag = jnp.concatenate(flags, axis=0)
    lines = 8 * slots
    r, c = (lax.broadcasted_iota(jnp.int32, (width, width), a) for a in range(2))
    upper = jnp.where(r <= c, 1.0, 0.0).astype(bf16)
    r, c = (lax.broadcasted_iota(jnp.int32, (lines, lines), a) for a in range(2))
    before = jnp.where((c < r) & (c // slots == r // slots), 1.0, 0.0).astype(bf16)
    within = jnp.dot(flag.astype(bf16), upper, preferred_element_type=f32)
    count = jnp.broadcast_to(jnp.sum(flag, axis=1, keepdims=True), (lines, width))
    earlier = jnp.dot(before, count.astype(bf16), preferred_element_type=f32)
    slot = jnp.where(flag > 0.0, earlier + within - 1.0, -1.0)
    slot_map[...] = slot
    over = jnp.zeros((slots, width), f32)
    for d in range(8):
        here = slot[d * slots : (d + 1) * slots]
        over = jnp.maximum(over, jnp.where(here >= plan.caps[d], 1.0, 0.0))
    note[...] = jnp.broadcast_to(jnp.max(over), note.shape)
    fill_one_hot(plan, slot_map, one_hot)
    stack = jnp.concatenate(thirds(data[...]), axis=0).astype(bf16)
    found = lax.dot_general(
        stack, one_hot[...], (((1,), (1,)), ((), ())), preferred_element_type=f32
    )
    found = found[0:16] + found[16:32] + found[32:48]
    lane = lax.broadcasted_iota(jnp.int32, (1, plan.listed), 1)
    for row, axis, size in ((6, 0, plan.size_x), (7, 1, plan.size_y)):
        shift = jnp.zeros((1, plan.listed), f32)
        for d in range(8):
            inside = (lane >= plan.starts[d]) & (lane < plan.starts[d] + plan.caps[d])
            shift = jnp.where(inside, float(WAYS[d][axis] * size), shift)
        moved_by = jnp.where(row_mask((16, plan.listed), row), shift * found[9:10], 0.0)
        found = found - moved_by
    lists[...] = found

    pl.semaphore_wait(barrier, devices - 1)
    copies = []
    for d, (step_x, step_y) in enumerate(WAYS):
        start, size = plan.span(d)
        target = inbox.at[:, pl.ds(start, size)] if d < 4 else corners.at[d - 4]
        copies.append(
            pltpu.make_async_remote_copy(
                src_ref=lists.at[:, pl.ds(start, size)],
                dst_ref=target,
                send_sem=send_sem.at[d],
                recv_sem=recv_sem.at[d],
                device_id=(lax.rem(mx + step_x + nx, nx), lax.rem(my + step_y + ny, ny)),
                device_id_type=MESH,
            )
        )
        copies[-1].start()

    def word(i):
        return pltpu.make_async_remote_copy(
            src_ref=note,
            dst_ref=notes.at[i],
            send_sem=note_send.at[i],
            recv_sem=note_recv.at[i],
            device_id=other(i),
            device_id_type=MESH,
        )

    def tell(i, carry):
        word(i).start()
        return carry

    lax.fori_loop(1, devices, tell, 0)
    prepare(plan, data, 0, slots, weights, own, plain, places)
    for copy in copies:
        copy.wait()

    def hear(i, most):
        word(i).wait()
        return jnp.maximum(most, notes[i])

    any_over[...] = lax.fori_loop(1, devices, hear, note[...])
    got[:, 0 : plan.faces] = inbox[...]
    lane = lax.broadcasted_iota(jnp.int32, (16, width), 1) // plan.caps[4]
    last = corners[0]
    for i in range(1, 4):
        last = jnp.where(lane == i, corners[i], last)
    got[:, plan.faces :] = last
    prepare(plan, got, slots, plan.tiles - slots, weights, own, plain, places)


def fill_one_hot(plan, slot_map, one_hot):
    for d in range(8):
        rows = plan.caps[d]
        index = lax.broadcasted_iota(jnp.int32, (rows, plan.width), 0).astype(jnp.float32)
        for t in range(plan.slots):
            line = slot_map[d * plan.slots + t : d * plan.slots + t + 1, :]
            hot = jnp.where(index == line, 1.0, 0.0).astype(jnp.bfloat16)
            one_hot[plan.starts[d] : plan.starts[d] + rows, t * plan.width : (t + 1) * plan.width] = hot


def main_kernel(plan, time_step, *refs):
    own, plain, weights, places, u_in, density_in, u_out, velocity = refs[:8]
    grid, table, found, u_s, density_s, sems = refs[8:]
    f32 = jnp.float32
    width, depth, size_y = plan.width, plan.depth, plan.size_y
    outer_rows, grid_rows = plan.outer_rows, plan.grid_rows
    loads = [
        pltpu.make_async_copy(u_in, u_s, sems.at[0]),
        pltpu.make_async_copy(density_in, density_s, sems.at[1]),
    ]
    for load in loads:
        load.start()
    zero = jnp.zeros((8, width), f32)
    group = divisor(4 * grid_rows // 8, 52)

    def clear(i, carry):
        for j in range(group):
            grid[pl.ds(pl.multiple_of((i * group + j) * 8, 8), 8), :] = zero
        return carry

    lax.fori_loop(0, 4 * grid_rows // 8 // group, clear, 0)
    for o in (0, 1, plan.outers - 2, plan.outers - 1):
        for g in range(2):
            at = g * grid_rows + o * outer_rows
            table[at : at + outer_rows, :] = jnp.zeros((outer_rows, width), f32)
    found[plan.markers :, :] = jnp.zeros((plan.listed, width), f32)

    def column(value, j):
        return jnp.broadcast_to(value[:, j : j + 1], (8, width))

    def spread_tile(t, carry):
        at = pl.ds(pl.multiple_of(t * width, width), width)
        first = t * width
        state = places[plan.tile_rows * width + first]

        @pl.when(state == 1)
        def _():
            w0, w1 = weights[0:8, at], weights[8:16, at]
            for j0 in range(0, width, BATCH):
                stores = []
                for j in range(j0, j0 + BATCH):
                    m = first + j
                    here = places[m]
                    row = jnp.broadcast_to(own[pl.ds(m, 1), :], (8, width))
                    one, two = pl.ds(here, 8), pl.ds(here + outer_rows, 8)
                    stores.append((one, grid[one, :] + column(w0, j) * row))
                    stores.append((two, grid[two, :] + column(w1, j) * row))
                for where, value in stores:
                    grid[where, :] = value

        @pl.when(state == 2)
        def _():
            w0, w1 = weights[0:8, at], weights[8:16, at]

            def single(j, c):
                m = first + j
                here = places[m]
                row = jnp.broadcast_to(own[pl.ds(m, 1), :], (8, width))
                turn = lax.rem(width - j, width)
                one, two = pl.ds(here, 8), pl.ds(here + outer_rows, 8)
                grid[one, :] = grid[one, :] + column(pltpu.roll(w0, turn, 1), 0) * row
                grid[two, :] = grid[two, :] + column(pltpu.roll(w1, turn, 1), 0) * row
                return c

            lax.fori_loop(0, width, single, 0)

        return carry

    lax.fori_loop(0, plan.tiles, spread_tile, 0)

    def fold(i, carry):
        at = i * outer_rows
        ends = [(2 * depth, 0, 2), (2, 2 * depth + 2, 4)]
        for to, source, rows in ends:
            grid[pl.ds(at + to, rows), :] = grid[pl.ds(at + to, rows), :] + grid[pl.ds(at + source, rows), :]
        return carry

    lax.fori_loop(0, 4 * plan.outers, fold, 0)
    for load in loads:
        load.wait()

    def lines(g, outer, side):
        return pl.ds(g * grid_rows + outer * outer_rows + 2 + side, depth, stride=2)

    def plane(p, spots):
        force = None
        for copy in range(2):
            for g, outer, side in spots:
                part = grid[lines(2 * copy + g, outer, side), :]
                force = part if force is None else force + part
        force = force.T
        scale = time_step / density_s[p]
        pieces = []
        for c in range(3):
            value = u_s[c, p] + force[c * size_y : (c + 1) * size_y] * scale
            u_s[c, p] = value
            pieces.append(value)
        if width > 3 * size_y:
            pieces.append(jnp.zeros((width - 3 * size_y, depth), f32))
        back = jnp.concatenate(pieces, axis=0).T
        for g, outer, side in spots:
            table[lines(g, outer, side), :] = back
            at = g * grid_rows + outer * outer_rows + side
            table[pl.ds(at, 1), :] = back[depth - 1 : depth]
            table[pl.ds(at + 2 * depth + 2, 1), :] = back[0:1]
            table[pl.ds(at + 2 * depth + 4, 1), :] = back[1:2]

    def pair(i, carry):
        plane(2 * i, [(0, i + 1, 1), (1, i + 1, 0)])
        plane(2 * i + 1, [(0, i + 2, 0), (1, i + 1, 1)])
        return carry

    lax.fori_loop(0, plan.size_x // 2, pair, 0)
    leave = pltpu.make_async_copy(u_s, u_out, sems.at[2])
    leave.start()
    sub = lax.broadcasted_iota(jnp.int32, (8, width), 0)

    def merge(a, b, h):
        low = sub % (2 * h) < h
        stay, go = jnp.where(low, a, b), jnp.where(low, b, a)
        if h == 4:
            return stay + pltpu.roll(go, 4, 0)
        return stay + jnp.where(low, pltpu.roll(go, 8 - h, 0), pltpu.roll(go, h, 0))

    def read_tile(t, carry):
        at = pl.ds(pl.multiple_of(t * width, width), width)
        first = t * width

        @pl.when(places[plan.tile_rows * width + first] > 0)
        def _():
            w0, w1 = weights[0:8, at], weights[8:16, at]
            for j0 in range(0, width, 8):
                sums = []
                for j in range(j0, j0 + 8):
                    here = places[first + j]
                    here = jnp.where(here >= 2 * grid_rows, here - 2 * grid_rows, here)
                    one, two = table[pl.ds(here, 8), :], table[pl.ds(here + outer_rows, 8), :]
                    sums.append(one * column(w0, j) + two * column(w1, j))
                for h in (4, 2, 1):
                    sums = [merge(sums[i], sums[i + h], h) for i in range(h)]
                block = pl.ds(pl.multiple_of(first + j0, 8), 8)
                found[block, :] = sums[0] * plain[block, :]

        return carry

    lax.fori_loop(0, plan.tiles, read_tile, 0)
    r = lax.broadcasted_iota(jnp.int32, (16, width), 0)
    lane = lax.broadcasted_iota(jnp.int32, (16, width), 1)
    by_part = jnp.where((lane // size_y == r) & (lane < 3 * size_y), 1.0, 0.0).astype(jnp.bfloat16)
    value = found[...]
    total = None
    for piece in thirds(value):
        part = lax.dot_general(
            by_part, piece.astype(jnp.bfloat16), (((1,), (1,)), ((), ())), preferred_element_type=f32
        )
        total = part if total is None else total + part
    velocity[...] = total[0:8]
    leave.wait()


def return_kernel(plan, *refs):
    velocity, slot_map, tile_count, out, one_hot, inbox, corners, send_sem, recv_sem = refs
    f32, bf16 = jnp.float32, jnp.bfloat16
    width = plan.width
    nx, ny, mx, my = place()
    barrier = pltpu.get_barrier_semaphore()

    def neighbour(step_x, step_y):
        return (lax.rem(mx + step_x + nx, nx), lax.rem(my + step_y + ny, ny))

    for way in WAYS:
        pl.semaphore_signal(barrier, inc=1, device_id=neighbour(*way), device_id_type=MESH)
    pl.semaphore_wait(barrier, len(WAYS))
    copies = []
    for d, (step_x, step_y) in enumerate(WAYS):
        start, size = plan.span(d)
        target = inbox.at[:, pl.ds(start, size)] if d < 4 else corners.at[d - 4]
        copies.append(
            pltpu.make_async_remote_copy(
                src_ref=velocity.at[:, pl.ds(plan.markers + start, size)],
                dst_ref=target,
                send_sem=send_sem.at[d],
                recv_sem=recv_sem.at[d],
                device_id=neighbour(-step_x, -step_y),
                device_id_type=MESH,
            )
        )
        copies[-1].start()
    fill_one_hot(plan, slot_map, one_hot)
    for copy in copies:
        copy.wait()
    lane = lax.broadcasted_iota(jnp.int32, (8, width), 1) // plan.caps[4]
    last = corners[0]
    for i in range(1, 4):
        last = jnp.where(lane == i, corners[i], last)
    back = jnp.concatenate([inbox[...], last], axis=1)
    stack = jnp.concatenate(thirds(back) + [jnp.zeros_like(back)], axis=0).astype(bf16)
    extra = jnp.dot(stack, one_hot[...], preferred_element_type=f32)
    extra = extra[0:8] + extra[8:16] + extra[16:24]
    total = velocity[:, 0 : plan.markers] + extra
    live = tile_count[0]
    for t in range(plan.slots):
        row = total[:, t * width : (t + 1) * width]
        row = jnp.where(lax.broadcasted_iota(jnp.int32, row.shape, 0) * 0 + t < live, row, 0.0)
        for c in range(3):
            out[c, t : t + 1, :] = row[c : c + 1, :]


def on_device(u_old, density, offsets, forces, base_x, base_y, base_z, tile_count):
    time_step = 0.5
    _, size_x, size_y, depth = u_old.shape
    slots, width = base_x.shape
    plan = Plan(size_x, size_y, depth, slots, width)
    f32, bf16 = jnp.float32, jnp.bfloat16
    devices = lax.axis_size("gx") * lax.axis_size("gy")
    whole, scalars = pl.BlockSpec(memory_space=pltpu.VMEM), pl.BlockSpec(memory_space=pltpu.SMEM)
    far = pl.BlockSpec(memory_space=pl.ANY)
    lines = 8 * slots
    dma = pltpu.SemaphoreType.DMA
    own, plain, weights, places, slot_map, over = pl.pallas_call(
        functools.partial(send_kernel, plan),
        out_shape=[
            jax.ShapeDtypeStruct((plan.total, width), f32),
            jax.ShapeDtypeStruct((plan.total, width), f32),
            jax.ShapeDtypeStruct((16, plan.total), f32),
            jax.ShapeDtypeStruct((2 * plan.tile_rows, width), jnp.int32),
            jax.ShapeDtypeStruct((lines, width), f32),
            jax.ShapeDtypeStruct((8, width), f32),
        ],
        in_specs=[whole] * 5 + [scalars],
        out_specs=[whole] * 6,
        scratch_shapes=[
            pltpu.VMEM((16, plan.markers), f32),
            pltpu.VMEM((plan.listed, plan.markers), bf16),
            pltpu.VMEM((16, plan.listed), f32),
            pltpu.VMEM((16, plan.faces), f32),
            pltpu.VMEM((4, 16, width), f32),
            pltpu.VMEM((16, plan.listed), f32),
            pltpu.VMEM((8, width), f32),
            pltpu.VMEM((devices, 8, width), f32),
            dma((8,)),
            dma((8,)),
            dma((devices,)),
            dma((devices,)),
        ],
        compiler_params=pltpu.CompilerParams(
            vmem_limit_bytes=VMEM_LIMIT, collective_id=0, has_side_effects=True
        ),
        name="send",
    )(offsets, forces, base_x, base_y, base_z, tile_count)

    def sparse(*args):
        u_new, velocity = pl.pallas_call(
            functools.partial(main_kernel, plan, time_step),
            out_shape=[
                jax.ShapeDtypeStruct(u_old.shape, f32),
                jax.ShapeDtypeStruct((8, plan.total), f32),
            ],
            in_specs=[whole] * 3 + [scalars] + [far] * 2,
            out_specs=[far, whole],
            scratch_shapes=[
                pltpu.VMEM((4 * plan.grid_rows, width), f32),
                pltpu.VMEM((2 * plan.grid_rows, width), f32),
                pltpu.VMEM((plan.total, width), f32),
                pltpu.VMEM(u_old.shape, f32),
                pltpu.VMEM(density.shape, f32),
                dma((3,)),
            ],
            compiler_params=pltpu.CompilerParams(vmem_limit_bytes=VMEM_LIMIT),
            name="main",
        )(own, plain, weights, places.reshape(-1), u_old, density)
        out = pl.pallas_call(
            functools.partial(return_kernel, plan),
            out_shape=jax.ShapeDtypeStruct((3, slots, width), f32),
            in_specs=[whole] * 2 + [scalars],
            out_specs=whole,
            scratch_shapes=[
                pltpu.VMEM((plan.listed, plan.markers), bf16),
                pltpu.VMEM((8, plan.faces), f32),
                pltpu.VMEM((4, 8, width), f32),
                dma((8,)),
                dma((8,)),
            ],
            compiler_params=pltpu.CompilerParams(
                vmem_limit_bytes=VMEM_LIMIT, collective_id=1, has_side_effects=True
            ),
            name="give_back",
        )(velocity, slot_map, tile_count)
        return u_new, out

    args = (u_old, density, offsets, forces, base_x, base_y, base_z, tile_count)
    return lax.cond(over[0, 0] > 0.0, dense_device, sparse, *args)


def solution(mesh):
    in_specs = (
        P(None, "gx", "gy", None),
        P("gx", "gy", None),
        P(None, ("gx", "gy"), None),
        P(None, ("gx", "gy"), None),
        P(("gx", "gy"), None),
        P(("gx", "gy"), None),
        P(("gx", "gy"), None),
        P(("gx", "gy")),
    )
    out_specs = (P(None, "gx", "gy", None), P(None, ("gx", "gy"), None))
    return jax.shard_map(
        on_device, mesh=mesh, in_specs=in_specs, out_specs=out_specs, check_vma=False
    )
```

```python
import functools

import jax
import jax.numpy as jnp
from jax import lax
from jax.experimental import pallas as pl
from jax.experimental.pallas import tpu as pltpu
from jax.sharding import PartitionSpec as P

VMEM_LIMIT = 60 * 1024 * 1024
SEND_LIMIT = 10 * 1024 * 1024
MAIN_LIMIT = 35 * 1024 * 1024


def divisor(count, most):
    return max(d for d in range(1, most + 1) if count % d == 0)


def moved(value, step_x, step_y):
    if step_y == 0:
        n = lax.axis_size("gx")
        return lax.ppermute(value, "gx", [(i, (i + step_x) % n) for i in range(n)])
    if step_x == 0:
        n = lax.axis_size("gy")
        return lax.ppermute(value, "gy", [(i, (i + step_y) % n) for i in range(n)])
    nx, ny = lax.axis_size("gx"), lax.axis_size("gy")
    pairs = [
        (i * ny + j, ((i + step_x) % nx) * ny + (j + step_y) % ny)
        for i in range(nx)
        for j in range(ny)
    ]
    return lax.ppermute(value, ("gx", "gy"), pairs)


def stencil(frac):
    root = jnp.sqrt(1.0 + 4.0 * frac - 4.0 * frac * frac)
    return [
        (3.0 - 2.0 * frac - root) / 8.0,
        (3.0 - 2.0 * frac + root) / 8.0,
        (1.0 + 2.0 * frac + root) / 8.0,
        (1.0 + 2.0 * frac - root) / 8.0,
    ]


def pick(delta, four):
    total = jnp.where(delta == 0, four[0], 0.0)
    for k in range(1, 4):
        total = jnp.where(delta == k, four[k], total)
    return total


def wrapped(delta, length):
    delta = jnp.where(delta < 0, delta + length, delta)
    return jnp.where(delta >= length, delta - length, delta)


def edge_weights(frac, base, rows, size):
    row = lax.broadcasted_iota(jnp.int32, (rows, base.shape[1]), 0)
    cell = jnp.where(row == size + 2, -1, row)
    cell = jnp.where(row > size + 2, -8, cell)
    return pick(cell - base + 1, stencil(frac))


def halves(value):
    high = value.astype(jnp.bfloat16)
    low = (value - high.astype(jnp.float32)).astype(jnp.bfloat16)
    return high, low


def edges(size):
    return (size - 1, size, size + 1), (size + 2, 0, 1)


def spread_kernel(size_x, size_y, feat, base, grid, *refs):
    slabs, (wx_s, wy_s, high_s, low_s) = refs[:8], refs[8:]
    planes, rows, depth = grid.shape[1], grid.shape[2], grid.shape[3]
    markers = feat.shape[1]
    wx_s[...] = edge_weights(feat[0:1, :], base[0:1, :], wx_s.shape[0], size_x)
    wy_s[...] = edge_weights(feat[1:2, :], base[1:2, :], rows, size_y)
    four = stencil(feat[2:3, :])
    column = jnp.concatenate(
        four + [base[2:3, :].astype(jnp.float32)] + [feat[3 + c : 4 + c, :] for c in range(3)], axis=0
    ).T
    cut = 256 if markers % 256 == 0 else 128
    for start in range(0, markers, cut):
        part = column[start : start + cut]
        lane = lax.broadcasted_iota(jnp.int32, (cut, depth), 1)
        delta = wrapped(lane - part[:, 4:5].astype(jnp.int32) + 1, depth)
        wz = pick(delta, [part[:, k : k + 1] for k in range(4)])
        for c in range(3):
            high, low = halves(wz * part[:, 5 + c : 6 + c])
            high_s[start : start + cut, c * depth : (c + 1) * depth] = high
            low_s[start : start + cut, c * depth : (c + 1) * depth] = low
    group = divisor(planes, 8)

    def turn(g, carry):
        first = g * group
        left = jnp.concatenate(
            [wy_s[...] * wx_s[pl.ds(first + j, 1), :] for j in range(group)], axis=0
        )
        high, low = halves(left)
        dot = functools.partial(jnp.dot, preferred_element_type=jnp.float32)
        total = dot(high, high_s[...]) + dot(low, high_s[...]) + dot(high, low_s[...])
        for j in range(group):
            for c in range(3):
                grid[c, first + j] = total[j * rows : (j + 1) * rows, c * depth : (c + 1) * depth]
        return carry

    lax.fori_loop(0, planes // group, turn, 0)
    sides_x, sides_y = edges(size_x), edges(size_y)
    for side in range(2):
        for c in range(3):
            for j, p in enumerate(sides_x[side]):
                slabs[side][c, j] = grid[c, p]
                for other in range(2):
                    for i, r in enumerate(sides_y[other]):
                        slabs[4 + 2 * side + other][c, j, i : i + 1] = grid[c, p, r : r + 1]
            for i, r in enumerate(sides_y[side]):
                for p in range(planes):
                    slabs[2 + side][c, i, p : p + 1] = grid[c, p, r : r + 1]


def read_kernel(size_x, size_y, time_step, *refs):
    feat, base, grid, u_old, density, low_x, high_x, low_y, high_y = refs[:9]
    slabs, (u_new, velocity) = refs[9:17], refs[17:19]
    total, wx_s, wy_s, wz3, table = refs[19:]
    planes, rows, depth = grid.shape[1], grid.shape[2], grid.shape[3]
    markers = feat.shape[1]
    wx_s[...] = edge_weights(feat[0:1, :], base[0:1, :], wx_s.shape[0], size_x)
    wy_s[...] = edge_weights(feat[1:2, :], base[1:2, :], rows, size_y)
    cut = 256 if markers % 256 == 0 else 128
    for start in range(0, markers, cut):
        at = slice(start, start + cut)
        row = lax.broadcasted_iota(jnp.int32, (depth, cut), 0)
        delta = wrapped(row - base[2:3, at] + 1, depth)
        high, low = halves(pick(delta, stencil(feat[2:3, at])))
        wz3[0:depth, at] = high
        wz3[depth : 2 * depth, at] = high
        wz3[2 * depth :, at] = low
    total[...] = grid[...]
    near_x, near_y = edges(size_x)[::-1], edges(size_y)[::-1]
    for side in range(2):
        for c in range(3):
            for j, p in enumerate(near_x[side]):
                total[c, p] = total[c, p] + slabs[side][c, j]
                for other in range(2):
                    for i, r in enumerate(near_y[other]):
                        total[c, p, r : r + 1] = (
                            total[c, p, r : r + 1] + slabs[4 + 2 * side + other][c, j, i : i + 1]
                        )
            for i, r in enumerate(near_y[side]):
                for p in range(planes):
                    total[c, p, r : r + 1] = total[c, p, r : r + 1] + slabs[2 + side][c, i, p : p + 1]
    group = divisor(planes, 6)
    spare = jnp.ones((rows - size_y - 3, depth), jnp.float32)

    def plane_state(k, p):
        if p < size_x:
            main = density[p] if k == 3 else u_old[k, p]
        elif p < size_x + 2:
            main = high_x[k, p - size_x]
        else:
            main = low_x[k, 0]
        edge = [high_y[k, 0, p : p + 1], high_y[k, 1, p : p + 1], low_y[k, 0, p : p + 1], spare]
        return jnp.concatenate([main] + edge, axis=0)

    for g in range(planes // group):
        pieces = []
        for p in range(g * group, (g + 1) * group):
            scale = time_step / plane_state(3, p)
            for c in range(3):
                value = plane_state(c, p) + total[c, p] * scale
                if p < size_x:
                    u_new[c, p] = value[:size_y]
                pieces.append(value)
        high, low = halves(jnp.concatenate(pieces, axis=0))
        table[g, :, 0:depth] = high
        table[g, :, depth : 2 * depth] = low
        table[g, :, 2 * depth :] = high

    def turn(step, carry):
        at = pl.ds(pl.multiple_of(step * cut, cut), cut)
        right = wz3[:, at]
        wy = wy_s[:, at]
        sums = [jnp.zeros((8, cut), jnp.float32) for _ in range(3)]
        for g in range(planes // group):
            found = jnp.dot(table[g], right, preferred_element_type=jnp.float32)
            for j in range(group):
                p = g * group + j
                weight = wy * wx_s[p : p + 1, at]
                for c in range(3):
                    first = (j * 3 + c) * rows
                    product = found[first : first + rows] * weight
                    for r in range(0, rows, 8):
                        sums[c] = sums[c] + product[r : r + 8]
        velocity[:, at] = (
            jnp.concatenate([jnp.sum(s, axis=0, keepdims=True) for s in sums], axis=0) * feat[6:7, at]
        )
        return carry

    lax.fori_loop(0, markers // cut, turn, 0)


def dense_device(u_old, density, offsets, forces, base_x, base_y, base_z, tile_count):
    time_step = 0.5
    _, size_x, size_y, depth = u_old.shape
    slots, width = base_x.shape
    markers = slots * width
    planes = size_x + 3
    rows = -(-(size_y + 3) // 8) * 8
    lines = -(-planes // 8) * 8
    f32, bf16 = jnp.float32, jnp.bfloat16
    live = (lax.broadcasted_iota(jnp.int32, (slots, width), 0) < tile_count[0]).astype(f32)
    feat = jnp.concatenate([offsets, forces * live[None], live[None]], axis=0).reshape(7, markers)
    base = jnp.stack([base_x, base_y, base_z], axis=0).reshape(3, markers)

    up = jnp.concatenate([u_old[:, size_x - 1 :], density[None, size_x - 1 :]], axis=0)
    down = jnp.concatenate([u_old[:, :2], density[None, :2]], axis=0)
    low_x, high_x = moved(up, 1, 0), moved(down, -1, 0)

    def strip(r):
        inner = jnp.concatenate([u_old[:, :, r], density[None, :, r]], axis=0)
        return jnp.concatenate([inner, high_x[:, :, r], low_x[:, :, r]], axis=1)

    low_y = moved(strip(size_y - 1)[:, None], 0, 1)
    high_y = moved(jnp.stack([strip(0), strip(1)], axis=1), 0, -1)

    params = pltpu.CompilerParams(vmem_limit_bytes=VMEM_LIMIT)
    slab_x = jax.ShapeDtypeStruct((3, 3, rows, depth), f32)
    slab_y = jax.ShapeDtypeStruct((3, 3, planes, depth), f32)
    corner = jax.ShapeDtypeStruct((3, 3, 3, depth), f32)
    whole = pl.BlockSpec(memory_space=pltpu.VMEM)
    flops = 6 * planes * rows * 3 * depth * markers
    cost = pl.CostEstimate(flops=flops, transcendentals=0, bytes_accessed=8 * planes * rows * depth)
    grid, *slabs = pl.pallas_call(
        functools.partial(spread_kernel, size_x, size_y),
        out_shape=[jax.ShapeDtypeStruct((3, planes, rows, depth), f32)]
        + [slab_x] * 2
        + [slab_y] * 2
        + [corner] * 4,
        in_specs=[whole] * 2,
        out_specs=[whole] * 9,
        scratch_shapes=[
            pltpu.VMEM((lines, markers), f32),
            pltpu.VMEM((rows, markers), f32),
            pltpu.VMEM((markers, 3 * depth), bf16),
            pltpu.VMEM((markers, 3 * depth), bf16),
        ],
        compiler_params=params,
        cost_estimate=cost,
        name="spread",
    )(feat, base)
    ways = [(1, 0), (-1, 0), (0, 1), (0, -1), (1, 1), (1, -1), (-1, 1), (-1, -1)]
    slabs = [moved(slab, *way) for slab, way in zip(slabs, ways)]
    group = divisor(planes, 6)
    u_new, velocity = pl.pallas_call(
        functools.partial(read_kernel, size_x, size_y, time_step),
        out_shape=[
            jax.ShapeDtypeStruct(u_old.shape, f32),
            jax.ShapeDtypeStruct((3, markers), f32),
        ],
        in_specs=[whole] * 17,
        out_specs=[whole] * 2,
        scratch_shapes=[
            pltpu.VMEM((3, planes, rows, depth), f32),
            pltpu.VMEM((lines, markers), f32),
            pltpu.VMEM((rows, markers), f32),
            pltpu.VMEM((3 * depth, markers), bf16),
            pltpu.VMEM((planes // group, group * 3 * rows, 3 * depth), bf16),
        ],
        compiler_params=params,
        cost_estimate=cost,
        name="read",
    )(feat, base, grid, u_old, density, low_x, high_x, low_y, high_y, *slabs)
    return (u_new, velocity.reshape(3, slots, width))


MESH = pl.DeviceIdType.MESH
WAYS = [(1, 0), (-1, 0), (0, 1), (0, -1), (1, 1), (1, -1), (-1, 1), (-1, -1)]
OWN_BATCH, LIST_BATCH = 16, 8
GROUP = 64
HOP = 17


def thirds(value):
    high = value.astype(jnp.bfloat16).astype(jnp.float32)
    rest = value - high
    middle = rest.astype(jnp.bfloat16).astype(jnp.float32)
    return [high, middle, rest - middle]


class Plan:
    def __init__(self, size_x, size_y, depth, slots, width):
        self.size_x, self.size_y, self.depth = size_x, size_y, depth
        self.slots, self.width = slots, width
        self.markers = slots * width

        def cap(reach, size):
            return -(-2 * reach * self.markers // size // width) * width

        corner = width // 4
        self.caps = [cap(2, size_x), cap(1, size_x), cap(2, size_y), cap(1, size_y)] + [corner] * 4
        self.starts = [sum(self.caps[:d]) for d in range(8)]
        self.listed = sum(self.caps)
        self.faces = self.starts[4]
        self.tiles = slots + self.listed // width
        self.total = self.tiles * width
        self.tile_rows = -(-self.tiles // 8) * 8
        self.outers = (size_x + 2) // 2 + 2
        self.outer_rows = 2 * (depth + 4)
        self.grid_rows = self.outers * self.outer_rows

    def span(self, d):
        if d < 4:
            return self.starts[d], self.caps[d]
        return self.faces, self.width


def row_mask(shape, value):
    return lax.broadcasted_iota(jnp.int32, shape, 0) == value


def prepare(plan, data, first, count, batch, spots, own, plain, places):
    width, size_y = plan.width, plan.size_y
    f32, bf16 = jnp.float32, jnp.bfloat16
    k_row = lax.broadcasted_iota(jnp.int32, (32, 6 * width), 0)
    n_lane = lax.broadcasted_iota(jnp.int32, (32, 6 * width), 1)
    kind = k_row % 8
    part, inside = n_lane // width, n_lane % width
    hit = ((kind < 5) & (part == kind)) | ((kind > 4) & (part == 5) & (inside // size_y == kind - 5))
    select = jnp.where(hit & (k_row < 24), 1.0, 0.0).astype(bf16)
    k_row = lax.broadcasted_iota(jnp.int32, (32, 8 * width), 0)
    n_lane = lax.broadcasted_iota(jnp.int32, (32, 8 * width), 1)
    hit = (k_row % 8 == n_lane // width) & (k_row < 24)
    spread_out = jnp.where(hit, 1.0, 0.0).astype(bf16)
    step = 4
    for t0 in range(0, count, step):
        n = min(step, count - t0) * width
        d = data[:, t0 * width : t0 * width + n]
        at = slice((first + t0) * width, (first + t0) * width + n)
        rows = lax.broadcasted_iota(jnp.int32, (8, n), 0)
        w = stencil(jnp.where(rows < 3, d[0:8], 0.5))
        factors = jnp.concatenate([v[2:3] for v in w] + [v[0:1] for v in w], axis=0)
        stack = jnp.concatenate(thirds(factors) + [jnp.zeros((8, n), f32)], axis=0)
        left = stack.T.astype(bf16)
        base = (first + t0) * width * HOP
        x = [
            jnp.dot(left, spread_out[:, i * width : (i + 2) * width], preferred_element_type=f32)
            for i in (4, 6)
        ]
        x = [x[i // 2][:, (i % 2) * width : (i % 2 + 1) * width] for i in range(4)]
        for i in range(0, 4, 2):
            z = jnp.dot(left, spread_out[:, i * width : (i + 2) * width], preferred_element_type=f32)
            for j in range(2):
                for h in range(2):
                    for side in range(2):
                        row = base + 8 * h + 2 * (i + j) + side
                        value = z[:, j * width : (j + 1) * width] * x[2 * h + side]
                        spots[pl.ds(row, n, stride=HOP), :] = value
        block = jnp.concatenate([v[1:2] for v in w] + [d[7:8], d[3:6]], axis=0)
        stack = jnp.concatenate(thirds(block) + [jnp.zeros((8, n), f32)], axis=0).astype(bf16)
        wide = lax.dot_general(
            stack, select, (((0,), (0,)), ((), ())), preferred_element_type=f32
        )
        cols = [wide[:, i * width : (i + 1) * width] for i in range(6)]
        lane = lax.broadcasted_iota(jnp.int32, (n, width), 1)
        y = jnp.where(lane < 3 * size_y, lane % size_y, -1000).astype(f32)
        pattern = pick(y - cols[4] + 1.0, cols[:4])
        plain[at, :] = pattern
        own[at, :] = pattern * cols[5]
    keys, zs, bases, goods = [], [], [], []
    for t in range(count):
        at = slice(t * width, (t + 1) * width)
        bx = data[6:7, at].astype(jnp.int32)
        bz = data[8:9, at].astype(jnp.int32)
        good = data[9:10, at] > 0.0
        lane = lax.broadcasted_iota(jnp.int32, (1, width), 1)
        step_in = lane % batch
        across = bx + 2
        side, outer = across % 2, across // 2
        spare = plan.grid_rows + ((plan.size_x + 2) // 2) * plan.outer_rows + 8 * step_in
        base = side * plan.grid_rows + outer * plan.outer_rows + 2 * bz
        bases.append(jnp.where(good, base, spare))
        keys.append(jnp.where(good, side * (plan.outers + 8) + outer, -100 - 10 * step_in))
        zs.append(bz)
        goods.append(jnp.where(good, 1, 0))
    rows = -(-count // 8) * 8
    fill = [jnp.zeros((rows - count, width), jnp.int32)] if rows > count else []
    key, z = jnp.concatenate(keys + fill, axis=0), jnp.concatenate(zs + fill, axis=0)
    base = jnp.concatenate(bases + fill, axis=0)
    lane = lax.broadcasted_iota(jnp.int32, (rows, width), 1) % batch

    def near(a, b, most):
        return (a - b <= most) & (b - a <= most)

    clashes = [
        (lane >= d) & near(key, pltpu.roll(key, d, 1), 1) & near(z, pltpu.roll(z, d, 1), 3)
        for d in range(1, batch)
    ]
    second = clashes[0]
    for clash in clashes[1:]:
        second = second | clash
    second = jnp.where(second, 1, 0)
    bad = jnp.zeros((rows, width), jnp.int32)
    for d, clash in enumerate(clashes):
        both = second * pltpu.roll(second, d + 1, 1)
        bad = jnp.maximum(bad, jnp.where(clash, both, 0))
    places[first : first + rows, :] = base + second * (2 * plan.grid_rows)
    good = jnp.concatenate(goods + fill, axis=0)
    lane = lax.broadcasted_iota(jnp.int32, (rows, width), 1) // GROUP
    state = jnp.zeros((rows, width), jnp.int32)
    for h in range(width // GROUP):
        here = lane == h
        worst = jnp.max(jnp.where(here, bad, 0), axis=1, keepdims=True)
        some = jnp.max(jnp.where(here, good, 0), axis=1, keepdims=True)
        filled = jnp.sum(jnp.where(here, good, 0), axis=1, keepdims=True)
        state = jnp.where(here, some * (1 + worst * filled), state)
    below = plan.tile_rows + first
    places[below : below + rows, :] = state
    below = 2 * plan.tile_rows + first
    places[below : below + rows, :] = base


def place():
    nx, ny = lax.axis_size("gx"), lax.axis_size("gy")
    return nx, ny, lax.axis_index("gx"), lax.axis_index("gy")


def send_kernel(plan, *refs):
    arguments, tile_count = refs[:5], refs[5]
    (own, plain, spots, places, slot_map, any_over) = refs[6:12]
    data, one_hot, lists, inbox, corners, got, note, notes = refs[12:20]
    send_sem, recv_sem, note_send, note_recv, load_sem = refs[20:25]
    offsets, forces, base_x, base_y, base_z = refs[25:]
    loads = [
        pltpu.make_async_copy(far, near, load_sem.at[i])
        for i, (far, near) in enumerate(zip(arguments, refs[25:]))
    ]
    for load in loads:
        load.start()
    f32, bf16 = jnp.float32, jnp.bfloat16
    slots, width, markers = plan.slots, plan.width, plan.markers
    nx, ny, mx, my = place()
    devices = nx * ny
    me = mx * ny + my

    def other(i):
        to = lax.rem(me + i, devices)
        return to // ny, lax.rem(to, ny)

    barrier = pltpu.get_barrier_semaphore()

    def greet(i, carry):
        pl.semaphore_signal(barrier, inc=1, device_id=other(i), device_id_type=MESH)
        return carry

    lax.fori_loop(1, devices, greet, 0)
    for load in loads:
        load.wait()

    live = jnp.where(lax.broadcasted_iota(jnp.int32, (slots, width), 0) < tile_count[0], 1.0, 0.0)
    bx, by, bz = base_x[...], base_y[...], base_z[...]
    values = [offsets[c] for c in range(3)] + [forces[c] * live for c in range(3)]
    values = values + [bx.astype(f32), by.astype(f32), bz.astype(f32), live]
    data[10:16, :] = jnp.zeros((6, markers), f32)
    for k, value in enumerate(values):
        for t in range(slots):
            data[k : k + 1, t * width : (t + 1) * width] = value[t : t + 1, :]
    ahead_x = jnp.where(bx >= plan.size_x - 2, live, 0.0)
    back_x = jnp.where(bx < 1, live, 0.0)
    ahead_y = jnp.where(by >= plan.size_y - 2, 1.0, 0.0)
    back_y = jnp.where(by < 1, 1.0, 0.0)
    flags = []
    for step_x, step_y in WAYS:
        flag = {1: ahead_x, -1: back_x, 0: live}[step_x]
        flags.append(flag if step_y == 0 else flag * (ahead_y if step_y > 0 else back_y))
    flag = jnp.concatenate(flags, axis=0)
    lines = 8 * slots
    r, c = (lax.broadcasted_iota(jnp.int32, (width, width), a) for a in range(2))
    upper = jnp.where(r <= c, 1.0, 0.0).astype(bf16)
    r, c = (lax.broadcasted_iota(jnp.int32, (lines, lines), a) for a in range(2))
    before = jnp.where((c < r) & (c // slots == r // slots), 1.0, 0.0).astype(bf16)
    within = jnp.dot(flag.astype(bf16), upper, preferred_element_type=f32)
    count = jnp.broadcast_to(jnp.sum(flag, axis=1, keepdims=True), (lines, width))
    earlier = jnp.dot(before, count.astype(bf16), preferred_element_type=f32)
    slot = jnp.where(flag > 0.0, earlier + within - 1.0, -1.0)
    slot_map[...] = slot
    over = jnp.zeros((slots, width), f32)
    for d in range(8):
        here = slot[d * slots : (d + 1) * slots]
        over = jnp.maximum(over, jnp.where(here >= plan.caps[d], 1.0, 0.0))
    note[...] = jnp.broadcast_to(jnp.max(over), note.shape)
    fill_one_hot(plan, slot_map, one_hot)
    stack = jnp.concatenate(thirds(data[...]), axis=0).astype(bf16)
    found = lax.dot_general(
        stack, one_hot[...], (((1,), (1,)), ((), ())), preferred_element_type=f32
    )
    found = found[0:16] + found[16:32] + found[32:48]
    lane = lax.broadcasted_iota(jnp.int32, (1, plan.listed), 1)
    for row, axis, size in ((6, 0, plan.size_x), (7, 1, plan.size_y)):
        shift = jnp.zeros((1, plan.listed), f32)
        for d in range(8):
            inside = (lane >= plan.starts[d]) & (lane < plan.starts[d] + plan.caps[d])
            shift = jnp.where(inside, float(WAYS[d][axis] * size), shift)
        moved_by = jnp.where(row_mask((16, plan.listed), row), shift * found[9:10], 0.0)
        found = found - moved_by
    lists[...] = found

    pl.semaphore_wait(barrier, devices - 1)

    def word(i):
        return pltpu.make_async_remote_copy(
            src_ref=note,
            dst_ref=notes.at[i],
            send_sem=note_send.at[i],
            recv_sem=note_recv.at[i],
            device_id=other(i),
            device_id_type=MESH,
        )

    def tell(i, carry):
        word(i).start()
        return carry

    lax.fori_loop(1, devices, tell, 0)
    copies = []
    for d, (step_x, step_y) in enumerate(WAYS):
        start, size = plan.span(d)
        target = inbox.at[:, pl.ds(start, size)] if d < 4 else corners.at[d - 4]
        copies.append(
            pltpu.make_async_remote_copy(
                src_ref=lists.at[:, pl.ds(start, size)],
                dst_ref=target,
                send_sem=send_sem.at[d],
                recv_sem=recv_sem.at[d],
                device_id=(lax.rem(mx + step_x + nx, nx), lax.rem(my + step_y + ny, ny)),
                device_id_type=MESH,
            )
        )
        copies[-1].start()

    prepare(plan, data, 0, slots, OWN_BATCH, spots, own, plain, places)
    for copy in copies:
        copy.wait()

    got[:, 0 : plan.faces] = inbox[...]
    lane = lax.broadcasted_iota(jnp.int32, (16, width), 1) // plan.caps[4]
    last = corners[0]
    for i in range(1, 4):
        last = jnp.where(lane == i, corners[i], last)
    got[:, plan.faces :] = last
    prepare(plan, got, slots, plan.tiles - slots, LIST_BATCH, spots, own, plain, places)

    def hear(i, most):
        word(i).wait()
        return jnp.maximum(most, notes[i])

    any_over[0] = jnp.max(lax.fori_loop(1, devices, hear, note[...])).astype(jnp.int32)


def fill_one_hot(plan, slot_map, one_hot):
    for d in range(8):
        rows = plan.caps[d]
        index = lax.broadcasted_iota(jnp.int32, (rows, plan.width), 0).astype(jnp.float32)
        for t in range(plan.slots):
            line = slot_map[d * plan.slots + t : d * plan.slots + t + 1, :]
            hot = jnp.where(index == line, 1.0, 0.0).astype(jnp.bfloat16)
            one_hot[plan.starts[d] : plan.starts[d] + rows, t * plan.width : (t + 1) * plan.width] = hot


def main_kernel(plan, time_step, *refs):
    own, plain, spots, places, tile_count, u_in, density_in, u_out, velocity = refs[:9]
    grid, table, found, sums, u_s, density_s, sems = refs[9:]
    f32, bf16 = jnp.float32, jnp.bfloat16
    width, depth, size_y, total = plan.width, plan.depth, plan.size_y, plan.total
    outer_rows, grid_rows = plan.outer_rows, plan.grid_rows
    loads = [
        pltpu.make_async_copy(u_in, u_s, sems.at[0]),
        pltpu.make_async_copy(density_in, density_s, sems.at[1]),
    ]
    for load in loads:
        load.start()
    zero = jnp.zeros((8, width), f32)
    group = divisor(4 * grid_rows // 8, 52)

    def clear(i, carry):
        for j in range(group):
            grid[pl.ds(pl.multiple_of((i * group + j) * 8, 8), 8), :] = zero
        return carry

    lax.fori_loop(0, 4 * grid_rows // 8 // group, clear, 0)
    for o in (0, 1, plan.outers - 2, plan.outers - 1):
        for g in range(2):
            at = g * grid_rows + o * outer_rows
            table[at : at + outer_rows, :] = jnp.zeros((outer_rows, width), f32)
    found[plan.markers :, :] = jnp.zeros((plan.listed, width), f32)

    def spread_group(batch, g, carry):
        first = g * GROUP
        state = places[plan.tile_rows * width + first]

        def windows(j):
            here = places[first + j]
            at = first * HOP + j * HOP
            row = jnp.broadcast_to(own[pl.ds(first + j, 1), :], (8, width))
            one, two = pl.ds(here, 8), pl.ds(here + outer_rows, 8)
            return [
                (one, grid[one, :] + spots[pl.ds(at, 8), :] * row),
                (two, grid[two, :] + spots[pl.ds(at + 8, 8), :] * row),
            ]

        @pl.when(state == 1)
        def _():
            for j0 in range(0, GROUP, batch):
                stores = []
                for j in range(j0, j0 + batch):
                    stores = stores + windows(j)
                for where, value in stores:
                    grid[where, :] = value

        @pl.when(state > 1)
        def _():
            def single(j, c):
                for where, value in windows(j):
                    grid[where, :] = value
                return c

            lax.fori_loop(0, state - 1, single, 0)

        return carry

    live_groups = tile_count[0] * (width // GROUP)
    lists_from, all_groups = plan.markers // GROUP, total // GROUP
    lax.fori_loop(0, live_groups, functools.partial(spread_group, OWN_BATCH), 0)
    lax.fori_loop(lists_from, all_groups, functools.partial(spread_group, LIST_BATCH), 0)

    def fold(i, carry):
        at = i * outer_rows
        ends = [(2 * depth, 0, 2), (2, 2 * depth + 2, 4)]
        for to, source, rows in ends:
            grid[pl.ds(at + to, rows), :] = grid[pl.ds(at + to, rows), :] + grid[pl.ds(at + source, rows), :]
        return carry

    lax.fori_loop(0, 4 * plan.outers, fold, 0)
    for load in loads:
        load.wait()

    def lines(g, outer, side):
        return pl.ds(g * grid_rows + outer * outer_rows + 2 + side, depth, stride=2)

    def plane(p, homes):
        force = None
        for copy in range(2):
            for g, outer, side in homes:
                part = grid[lines(2 * copy + g, outer, side), :]
                force = part if force is None else force + part
        force = force.T
        scale = time_step / density_s[p]
        pieces = []
        for c in range(3):
            value = u_s[c, p] + force[c * size_y : (c + 1) * size_y] * scale
            u_s[c, p] = value
            pieces.append(value)
        if width > 3 * size_y:
            pieces.append(jnp.zeros((width - 3 * size_y, depth), f32))
        back = jnp.concatenate(pieces, axis=0).T
        for g, outer, side in homes:
            table[lines(g, outer, side), :] = back
            at = g * grid_rows + outer * outer_rows + side
            table[pl.ds(at, 1), :] = back[depth - 1 : depth]
            table[pl.ds(at + 2 * depth + 2, 1), :] = back[0:1]
            table[pl.ds(at + 2 * depth + 4, 1), :] = back[1:2]

    def pair(i, carry):
        plane(2 * i, [(0, i + 1, 1), (1, i + 1, 0)])
        plane(2 * i + 1, [(0, i + 2, 0), (1, i + 1, 1)])
        return carry

    lax.fori_loop(0, plan.size_x // 2, pair, 0)
    leave = pltpu.make_async_copy(u_s, u_out, sems.at[2])
    leave.start()

    def read_group(g, carry):
        first = g * GROUP

        @pl.when(places[plan.tile_rows * width + first] > 0)
        def _():
            for j in range(GROUP):
                here = places[2 * plan.tile_rows * width + first + j]
                at = first * HOP + j * HOP
                sums[9 * j : 9 * j + 8, :] = (
                    table[pl.ds(here, 8), :] * spots[pl.ds(at, 8), :]
                    + table[pl.ds(here + outer_rows, 8), :] * spots[pl.ds(at + 8, 8), :]
                )
            for j in range(0, GROUP, 8):
                row = sums[pl.ds(9 * j, 8, stride=9), :]
                for s in range(1, 8):
                    row = row + sums[pl.ds(9 * j + s, 8, stride=9), :]
                block = pl.ds(pl.multiple_of(first + j, 8), 8)
                found[block, :] = row * plain[block, :]

        return carry

    lax.fori_loop(0, live_groups, read_group, 0)
    lax.fori_loop(lists_from, all_groups, read_group, 0)
    r = lax.broadcasted_iota(jnp.int32, (16, width), 0)
    lane = lax.broadcasted_iota(jnp.int32, (16, width), 1)
    by_part = jnp.where((lane // size_y == r) & (lane < 3 * size_y), 1.0, 0.0).astype(bf16)
    block = 4 * width
    for first in range(0, total, block):
        n = min(block, total - first)
        value = found[first : first + n, :]
        result = None
        for piece in thirds(value):
            part = lax.dot_general(
                by_part, piece.astype(bf16), (((1,), (1,)), ((), ())), preferred_element_type=f32
            )
            result = part if result is None else result + part
        velocity[:, first : first + n] = result[0:8]
    leave.wait()


def return_kernel(plan, *refs):
    velocity, slot_map, tile_count, out, one_hot, inbox, corners, send_sem, recv_sem = refs
    f32, bf16 = jnp.float32, jnp.bfloat16
    width = plan.width
    nx, ny, mx, my = place()
    barrier = pltpu.get_barrier_semaphore()

    def neighbour(step_x, step_y):
        return (lax.rem(mx + step_x + nx, nx), lax.rem(my + step_y + ny, ny))

    for way in WAYS:
        pl.semaphore_signal(barrier, inc=1, device_id=neighbour(*way), device_id_type=MESH)
    pl.semaphore_wait(barrier, len(WAYS))
    copies = []
    for d, (step_x, step_y) in enumerate(WAYS):
        start, size = plan.span(d)
        target = inbox.at[:, pl.ds(start, size)] if d < 4 else corners.at[d - 4]
        copies.append(
            pltpu.make_async_remote_copy(
                src_ref=velocity.at[:, pl.ds(plan.markers + start, size)],
                dst_ref=target,
                send_sem=send_sem.at[d],
                recv_sem=recv_sem.at[d],
                device_id=neighbour(-step_x, -step_y),
                device_id_type=MESH,
            )
        )
        copies[-1].start()
    fill_one_hot(plan, slot_map, one_hot)
    for copy in copies:
        copy.wait()
    lane = lax.broadcasted_iota(jnp.int32, (8, width), 1) // plan.caps[4]
    last = corners[0]
    for i in range(1, 4):
        last = jnp.where(lane == i, corners[i], last)
    back = jnp.concatenate([inbox[...], last], axis=1)
    stack = jnp.concatenate(thirds(back) + [jnp.zeros_like(back)], axis=0).astype(bf16)
    extra = jnp.dot(stack, one_hot[...], preferred_element_type=f32)
    extra = extra[0:8] + extra[8:16] + extra[16:24]
    total = velocity[:, 0 : plan.markers] + extra
    live = tile_count[0]
    for t in range(plan.slots):
        row = total[:, t * width : (t + 1) * width]
        row = jnp.where(lax.broadcasted_iota(jnp.int32, row.shape, 0) * 0 + t < live, row, 0.0)
        for c in range(3):
            out[c, t : t + 1, :] = row[c : c + 1, :]


def on_device(u_old, density, offsets, forces, base_x, base_y, base_z, tile_count):
    time_step = 0.5
    _, size_x, size_y, depth = u_old.shape
    slots, width = base_x.shape
    plan = Plan(size_x, size_y, depth, slots, width)
    f32, bf16 = jnp.float32, jnp.bfloat16
    devices = lax.axis_size("gx") * lax.axis_size("gy")
    whole, scalars = pl.BlockSpec(memory_space=pltpu.VMEM), pl.BlockSpec(memory_space=pltpu.SMEM)
    far = pl.BlockSpec(memory_space=pl.ANY)
    lines = 8 * slots
    dma = pltpu.SemaphoreType.DMA
    own, plain, spots, places, slot_map, over = pl.pallas_call(
        functools.partial(send_kernel, plan),
        out_shape=[
            jax.ShapeDtypeStruct((plan.total, width), f32),
            jax.ShapeDtypeStruct((plan.total, width), f32),
            jax.ShapeDtypeStruct((plan.total * HOP, width), f32),
            jax.ShapeDtypeStruct((3 * plan.tile_rows, width), jnp.int32),
            jax.ShapeDtypeStruct((lines, width), f32),
            jax.ShapeDtypeStruct((1,), jnp.int32),
        ],
        in_specs=[far] * 5 + [scalars],
        out_specs=[whole] * 5 + [scalars],
        scratch_shapes=[
            pltpu.VMEM((16, plan.markers), f32),
            pltpu.VMEM((plan.listed, plan.markers), bf16),
            pltpu.VMEM((16, plan.listed), f32),
            pltpu.VMEM((16, plan.faces), f32),
            pltpu.VMEM((4, 16, width), f32),
            pltpu.VMEM((16, plan.listed), f32),
            pltpu.VMEM((8, width), f32),
            pltpu.VMEM((devices, 8, width), f32),
            dma((8,)),
            dma((8,)),
            dma((devices,)),
            dma((devices,)),
            dma((5,)),
        ]
        + [pltpu.VMEM(offsets.shape, f32)] * 2
        + [pltpu.VMEM(base_x.shape, jnp.int32)] * 3,
        compiler_params=pltpu.CompilerParams(
            vmem_limit_bytes=SEND_LIMIT, collective_id=0, has_side_effects=True
        ),
        name="send",
    )(offsets, forces, base_x, base_y, base_z, tile_count)

    def sparse(*args):
        u_new, velocity = pl.pallas_call(
            functools.partial(main_kernel, plan, time_step),
            out_shape=[
                jax.ShapeDtypeStruct(u_old.shape, f32),
                jax.ShapeDtypeStruct((8, plan.total), f32),
            ],
            in_specs=[whole] * 3 + [scalars] * 2 + [far] * 2,
            out_specs=[far, whole],
            scratch_shapes=[
                pltpu.VMEM((4 * plan.grid_rows, width), f32),
                pltpu.VMEM((2 * plan.grid_rows, width), f32),
                pltpu.VMEM((plan.total, width), f32),
                pltpu.VMEM((9 * GROUP, width), f32),
                pltpu.VMEM(u_old.shape, f32),
                pltpu.VMEM(density.shape, f32),
                dma((3,)),
            ],
            compiler_params=pltpu.CompilerParams(vmem_limit_bytes=MAIN_LIMIT),
            name="main",
        )(own, plain, spots, places.reshape(-1), tile_count, u_old, density)
        out = pl.pallas_call(
            functools.partial(return_kernel, plan),
            out_shape=jax.ShapeDtypeStruct((3, slots, width), f32),
            in_specs=[whole] * 2 + [scalars],
            out_specs=whole,
            scratch_shapes=[
                pltpu.VMEM((plan.listed, plan.markers), bf16),
                pltpu.VMEM((8, plan.faces), f32),
                pltpu.VMEM((4, 8, width), f32),
                dma((8,)),
                dma((8,)),
            ],
            compiler_params=pltpu.CompilerParams(
                vmem_limit_bytes=VMEM_LIMIT, collective_id=1, has_side_effects=True
            ),
            name="give_back",
        )(velocity, slot_map, tile_count)
        return u_new, out

    args = (u_old, density, offsets, forces, base_x, base_y, base_z, tile_count)
    return lax.cond(over[0] > 0, dense_device, sparse, *args)


def solution(mesh):
    in_specs = (
        P(None, "gx", "gy", None),
        P("gx", "gy", None),
        P(None, ("gx", "gy"), None),
        P(None, ("gx", "gy"), None),
        P(("gx", "gy"), None),
        P(("gx", "gy"), None),
        P(("gx", "gy"), None),
        P(("gx", "gy")),
    )
    out_specs = (P(None, "gx", "gy", None), P(None, ("gx", "gy"), None))
    return jax.shard_map(
        on_device, mesh=mesh, in_specs=in_specs, out_specs=out_specs, check_vma=False
    )
```

```python
import functools

import jax
import jax.numpy as jnp
from jax import lax
from jax.experimental import pallas as pl
from jax.experimental.pallas import tpu as pltpu
from jax.sharding import PartitionSpec as P

VMEM_LIMIT = 60 * 1024 * 1024
SEND_LIMIT = 10 * 1024 * 1024
MAIN_LIMIT = 26 * 1024 * 1024


def divisor(count, most):
    return max(d for d in range(1, most + 1) if count % d == 0)


def moved(value, step_x, step_y):
    if step_y == 0:
        n = lax.axis_size("gx")
        return lax.ppermute(value, "gx", [(i, (i + step_x) % n) for i in range(n)])
    if step_x == 0:
        n = lax.axis_size("gy")
        return lax.ppermute(value, "gy", [(i, (i + step_y) % n) for i in range(n)])
    nx, ny = lax.axis_size("gx"), lax.axis_size("gy")
    pairs = [
        (i * ny + j, ((i + step_x) % nx) * ny + (j + step_y) % ny)
        for i in range(nx)
        for j in range(ny)
    ]
    return lax.ppermute(value, ("gx", "gy"), pairs)


def stencil(frac):
    root = jnp.sqrt(1.0 + 4.0 * frac - 4.0 * frac * frac)
    return [
        (3.0 - 2.0 * frac - root) / 8.0,
        (3.0 - 2.0 * frac + root) / 8.0,
        (1.0 + 2.0 * frac + root) / 8.0,
        (1.0 + 2.0 * frac - root) / 8.0,
    ]


def pick(delta, four):
    total = jnp.where(delta == 0, four[0], 0.0)
    for k in range(1, 4):
        total = jnp.where(delta == k, four[k], total)
    return total


def wrapped(delta, length):
    delta = jnp.where(delta < 0, delta + length, delta)
    return jnp.where(delta >= length, delta - length, delta)


def edge_weights(frac, base, rows, size):
    row = lax.broadcasted_iota(jnp.int32, (rows, base.shape[1]), 0)
    cell = jnp.where(row == size + 2, -1, row)
    cell = jnp.where(row > size + 2, -8, cell)
    return pick(cell - base + 1, stencil(frac))


def halves(value):
    high = value.astype(jnp.bfloat16)
    low = (value - high.astype(jnp.float32)).astype(jnp.bfloat16)
    return high, low


def edges(size):
    return (size - 1, size, size + 1), (size + 2, 0, 1)


def spread_kernel(size_x, size_y, feat, base, grid, *refs):
    slabs, (wx_s, wy_s, high_s, low_s) = refs[:8], refs[8:]
    planes, rows, depth = grid.shape[1], grid.shape[2], grid.shape[3]
    markers = feat.shape[1]
    wx_s[...] = edge_weights(feat[0:1, :], base[0:1, :], wx_s.shape[0], size_x)
    wy_s[...] = edge_weights(feat[1:2, :], base[1:2, :], rows, size_y)
    four = stencil(feat[2:3, :])
    column = jnp.concatenate(
        four + [base[2:3, :].astype(jnp.float32)] + [feat[3 + c : 4 + c, :] for c in range(3)], axis=0
    ).T
    cut = 256 if markers % 256 == 0 else 128
    for start in range(0, markers, cut):
        part = column[start : start + cut]
        lane = lax.broadcasted_iota(jnp.int32, (cut, depth), 1)
        delta = wrapped(lane - part[:, 4:5].astype(jnp.int32) + 1, depth)
        wz = pick(delta, [part[:, k : k + 1] for k in range(4)])
        for c in range(3):
            high, low = halves(wz * part[:, 5 + c : 6 + c])
            high_s[start : start + cut, c * depth : (c + 1) * depth] = high
            low_s[start : start + cut, c * depth : (c + 1) * depth] = low
    group = divisor(planes, 8)

    def turn(g, carry):
        first = g * group
        left = jnp.concatenate(
            [wy_s[...] * wx_s[pl.ds(first + j, 1), :] for j in range(group)], axis=0
        )
        high, low = halves(left)
        dot = functools.partial(jnp.dot, preferred_element_type=jnp.float32)
        total = dot(high, high_s[...]) + dot(low, high_s[...]) + dot(high, low_s[...])
        for j in range(group):
            for c in range(3):
                grid[c, first + j] = total[j * rows : (j + 1) * rows, c * depth : (c + 1) * depth]
        return carry

    lax.fori_loop(0, planes // group, turn, 0)
    sides_x, sides_y = edges(size_x), edges(size_y)
    for side in range(2):
        for c in range(3):
            for j, p in enumerate(sides_x[side]):
                slabs[side][c, j] = grid[c, p]
                for other in range(2):
                    for i, r in enumerate(sides_y[other]):
                        slabs[4 + 2 * side + other][c, j, i : i + 1] = grid[c, p, r : r + 1]
            for i, r in enumerate(sides_y[side]):
                for p in range(planes):
                    slabs[2 + side][c, i, p : p + 1] = grid[c, p, r : r + 1]


def read_kernel(size_x, size_y, time_step, *refs):
    feat, base, grid, u_old, density, low_x, high_x, low_y, high_y = refs[:9]
    slabs, (u_new, velocity) = refs[9:17], refs[17:19]
    total, wx_s, wy_s, wz3, table = refs[19:]
    planes, rows, depth = grid.shape[1], grid.shape[2], grid.shape[3]
    markers = feat.shape[1]
    wx_s[...] = edge_weights(feat[0:1, :], base[0:1, :], wx_s.shape[0], size_x)
    wy_s[...] = edge_weights(feat[1:2, :], base[1:2, :], rows, size_y)
    cut = 256 if markers % 256 == 0 else 128
    for start in range(0, markers, cut):
        at = slice(start, start + cut)
        row = lax.broadcasted_iota(jnp.int32, (depth, cut), 0)
        delta = wrapped(row - base[2:3, at] + 1, depth)
        high, low = halves(pick(delta, stencil(feat[2:3, at])))
        wz3[0:depth, at] = high
        wz3[depth : 2 * depth, at] = high
        wz3[2 * depth :, at] = low
    total[...] = grid[...]
    near_x, near_y = edges(size_x)[::-1], edges(size_y)[::-1]
    for side in range(2):
        for c in range(3):
            for j, p in enumerate(near_x[side]):
                total[c, p] = total[c, p] + slabs[side][c, j]
                for other in range(2):
                    for i, r in enumerate(near_y[other]):
                        total[c, p, r : r + 1] = (
                            total[c, p, r : r + 1] + slabs[4 + 2 * side + other][c, j, i : i + 1]
                        )
            for i, r in enumerate(near_y[side]):
                for p in range(planes):
                    total[c, p, r : r + 1] = total[c, p, r : r + 1] + slabs[2 + side][c, i, p : p + 1]
    group = divisor(planes, 6)
    spare = jnp.ones((rows - size_y - 3, depth), jnp.float32)

    def plane_state(k, p):
        if p < size_x:
            main = density[p] if k == 3 else u_old[k, p]
        elif p < size_x + 2:
            main = high_x[k, p - size_x]
        else:
            main = low_x[k, 0]
        edge = [high_y[k, 0, p : p + 1], high_y[k, 1, p : p + 1], low_y[k, 0, p : p + 1], spare]
        return jnp.concatenate([main] + edge, axis=0)

    for g in range(planes // group):
        pieces = []
        for p in range(g * group, (g + 1) * group):
            scale = time_step / plane_state(3, p)
            for c in range(3):
                value = plane_state(c, p) + total[c, p] * scale
                if p < size_x:
                    u_new[c, p] = value[:size_y]
                pieces.append(value)
        high, low = halves(jnp.concatenate(pieces, axis=0))
        table[g, :, 0:depth] = high
        table[g, :, depth : 2 * depth] = low
        table[g, :, 2 * depth :] = high

    def turn(step, carry):
        at = pl.ds(pl.multiple_of(step * cut, cut), cut)
        right = wz3[:, at]
        wy = wy_s[:, at]
        sums = [jnp.zeros((8, cut), jnp.float32) for _ in range(3)]
        for g in range(planes // group):
            found = jnp.dot(table[g], right, preferred_element_type=jnp.float32)
            for j in range(group):
                p = g * group + j
                weight = wy * wx_s[p : p + 1, at]
                for c in range(3):
                    first = (j * 3 + c) * rows
                    product = found[first : first + rows] * weight
                    for r in range(0, rows, 8):
                        sums[c] = sums[c] + product[r : r + 8]
        velocity[:, at] = (
            jnp.concatenate([jnp.sum(s, axis=0, keepdims=True) for s in sums], axis=0) * feat[6:7, at]
        )
        return carry

    lax.fori_loop(0, markers // cut, turn, 0)


def dense_device(u_old, density, offsets, forces, base_x, base_y, base_z, tile_count):
    time_step = 0.5
    _, size_x, size_y, depth = u_old.shape
    slots, width = base_x.shape
    markers = slots * width
    planes = size_x + 3
    rows = -(-(size_y + 3) // 8) * 8
    lines = -(-planes // 8) * 8
    f32, bf16 = jnp.float32, jnp.bfloat16
    live = (lax.broadcasted_iota(jnp.int32, (slots, width), 0) < tile_count[0]).astype(f32)
    feat = jnp.concatenate([offsets, forces * live[None], live[None]], axis=0).reshape(7, markers)
    base = jnp.stack([base_x, base_y, base_z], axis=0).reshape(3, markers)

    up = jnp.concatenate([u_old[:, size_x - 1 :], density[None, size_x - 1 :]], axis=0)
    down = jnp.concatenate([u_old[:, :2], density[None, :2]], axis=0)
    low_x, high_x = moved(up, 1, 0), moved(down, -1, 0)

    def strip(r):
        inner = jnp.concatenate([u_old[:, :, r], density[None, :, r]], axis=0)
        return jnp.concatenate([inner, high_x[:, :, r], low_x[:, :, r]], axis=1)

    low_y = moved(strip(size_y - 1)[:, None], 0, 1)
    high_y = moved(jnp.stack([strip(0), strip(1)], axis=1), 0, -1)

    params = pltpu.CompilerParams(vmem_limit_bytes=VMEM_LIMIT)
    slab_x = jax.ShapeDtypeStruct((3, 3, rows, depth), f32)
    slab_y = jax.ShapeDtypeStruct((3, 3, planes, depth), f32)
    corner = jax.ShapeDtypeStruct((3, 3, 3, depth), f32)
    whole = pl.BlockSpec(memory_space=pltpu.VMEM)
    flops = 6 * planes * rows * 3 * depth * markers
    cost = pl.CostEstimate(flops=flops, transcendentals=0, bytes_accessed=8 * planes * rows * depth)
    grid, *slabs = pl.pallas_call(
        functools.partial(spread_kernel, size_x, size_y),
        out_shape=[jax.ShapeDtypeStruct((3, planes, rows, depth), f32)]
        + [slab_x] * 2
        + [slab_y] * 2
        + [corner] * 4,
        in_specs=[whole] * 2,
        out_specs=[whole] * 9,
        scratch_shapes=[
            pltpu.VMEM((lines, markers), f32),
            pltpu.VMEM((rows, markers), f32),
            pltpu.VMEM((markers, 3 * depth), bf16),
            pltpu.VMEM((markers, 3 * depth), bf16),
        ],
        compiler_params=params,
        cost_estimate=cost,
        name="spread",
    )(feat, base)
    ways = [(1, 0), (-1, 0), (0, 1), (0, -1), (1, 1), (1, -1), (-1, 1), (-1, -1)]
    slabs = [moved(slab, *way) for slab, way in zip(slabs, ways)]
    group = divisor(planes, 6)
    u_new, velocity = pl.pallas_call(
        functools.partial(read_kernel, size_x, size_y, time_step),
        out_shape=[
            jax.ShapeDtypeStruct(u_old.shape, f32),
            jax.ShapeDtypeStruct((3, markers), f32),
        ],
        in_specs=[whole] * 17,
        out_specs=[whole] * 2,
        scratch_shapes=[
            pltpu.VMEM((3, planes, rows, depth), f32),
            pltpu.VMEM((lines, markers), f32),
            pltpu.VMEM((rows, markers), f32),
            pltpu.VMEM((3 * depth, markers), bf16),
            pltpu.VMEM((planes // group, group * 3 * rows, 3 * depth), bf16),
        ],
        compiler_params=params,
        cost_estimate=cost,
        name="read",
    )(feat, base, grid, u_old, density, low_x, high_x, low_y, high_y, *slabs)
    return (u_new, velocity.reshape(3, slots, width))


MESH = pl.DeviceIdType.MESH
WAYS = [(1, 0), (-1, 0), (0, 1), (0, -1), (1, 1), (1, -1), (-1, 1), (-1, -1)]
OWN_BATCH, LIST_BATCH = 16, 8
GROUP = 64
HOP = 17


def thirds(value):
    high = value.astype(jnp.bfloat16).astype(jnp.float32)
    rest = value - high
    middle = rest.astype(jnp.bfloat16).astype(jnp.float32)
    return [high, middle, rest - middle]


class Plan:
    def __init__(self, size_x, size_y, depth, slots, width):
        self.size_x, self.size_y, self.depth = size_x, size_y, depth
        self.slots, self.width = slots, width
        self.markers = slots * width

        def cap(reach, size):
            return -(-2 * reach * self.markers // size // width) * width

        corner = width // 4
        self.caps = [cap(2, size_x), cap(1, size_x), cap(2, size_y), cap(1, size_y)] + [corner] * 4
        self.starts = [sum(self.caps[:d]) for d in range(8)]
        self.listed = sum(self.caps)
        self.faces = self.starts[4]
        self.tiles = slots + self.listed // width
        self.total = self.tiles * width
        self.tile_rows = -(-self.tiles // 8) * 8
        self.outers = (size_x + 2) // 2 + 2
        self.outer_rows = 2 * (depth + 4)
        self.grid_rows = self.outers * self.outer_rows

    def span(self, d):
        if d < 4:
            return self.starts[d], self.caps[d]
        return self.faces, self.width


def row_mask(shape, value):
    return lax.broadcasted_iota(jnp.int32, shape, 0) == value


def prepare(plan, data, first, count, batch, spots, own, plain, places):
    width, size_y = plan.width, plan.size_y
    f32, bf16 = jnp.float32, jnp.bfloat16
    k_row = lax.broadcasted_iota(jnp.int32, (32, 6 * width), 0)
    n_lane = lax.broadcasted_iota(jnp.int32, (32, 6 * width), 1)
    kind = k_row % 8
    part, inside = n_lane // width, n_lane % width
    hit = ((kind < 5) & (part == kind)) | ((kind > 4) & (part == 5) & (inside // size_y == kind - 5))
    select = jnp.where(hit & (k_row < 24), 1.0, 0.0).astype(bf16)
    k_row = lax.broadcasted_iota(jnp.int32, (32, 8 * width), 0)
    n_lane = lax.broadcasted_iota(jnp.int32, (32, 8 * width), 1)
    hit = (k_row % 8 == n_lane // width) & (k_row < 24)
    spread_out = jnp.where(hit, 1.0, 0.0).astype(bf16)
    step = 4
    for t0 in range(0, count, step):
        n = min(step, count - t0) * width
        d = data[:, t0 * width : t0 * width + n]
        at = slice((first + t0) * width, (first + t0) * width + n)
        rows = lax.broadcasted_iota(jnp.int32, (8, n), 0)
        w = stencil(jnp.where(rows < 3, d[0:8], 0.5))
        factors = jnp.concatenate([v[2:3] for v in w] + [v[0:1] for v in w], axis=0)
        stack = jnp.concatenate(thirds(factors) + [jnp.zeros((8, n), f32)], axis=0)
        left = stack.T.astype(bf16)
        base = (first + t0) * width * HOP
        x = [
            jnp.dot(left, spread_out[:, i * width : (i + 2) * width], preferred_element_type=f32)
            for i in (4, 6)
        ]
        x = [x[i // 2][:, (i % 2) * width : (i % 2 + 1) * width] for i in range(4)]
        for i in range(0, 4, 2):
            z = jnp.dot(left, spread_out[:, i * width : (i + 2) * width], preferred_element_type=f32)
            for j in range(2):
                for h in range(2):
                    for side in range(2):
                        row = base + 8 * h + 2 * (i + j) + side
                        value = z[:, j * width : (j + 1) * width] * x[2 * h + side]
                        spots[pl.ds(row, n, stride=HOP), :] = value
        block = jnp.concatenate([v[1:2] for v in w] + [d[7:8], d[3:6]], axis=0)
        stack = jnp.concatenate(thirds(block) + [jnp.zeros((8, n), f32)], axis=0).astype(bf16)
        wide = lax.dot_general(
            stack, select, (((0,), (0,)), ((), ())), preferred_element_type=f32
        )
        cols = [wide[:, i * width : (i + 1) * width] for i in range(6)]
        lane = lax.broadcasted_iota(jnp.int32, (n, width), 1)
        y = jnp.where(lane < 3 * size_y, lane % size_y, -1000).astype(f32)
        pattern = pick(y - cols[4] + 1.0, cols[:4])
        plain[at, :] = pattern
        own[at, :] = pattern * cols[5]
    keys, zs, bases, goods = [], [], [], []
    for t in range(count):
        at = slice(t * width, (t + 1) * width)
        bx = data[6:7, at].astype(jnp.int32)
        bz = data[8:9, at].astype(jnp.int32)
        good = data[9:10, at] > 0.0
        lane = lax.broadcasted_iota(jnp.int32, (1, width), 1)
        step_in = lane % batch
        across = bx + 2
        side, outer = across % 2, across // 2
        spare = plan.grid_rows + ((plan.size_x + 2) // 2) * plan.outer_rows + 8 * step_in
        base = side * plan.grid_rows + outer * plan.outer_rows + 2 * bz
        bases.append(jnp.where(good, base, spare))
        keys.append(jnp.where(good, side * (plan.outers + 8) + outer, -100 - 10 * step_in))
        zs.append(bz)
        goods.append(jnp.where(good, 1, 0))
    rows = -(-count // 8) * 8
    fill = [jnp.zeros((rows - count, width), jnp.int32)] if rows > count else []
    key, z = jnp.concatenate(keys + fill, axis=0), jnp.concatenate(zs + fill, axis=0)
    base = jnp.concatenate(bases + fill, axis=0)
    lane = lax.broadcasted_iota(jnp.int32, (rows, width), 1) % batch

    def near(a, b, most):
        return (a - b <= most) & (b - a <= most)

    clashes = [
        (lane >= d) & near(key, pltpu.roll(key, d, 1), 1) & near(z, pltpu.roll(z, d, 1), 3)
        for d in range(1, batch)
    ]
    second = clashes[0]
    for clash in clashes[1:]:
        second = second | clash
    second = jnp.where(second, 1, 0)
    bad = jnp.zeros((rows, width), jnp.int32)
    for d, clash in enumerate(clashes):
        both = second * pltpu.roll(second, d + 1, 1)
        bad = jnp.maximum(bad, jnp.where(clash, both, 0))
    places[first : first + rows, :] = base + second * (2 * plan.grid_rows)
    good = jnp.concatenate(goods + fill, axis=0)
    lane = lax.broadcasted_iota(jnp.int32, (rows, width), 1) // GROUP
    state = jnp.zeros((rows, width), jnp.int32)
    for h in range(width // GROUP):
        here = lane == h
        worst = jnp.max(jnp.where(here, bad, 0), axis=1, keepdims=True)
        some = jnp.max(jnp.where(here, good, 0), axis=1, keepdims=True)
        filled = jnp.sum(jnp.where(here, good, 0), axis=1, keepdims=True)
        state = jnp.where(here, some * (1 + worst * filled), state)
    below = plan.tile_rows + first
    places[below : below + rows, :] = state
    below = 2 * plan.tile_rows + first
    places[below : below + rows, :] = base


def place():
    nx, ny = lax.axis_size("gx"), lax.axis_size("gy")
    return nx, ny, lax.axis_index("gx"), lax.axis_index("gy")


def list_slots(plan, bx, by, live):
    f32, bf16 = jnp.float32, jnp.bfloat16
    slots, width = plan.slots, plan.width
    ahead_x = jnp.where(bx >= plan.size_x - 2, live, 0.0)
    back_x = jnp.where(bx < 1, live, 0.0)
    ahead_y = jnp.where(by >= plan.size_y - 2, 1.0, 0.0)
    back_y = jnp.where(by < 1, 1.0, 0.0)
    flags = []
    for step_x, step_y in WAYS:
        flag = {1: ahead_x, -1: back_x, 0: live}[step_x]
        flags.append(flag if step_y == 0 else flag * (ahead_y if step_y > 0 else back_y))
    flag = jnp.concatenate(flags, axis=0)
    lines = 8 * slots
    r, c = (lax.broadcasted_iota(jnp.int32, (width, width), a) for a in range(2))
    upper = jnp.where(r <= c, 1.0, 0.0).astype(bf16)
    r, c = (lax.broadcasted_iota(jnp.int32, (lines, lines), a) for a in range(2))
    before = jnp.where((c < r) & (c // slots == r // slots), 1.0, 0.0).astype(bf16)
    within = jnp.dot(flag.astype(bf16), upper, preferred_element_type=f32)
    count = jnp.broadcast_to(jnp.sum(flag, axis=1, keepdims=True), (lines, width))
    earlier = jnp.dot(before, count.astype(bf16), preferred_element_type=f32)
    slot = jnp.where(flag > 0.0, earlier + within - 1.0, -1.0)
    return slot


def read_group(plan, places, table, spots, plain, sums, found, first, to):
    for j in range(GROUP):
        here = places[2 * plan.tile_rows * plan.width + first + j]
        at = first * HOP + j * HOP
        sums[9 * j : 9 * j + 8, :] = (
            table[pl.ds(here, 8), :] * spots[pl.ds(at, 8), :]
            + table[pl.ds(here + plan.outer_rows, 8), :] * spots[pl.ds(at + 8, 8), :]
        )
    for j in range(0, GROUP, 8):
        row = sums[pl.ds(9 * j, 8, stride=9), :]
        for s in range(1, 8):
            row = row + sums[pl.ds(9 * j + s, 8, stride=9), :]
        row = row * plain[pl.ds(pl.multiple_of(first + j, 8), 8), :]
        found[pl.ds(pl.multiple_of(to + j, 8), 8), :] = row


def component_sums(plan, found, count, out):
    f32, bf16 = jnp.float32, jnp.bfloat16
    width, size_y = plan.width, plan.size_y
    r = lax.broadcasted_iota(jnp.int32, (16, width), 0)
    lane = lax.broadcasted_iota(jnp.int32, (16, width), 1)
    by_part = jnp.where((lane // size_y == r) & (lane < 3 * size_y), 1.0, 0.0).astype(bf16)
    block = 2 * width
    for first in range(0, count, block):
        n = min(block, count - first)
        value = found[first : first + n, :]
        result = None
        for piece in thirds(value):
            part = lax.dot_general(
                by_part, piece.astype(bf16), (((1,), (1,)), ((), ())), preferred_element_type=f32
            )
            result = part if result is None else result + part
        out[:, first : first + n] = result[0:8]


def send_kernel(plan, *refs):
    arguments, tile_count = refs[:5], refs[5]
    (own, plain, spots, places, any_over) = refs[6:11]
    data, one_hot, lists, inbox, corners, got, note, notes, slot_map = refs[11:20]
    send_sem, recv_sem, note_send, note_recv, load_sem = refs[20:25]
    offsets, forces, base_x, base_y, base_z = refs[25:]
    loads = [
        pltpu.make_async_copy(far, near, load_sem.at[i])
        for i, (far, near) in enumerate(zip(arguments, refs[25:]))
    ]
    for load in loads:
        load.start()
    f32, bf16 = jnp.float32, jnp.bfloat16
    slots, width, markers = plan.slots, plan.width, plan.markers
    nx, ny, mx, my = place()
    devices = nx * ny
    me = mx * ny + my

    def other(i):
        to = lax.rem(me + i, devices)
        return to // ny, lax.rem(to, ny)

    barrier = pltpu.get_barrier_semaphore()

    def greet(i, carry):
        pl.semaphore_signal(barrier, inc=1, device_id=other(i), device_id_type=MESH)
        return carry

    lax.fori_loop(1, devices, greet, 0)
    for load in loads:
        load.wait()

    live = jnp.where(lax.broadcasted_iota(jnp.int32, (slots, width), 0) < tile_count[0], 1.0, 0.0)
    bx, by, bz = base_x[...], base_y[...], base_z[...]
    values = [offsets[c] for c in range(3)] + [forces[c] * live for c in range(3)]
    values = values + [bx.astype(f32), by.astype(f32), bz.astype(f32), live]
    data[10:16, :] = jnp.zeros((6, markers), f32)
    for k, value in enumerate(values):
        for t in range(slots):
            data[k : k + 1, t * width : (t + 1) * width] = value[t : t + 1, :]
    slot = list_slots(plan, bx, by, live)
    slot_map[...] = slot
    over = jnp.zeros((slots, width), f32)
    for d in range(8):
        here = slot[d * slots : (d + 1) * slots]
        over = jnp.maximum(over, jnp.where(here >= plan.caps[d], 1.0, 0.0))
    note[...] = jnp.broadcast_to(jnp.max(over), note.shape)
    fill_one_hot(plan, slot_map, one_hot)
    stack = jnp.concatenate(thirds(data[...]), axis=0).astype(bf16)
    found = lax.dot_general(
        stack, one_hot[...], (((1,), (1,)), ((), ())), preferred_element_type=f32
    )
    found = found[0:16] + found[16:32] + found[32:48]
    lane = lax.broadcasted_iota(jnp.int32, (1, plan.listed), 1)
    for row, axis, size in ((6, 0, plan.size_x), (7, 1, plan.size_y)):
        shift = jnp.zeros((1, plan.listed), f32)
        for d in range(8):
            inside = (lane >= plan.starts[d]) & (lane < plan.starts[d] + plan.caps[d])
            shift = jnp.where(inside, float(WAYS[d][axis] * size), shift)
        moved_by = jnp.where(row_mask((16, plan.listed), row), shift * found[9:10], 0.0)
        found = found - moved_by
    lists[...] = found

    pl.semaphore_wait(barrier, devices - 1)

    def word(i):
        return pltpu.make_async_remote_copy(
            src_ref=note,
            dst_ref=notes.at[i],
            send_sem=note_send.at[i],
            recv_sem=note_recv.at[i],
            device_id=other(i),
            device_id_type=MESH,
        )

    copies = []
    for d, (step_x, step_y) in enumerate(WAYS):
        start, size = plan.span(d)
        target = inbox.at[:, pl.ds(start, size)] if d < 4 else corners.at[d - 4]
        copies.append(
            pltpu.make_async_remote_copy(
                src_ref=lists.at[:, pl.ds(start, size)],
                dst_ref=target,
                send_sem=send_sem.at[d],
                recv_sem=recv_sem.at[d],
                device_id=(lax.rem(mx + step_x + nx, nx), lax.rem(my + step_y + ny, ny)),
                device_id_type=MESH,
            )
        )
        copies[-1].start()

    def tell(i, carry):
        word(i).start()
        return carry

    lax.fori_loop(1, devices, tell, 0)
    prepare(plan, data, 0, slots, OWN_BATCH, spots, own, plain, places)
    for copy in copies:
        copy.wait()

    got[:, 0 : plan.faces] = inbox[...]
    lane = lax.broadcasted_iota(jnp.int32, (16, width), 1) // plan.caps[4]
    last = corners[0]
    for i in range(1, 4):
        last = jnp.where(lane == i, corners[i], last)
    got[:, plan.faces :] = last
    prepare(plan, got, slots, plan.tiles - slots, LIST_BATCH, spots, own, plain, places)

    def hear(i, most):
        word(i).wait()
        return jnp.maximum(most, notes[i])

    any_over[0] = jnp.max(lax.fori_loop(1, devices, hear, note[...])).astype(jnp.int32)


def fill_one_hot(plan, slot_map, one_hot):
    for d in range(8):
        rows = plan.caps[d]
        index = lax.broadcasted_iota(jnp.int32, (rows, plan.width), 0).astype(jnp.float32)
        for t in range(plan.slots):
            line = slot_map[d * plan.slots + t : d * plan.slots + t + 1, :]
            hot = jnp.where(index == line, 1.0, 0.0).astype(jnp.bfloat16)
            one_hot[plan.starts[d] : plan.starts[d] + rows, t * plan.width : (t + 1) * plan.width] = hot


def main_kernel(plan, time_step, *refs):
    own, plain, spots, places, tile_count, u_in, density_in, u_out, partial, table = refs[:10]
    grid, found, sums, u_s, density_s, sems = refs[10:]
    f32, bf16 = jnp.float32, jnp.bfloat16
    width, depth, size_y, total = plan.width, plan.depth, plan.size_y, plan.total
    outer_rows, grid_rows = plan.outer_rows, plan.grid_rows
    loads = [
        pltpu.make_async_copy(u_in, u_s, sems.at[0]),
        pltpu.make_async_copy(density_in, density_s, sems.at[1]),
    ]
    for load in loads:
        load.start()
    zero = jnp.zeros((8, width), f32)
    group = divisor(4 * grid_rows // 8, 52)

    def clear(i, carry):
        for j in range(group):
            grid[pl.ds(pl.multiple_of((i * group + j) * 8, 8), 8), :] = zero
        return carry

    lax.fori_loop(0, 4 * grid_rows // 8 // group, clear, 0)
    for o in (0, 1, plan.outers - 2, plan.outers - 1):
        for g in range(2):
            at = g * grid_rows + o * outer_rows
            table[at : at + outer_rows, :] = jnp.zeros((outer_rows, width), f32)
    found[...] = jnp.zeros((plan.listed, width), f32)

    def spread_group(batch, g, carry):
        first = g * GROUP
        state = places[plan.tile_rows * width + first]

        def windows(j):
            here = places[first + j]
            at = first * HOP + j * HOP
            row = jnp.broadcast_to(own[pl.ds(first + j, 1), :], (8, width))
            one, two = pl.ds(here, 8), pl.ds(here + outer_rows, 8)
            return [
                (one, grid[one, :] + spots[pl.ds(at, 8), :] * row),
                (two, grid[two, :] + spots[pl.ds(at + 8, 8), :] * row),
            ]

        @pl.when(state == 1)
        def _():
            for j0 in range(0, GROUP, batch):
                stores = []
                for j in range(j0, j0 + batch):
                    stores = stores + windows(j)
                for where, value in stores:
                    grid[where, :] = value

        @pl.when(state > 1)
        def _():
            def single(j, c):
                for where, value in windows(j):
                    grid[where, :] = value
                return c

            lax.fori_loop(0, state - 1, single, 0)

        return carry

    live_groups = tile_count[0] * (width // GROUP)
    lists_from, all_groups = plan.markers // GROUP, total // GROUP
    lax.fori_loop(0, live_groups, functools.partial(spread_group, OWN_BATCH), 0)
    lax.fori_loop(lists_from, all_groups, functools.partial(spread_group, LIST_BATCH), 0)

    def fold(i, carry):
        at = i * outer_rows
        ends = [(2 * depth, 0, 2), (2, 2 * depth + 2, 4)]
        for to, source, rows in ends:
            grid[pl.ds(at + to, rows), :] = grid[pl.ds(at + to, rows), :] + grid[pl.ds(at + source, rows), :]
        return carry

    lax.fori_loop(0, 4 * plan.outers, fold, 0)
    for load in loads:
        load.wait()

    def lines(g, outer, side):
        return pl.ds(g * grid_rows + outer * outer_rows + 2 + side, depth, stride=2)

    def plane(p, homes):
        force = None
        for copy in range(2):
            for g, outer, side in homes:
                part = grid[lines(2 * copy + g, outer, side), :]
                force = part if force is None else force + part
        force = force.T
        scale = time_step / density_s[p]
        pieces = []
        for c in range(3):
            value = u_s[c, p] + force[c * size_y : (c + 1) * size_y] * scale
            u_s[c, p] = value
            pieces.append(value)
        if width > 3 * size_y:
            pieces.append(jnp.zeros((width - 3 * size_y, depth), f32))
        back = jnp.concatenate(pieces, axis=0).T
        for g, outer, side in homes:
            table[lines(g, outer, side), :] = back
            at = g * grid_rows + outer * outer_rows + side
            table[pl.ds(at, 1), :] = back[depth - 1 : depth]
            table[pl.ds(at + 2 * depth + 2, 1), :] = back[0:1]
            table[pl.ds(at + 2 * depth + 4, 1), :] = back[1:2]

    def pair(i, carry):
        for j in range(pairs):
            o = i * pairs + j
            plane(2 * o, [(0, o + 1, 1), (1, o + 1, 0)])
            plane(2 * o + 1, [(0, o + 2, 0), (1, o + 1, 1)])
        return carry

    pairs = divisor(plan.size_x // 2, 2)
    lax.fori_loop(0, plan.size_x // 2 // pairs, pair, 0)
    leave = pltpu.make_async_copy(u_s, u_out, sems.at[2])
    leave.start()

    def read_list(g, carry):
        first = g * GROUP

        @pl.when(places[plan.tile_rows * width + first] > 0)
        def _():
            read_group(plan, places, table, spots, plain, sums, found, first, first - plan.markers)

        return carry

    lax.fori_loop(lists_from, all_groups, read_list, 0)
    component_sums(plan, found, plan.listed, partial)
    leave.wait()


def return_kernel(plan, *refs):
    partial, plain, spots, table, base_x, base_y, places, tile_count, out = refs[:9]
    slot_map, one_hot, found, sums, velocity, inbox, corners, send_sem, recv_sem = refs[9:]
    f32, bf16 = jnp.float32, jnp.bfloat16
    width = plan.width
    nx, ny, mx, my = place()
    barrier = pltpu.get_barrier_semaphore()

    def neighbour(step_x, step_y):
        return (lax.rem(mx + step_x + nx, nx), lax.rem(my + step_y + ny, ny))

    for way in WAYS:
        pl.semaphore_signal(barrier, inc=1, device_id=neighbour(*way), device_id_type=MESH)
    pl.semaphore_wait(barrier, len(WAYS))
    copies = []
    for d, (step_x, step_y) in enumerate(WAYS):
        start, size = plan.span(d)
        target = inbox.at[:, pl.ds(start, size)] if d < 4 else corners.at[d - 4]
        copies.append(
            pltpu.make_async_remote_copy(
                src_ref=partial.at[:, pl.ds(start, size)],
                dst_ref=target,
                send_sem=send_sem.at[d],
                recv_sem=recv_sem.at[d],
                device_id=neighbour(-step_x, -step_y),
                device_id_type=MESH,
            )
        )
        copies[-1].start()

    def read(g, carry):
        first = g * GROUP
        read_group(plan, places, table, spots, plain, sums, found, first, first)
        return carry

    lax.fori_loop(0, plan.markers // GROUP, read, 0)
    component_sums(plan, found, plan.markers, velocity)
    shape = (plan.slots, width)
    live = jnp.where(lax.broadcasted_iota(jnp.int32, shape, 0) < tile_count[0], 1.0, 0.0)
    slot_map[...] = list_slots(plan, base_x[...], base_y[...], live)
    fill_one_hot(plan, slot_map, one_hot)
    for copy in copies:
        copy.wait()
    lane = lax.broadcasted_iota(jnp.int32, (8, width), 1) // plan.caps[4]
    last = corners[0]
    for i in range(1, 4):
        last = jnp.where(lane == i, corners[i], last)
    back = jnp.concatenate([inbox[...], last], axis=1)
    stack = jnp.concatenate(thirds(back) + [jnp.zeros_like(back)], axis=0).astype(bf16)
    extra = jnp.dot(stack, one_hot[...], preferred_element_type=f32)
    extra = extra[0:8] + extra[8:16] + extra[16:24]
    total = velocity[...] + extra
    live = tile_count[0]
    for t in range(plan.slots):
        row = total[:, t * width : (t + 1) * width]
        row = jnp.where(lax.broadcasted_iota(jnp.int32, row.shape, 0) * 0 + t < live, row, 0.0)
        for c in range(3):
            out[c, t : t + 1, :] = row[c : c + 1, :]


def on_device(u_old, density, offsets, forces, base_x, base_y, base_z, tile_count):
    time_step = 0.5
    _, size_x, size_y, depth = u_old.shape
    slots, width = base_x.shape
    plan = Plan(size_x, size_y, depth, slots, width)
    f32, bf16 = jnp.float32, jnp.bfloat16
    devices = lax.axis_size("gx") * lax.axis_size("gy")
    whole, scalars = pl.BlockSpec(memory_space=pltpu.VMEM), pl.BlockSpec(memory_space=pltpu.SMEM)
    far = pl.BlockSpec(memory_space=pl.ANY)
    lines = 8 * slots
    dma = pltpu.SemaphoreType.DMA
    own, plain, spots, places, over = pl.pallas_call(
        functools.partial(send_kernel, plan),
        out_shape=[
            jax.ShapeDtypeStruct((plan.total, width), f32),
            jax.ShapeDtypeStruct((plan.total, width), f32),
            jax.ShapeDtypeStruct((plan.total * HOP, width), f32),
            jax.ShapeDtypeStruct((3 * plan.tile_rows, width), jnp.int32),
            jax.ShapeDtypeStruct((1,), jnp.int32),
        ],
        in_specs=[far] * 5 + [scalars],
        out_specs=[whole] * 4 + [scalars],
        scratch_shapes=[
            pltpu.VMEM((16, plan.markers), f32),
            pltpu.VMEM((plan.listed, plan.markers), bf16),
            pltpu.VMEM((16, plan.listed), f32),
            pltpu.VMEM((16, plan.faces), f32),
            pltpu.VMEM((4, 16, width), f32),
            pltpu.VMEM((16, plan.listed), f32),
            pltpu.VMEM((8, width), f32),
            pltpu.VMEM((devices, 8, width), f32),
            pltpu.VMEM((lines, width), f32),
            dma((8,)),
            dma((8,)),
            dma((devices,)),
            dma((devices,)),
            dma((5,)),
        ]
        + [pltpu.VMEM(offsets.shape, f32)] * 2
        + [pltpu.VMEM(base_x.shape, jnp.int32)] * 3,
        compiler_params=pltpu.CompilerParams(
            vmem_limit_bytes=SEND_LIMIT, collective_id=0, has_side_effects=True
        ),
        name="send",
    )(offsets, forces, base_x, base_y, base_z, tile_count)

    def sparse(*args):
        places_line = places.reshape(-1)
        u_new, partial, table = pl.pallas_call(
            functools.partial(main_kernel, plan, time_step),
            out_shape=[
                jax.ShapeDtypeStruct(u_old.shape, f32),
                jax.ShapeDtypeStruct((8, plan.listed), f32),
                jax.ShapeDtypeStruct((2 * plan.grid_rows, width), f32),
            ],
            in_specs=[whole] * 3 + [scalars] * 2 + [far] * 2,
            out_specs=[far, whole, whole],
            scratch_shapes=[
                pltpu.VMEM((4 * plan.grid_rows, width), f32),
                pltpu.VMEM((plan.listed, width), f32),
                pltpu.VMEM((9 * GROUP, width), f32),
                pltpu.VMEM(u_old.shape, f32),
                pltpu.VMEM(density.shape, f32),
                dma((3,)),
            ],
            compiler_params=pltpu.CompilerParams(vmem_limit_bytes=MAIN_LIMIT),
            name="main",
        )(own, plain, spots, places_line, tile_count, u_old, density)
        out = pl.pallas_call(
            functools.partial(return_kernel, plan),
            out_shape=jax.ShapeDtypeStruct((3, slots, width), f32),
            in_specs=[whole] * 6 + [scalars] * 2,
            out_specs=whole,
            scratch_shapes=[
                pltpu.VMEM((lines, width), f32),
                pltpu.VMEM((plan.listed, plan.markers), bf16),
                pltpu.VMEM((plan.markers, width), f32),
                pltpu.VMEM((9 * GROUP, width), f32),
                pltpu.VMEM((8, plan.markers), f32),
                pltpu.VMEM((8, plan.faces), f32),
                pltpu.VMEM((4, 8, width), f32),
                dma((8,)),
                dma((8,)),
            ],
            compiler_params=pltpu.CompilerParams(
                vmem_limit_bytes=SEND_LIMIT, collective_id=1, has_side_effects=True
            ),
            name="give_back",
        )(partial, plain, spots, table, base_x, base_y, places_line, tile_count)
        return u_new, out

    args = (u_old, density, offsets, forces, base_x, base_y, base_z, tile_count)
    return lax.cond(over[0] > 0, dense_device, sparse, *args)


def solution(mesh):
    in_specs = (
        P(None, "gx", "gy", None),
        P("gx", "gy", None),
        P(None, ("gx", "gy"), None),
        P(None, ("gx", "gy"), None),
        P(("gx", "gy"), None),
        P(("gx", "gy"), None),
        P(("gx", "gy"), None),
        P(("gx", "gy")),
    )
    out_specs = (P(None, "gx", "gy", None), P(None, ("gx", "gy"), None))
    return jax.shard_map(
        on_device, mesh=mesh, in_specs=in_specs, out_specs=out_specs, check_vma=False
    )
```

```python
import functools

import jax
import jax.numpy as jnp
from jax import lax
from jax.experimental import pallas as pl
from jax.experimental.pallas import tpu as pltpu
from jax.sharding import PartitionSpec as P

VMEM_LIMIT = 60 * 1024 * 1024
SEND_LIMIT = 10 * 1024 * 1024
MAIN_LIMIT = 26 * 1024 * 1024


def divisor(count, most):
    return max(d for d in range(1, most + 1) if count % d == 0)


def moved(value, step_x, step_y):
    if step_y == 0:
        n = lax.axis_size("gx")
        return lax.ppermute(value, "gx", [(i, (i + step_x) % n) for i in range(n)])
    if step_x == 0:
        n = lax.axis_size("gy")
        return lax.ppermute(value, "gy", [(i, (i + step_y) % n) for i in range(n)])
    nx, ny = lax.axis_size("gx"), lax.axis_size("gy")
    pairs = [
        (i * ny + j, ((i + step_x) % nx) * ny + (j + step_y) % ny)
        for i in range(nx)
        for j in range(ny)
    ]
    return lax.ppermute(value, ("gx", "gy"), pairs)


def stencil(frac):
    root = jnp.sqrt(1.0 + 4.0 * frac - 4.0 * frac * frac)
    return [
        (3.0 - 2.0 * frac - root) / 8.0,
        (3.0 - 2.0 * frac + root) / 8.0,
        (1.0 + 2.0 * frac + root) / 8.0,
        (1.0 + 2.0 * frac - root) / 8.0,
    ]


def pick(delta, four):
    total = jnp.where(delta == 0, four[0], 0.0)
    for k in range(1, 4):
        total = jnp.where(delta == k, four[k], total)
    return total


def wrapped(delta, length):
    delta = jnp.where(delta < 0, delta + length, delta)
    return jnp.where(delta >= length, delta - length, delta)


def edge_weights(frac, base, rows, size):
    row = lax.broadcasted_iota(jnp.int32, (rows, base.shape[1]), 0)
    cell = jnp.where(row == size + 2, -1, row)
    cell = jnp.where(row > size + 2, -8, cell)
    return pick(cell - base + 1, stencil(frac))


def halves(value):
    high = value.astype(jnp.bfloat16)
    low = (value - high.astype(jnp.float32)).astype(jnp.bfloat16)
    return high, low


def edges(size):
    return (size - 1, size, size + 1), (size + 2, 0, 1)


def spread_kernel(size_x, size_y, feat, base, grid, *refs):
    slabs, (wx_s, wy_s, high_s, low_s) = refs[:8], refs[8:]
    planes, rows, depth = grid.shape[1], grid.shape[2], grid.shape[3]
    markers = feat.shape[1]
    wx_s[...] = edge_weights(feat[0:1, :], base[0:1, :], wx_s.shape[0], size_x)
    wy_s[...] = edge_weights(feat[1:2, :], base[1:2, :], rows, size_y)
    four = stencil(feat[2:3, :])
    column = jnp.concatenate(
        four + [base[2:3, :].astype(jnp.float32)] + [feat[3 + c : 4 + c, :] for c in range(3)], axis=0
    ).T
    cut = 256 if markers % 256 == 0 else 128
    for start in range(0, markers, cut):
        part = column[start : start + cut]
        lane = lax.broadcasted_iota(jnp.int32, (cut, depth), 1)
        delta = wrapped(lane - part[:, 4:5].astype(jnp.int32) + 1, depth)
        wz = pick(delta, [part[:, k : k + 1] for k in range(4)])
        for c in range(3):
            high, low = halves(wz * part[:, 5 + c : 6 + c])
            high_s[start : start + cut, c * depth : (c + 1) * depth] = high
            low_s[start : start + cut, c * depth : (c + 1) * depth] = low
    group = divisor(planes, 8)

    def turn(g, carry):
        first = g * group
        left = jnp.concatenate(
            [wy_s[...] * wx_s[pl.ds(first + j, 1), :] for j in range(group)], axis=0
        )
        high, low = halves(left)
        dot = functools.partial(jnp.dot, preferred_element_type=jnp.float32)
        total = dot(high, high_s[...]) + dot(low, high_s[...]) + dot(high, low_s[...])
        for j in range(group):
            for c in range(3):
                grid[c, first + j] = total[j * rows : (j + 1) * rows, c * depth : (c + 1) * depth]
        return carry

    lax.fori_loop(0, planes // group, turn, 0)
    sides_x, sides_y = edges(size_x), edges(size_y)
    for side in range(2):
        for c in range(3):
            for j, p in enumerate(sides_x[side]):
                slabs[side][c, j] = grid[c, p]
                for other in range(2):
                    for i, r in enumerate(sides_y[other]):
                        slabs[4 + 2 * side + other][c, j, i : i + 1] = grid[c, p, r : r + 1]
            for i, r in enumerate(sides_y[side]):
                for p in range(planes):
                    slabs[2 + side][c, i, p : p + 1] = grid[c, p, r : r + 1]


def read_kernel(size_x, size_y, time_step, *refs):
    feat, base, grid, u_old, density, low_x, high_x, low_y, high_y = refs[:9]
    slabs, (u_new, velocity) = refs[9:17], refs[17:19]
    total, wx_s, wy_s, wz3, table = refs[19:]
    planes, rows, depth = grid.shape[1], grid.shape[2], grid.shape[3]
    markers = feat.shape[1]
    wx_s[...] = edge_weights(feat[0:1, :], base[0:1, :], wx_s.shape[0], size_x)
    wy_s[...] = edge_weights(feat[1:2, :], base[1:2, :], rows, size_y)
    cut = 256 if markers % 256 == 0 else 128
    for start in range(0, markers, cut):
        at = slice(start, start + cut)
        row = lax.broadcasted_iota(jnp.int32, (depth, cut), 0)
        delta = wrapped(row - base[2:3, at] + 1, depth)
        high, low = halves(pick(delta, stencil(feat[2:3, at])))
        wz3[0:depth, at] = high
        wz3[depth : 2 * depth, at] = high
        wz3[2 * depth :, at] = low
    total[...] = grid[...]
    near_x, near_y = edges(size_x)[::-1], edges(size_y)[::-1]
    for side in range(2):
        for c in range(3):
            for j, p in enumerate(near_x[side]):
                total[c, p] = total[c, p] + slabs[side][c, j]
                for other in range(2):
                    for i, r in enumerate(near_y[other]):
                        total[c, p, r : r + 1] = (
                            total[c, p, r : r + 1] + slabs[4 + 2 * side + other][c, j, i : i + 1]
                        )
            for i, r in enumerate(near_y[side]):
                for p in range(planes):
                    total[c, p, r : r + 1] = total[c, p, r : r + 1] + slabs[2 + side][c, i, p : p + 1]
    group = divisor(planes, 6)
    spare = jnp.ones((rows - size_y - 3, depth), jnp.float32)

    def plane_state(k, p):
        if p < size_x:
            main = density[p] if k == 3 else u_old[k, p]
        elif p < size_x + 2:
            main = high_x[k, p - size_x]
        else:
            main = low_x[k, 0]
        edge = [high_y[k, 0, p : p + 1], high_y[k, 1, p : p + 1], low_y[k, 0, p : p + 1], spare]
        return jnp.concatenate([main] + edge, axis=0)

    for g in range(planes // group):
        pieces = []
        for p in range(g * group, (g + 1) * group):
            scale = time_step / plane_state(3, p)
            for c in range(3):
                value = plane_state(c, p) + total[c, p] * scale
                if p < size_x:
                    u_new[c, p] = value[:size_y]
                pieces.append(value)
        high, low = halves(jnp.concatenate(pieces, axis=0))
        table[g, :, 0:depth] = high
        table[g, :, depth : 2 * depth] = low
        table[g, :, 2 * depth :] = high

    def turn(step, carry):
        at = pl.ds(pl.multiple_of(step * cut, cut), cut)
        right = wz3[:, at]
        wy = wy_s[:, at]
        sums = [jnp.zeros((8, cut), jnp.float32) for _ in range(3)]
        for g in range(planes // group):
            found = jnp.dot(table[g], right, preferred_element_type=jnp.float32)
            for j in range(group):
                p = g * group + j
                weight = wy * wx_s[p : p + 1, at]
                for c in range(3):
                    first = (j * 3 + c) * rows
                    product = found[first : first + rows] * weight
                    for r in range(0, rows, 8):
                        sums[c] = sums[c] + product[r : r + 8]
        velocity[:, at] = (
            jnp.concatenate([jnp.sum(s, axis=0, keepdims=True) for s in sums], axis=0) * feat[6:7, at]
        )
        return carry

    lax.fori_loop(0, markers // cut, turn, 0)


def dense_device(u_old, density, offsets, forces, base_x, base_y, base_z, tile_count):
    time_step = 0.5
    _, size_x, size_y, depth = u_old.shape
    slots, width = base_x.shape
    markers = slots * width
    planes = size_x + 3
    rows = -(-(size_y + 3) // 8) * 8
    lines = -(-planes // 8) * 8
    f32, bf16 = jnp.float32, jnp.bfloat16
    live = (lax.broadcasted_iota(jnp.int32, (slots, width), 0) < tile_count[0]).astype(f32)
    feat = jnp.concatenate([offsets, forces * live[None], live[None]], axis=0).reshape(7, markers)
    base = jnp.stack([base_x, base_y, base_z], axis=0).reshape(3, markers)

    up = jnp.concatenate([u_old[:, size_x - 1 :], density[None, size_x - 1 :]], axis=0)
    down = jnp.concatenate([u_old[:, :2], density[None, :2]], axis=0)
    low_x, high_x = moved(up, 1, 0), moved(down, -1, 0)

    def strip(r):
        inner = jnp.concatenate([u_old[:, :, r], density[None, :, r]], axis=0)
        return jnp.concatenate([inner, high_x[:, :, r], low_x[:, :, r]], axis=1)

    low_y = moved(strip(size_y - 1)[:, None], 0, 1)
    high_y = moved(jnp.stack([strip(0), strip(1)], axis=1), 0, -1)

    params = pltpu.CompilerParams(vmem_limit_bytes=VMEM_LIMIT)
    slab_x = jax.ShapeDtypeStruct((3, 3, rows, depth), f32)
    slab_y = jax.ShapeDtypeStruct((3, 3, planes, depth), f32)
    corner = jax.ShapeDtypeStruct((3, 3, 3, depth), f32)
    whole = pl.BlockSpec(memory_space=pltpu.VMEM)
    flops = 6 * planes * rows * 3 * depth * markers
    cost = pl.CostEstimate(flops=flops, transcendentals=0, bytes_accessed=8 * planes * rows * depth)
    grid, *slabs = pl.pallas_call(
        functools.partial(spread_kernel, size_x, size_y),
        out_shape=[jax.ShapeDtypeStruct((3, planes, rows, depth), f32)]
        + [slab_x] * 2
        + [slab_y] * 2
        + [corner] * 4,
        in_specs=[whole] * 2,
        out_specs=[whole] * 9,
        scratch_shapes=[
            pltpu.VMEM((lines, markers), f32),
            pltpu.VMEM((rows, markers), f32),
            pltpu.VMEM((markers, 3 * depth), bf16),
            pltpu.VMEM((markers, 3 * depth), bf16),
        ],
        compiler_params=params,
        cost_estimate=cost,
        name="spread",
    )(feat, base)
    ways = [(1, 0), (-1, 0), (0, 1), (0, -1), (1, 1), (1, -1), (-1, 1), (-1, -1)]
    slabs = [moved(slab, *way) for slab, way in zip(slabs, ways)]
    group = divisor(planes, 6)
    u_new, velocity = pl.pallas_call(
        functools.partial(read_kernel, size_x, size_y, time_step),
        out_shape=[
            jax.ShapeDtypeStruct(u_old.shape, f32),
            jax.ShapeDtypeStruct((3, markers), f32),
        ],
        in_specs=[whole] * 17,
        out_specs=[whole] * 2,
        scratch_shapes=[
            pltpu.VMEM((3, planes, rows, depth), f32),
            pltpu.VMEM((lines, markers), f32),
            pltpu.VMEM((rows, markers), f32),
            pltpu.VMEM((3 * depth, markers), bf16),
            pltpu.VMEM((planes // group, group * 3 * rows, 3 * depth), bf16),
        ],
        compiler_params=params,
        cost_estimate=cost,
        name="read",
    )(feat, base, grid, u_old, density, low_x, high_x, low_y, high_y, *slabs)
    return (u_new, velocity.reshape(3, slots, width))


MESH = pl.DeviceIdType.MESH
WAYS = [(1, 0), (-1, 0), (0, 1), (0, -1), (1, 1), (1, -1), (-1, 1), (-1, -1)]
OWN_BATCH, LIST_BATCH = 8, 8
GROUP = 64
HOP = 17


def thirds(value):
    high = value.astype(jnp.bfloat16).astype(jnp.float32)
    rest = value - high
    middle = rest.astype(jnp.bfloat16).astype(jnp.float32)
    return [high, middle, rest - middle]


class Plan:
    def __init__(self, size_x, size_y, depth, slots, width):
        self.size_x, self.size_y, self.depth = size_x, size_y, depth
        self.slots, self.width = slots, width
        self.markers = slots * width

        def cap(reach, size):
            return -(-2 * reach * self.markers // size // width) * width

        corner = width // 4
        self.caps = [cap(2, size_x), cap(1, size_x), cap(2, size_y), cap(1, size_y)] + [corner] * 4
        self.starts = [sum(self.caps[:d]) for d in range(8)]
        self.listed = sum(self.caps)
        self.faces = self.starts[4]
        self.tiles = slots + self.listed // width
        self.total = self.tiles * width
        self.tile_rows = -(-self.tiles // 8) * 8
        self.outers = (size_x + 2) // 2 + 2
        self.outer_rows = 2 * (depth + 4)
        self.grid_rows = self.outers * self.outer_rows

    def span(self, d):
        if d < 4:
            return self.starts[d], self.caps[d]
        return self.faces, self.width


def row_mask(shape, value):
    return lax.broadcasted_iota(jnp.int32, shape, 0) == value


def prepare(plan, data, first, count, batch, spots, own, plain, places):
    width, size_y = plan.width, plan.size_y
    f32, bf16 = jnp.float32, jnp.bfloat16
    k_row = lax.broadcasted_iota(jnp.int32, (32, 6 * width), 0)
    n_lane = lax.broadcasted_iota(jnp.int32, (32, 6 * width), 1)
    kind = k_row % 8
    part, inside = n_lane // width, n_lane % width
    hit = ((kind < 5) & (part == kind)) | ((kind > 4) & (part == 5) & (inside // size_y == kind - 5))
    select = jnp.where(hit & (k_row < 24), 1.0, 0.0).astype(bf16)
    k_row = lax.broadcasted_iota(jnp.int32, (32, 8 * width), 0)
    n_lane = lax.broadcasted_iota(jnp.int32, (32, 8 * width), 1)
    hit = (k_row % 8 == n_lane // width) & (k_row < 24)
    spread_out = jnp.where(hit, 1.0, 0.0).astype(bf16)
    step = 4
    for t0 in range(0, count, step):
        n = min(step, count - t0) * width
        d = data[:, t0 * width : t0 * width + n]
        at = slice((first + t0) * width, (first + t0) * width + n)
        rows = lax.broadcasted_iota(jnp.int32, (8, n), 0)
        w = stencil(jnp.where(rows < 3, d[0:8], 0.5))
        factors = jnp.concatenate([v[2:3] for v in w] + [v[0:1] for v in w], axis=0)
        stack = jnp.concatenate(thirds(factors) + [jnp.zeros((8, n), f32)], axis=0)
        left = stack.T.astype(bf16)
        base = (first + t0) * width * HOP
        x = [
            jnp.dot(left, spread_out[:, i * width : (i + 2) * width], preferred_element_type=f32)
            for i in (4, 6)
        ]
        x = [x[i // 2][:, (i % 2) * width : (i % 2 + 1) * width] for i in range(4)]
        for i in range(0, 4, 2):
            z = jnp.dot(left, spread_out[:, i * width : (i + 2) * width], preferred_element_type=f32)
            for j in range(2):
                for h in range(2):
                    for side in range(2):
                        row = base + 8 * h + 2 * (i + j) + side
                        value = z[:, j * width : (j + 1) * width] * x[2 * h + side]
                        spots[pl.ds(row, n, stride=HOP), :] = value
        block = jnp.concatenate([v[1:2] for v in w] + [d[7:8], d[3:6]], axis=0)
        stack = jnp.concatenate(thirds(block) + [jnp.zeros((8, n), f32)], axis=0).astype(bf16)
        wide = lax.dot_general(
            stack, select, (((0,), (0,)), ((), ())), preferred_element_type=f32
        )
        cols = [wide[:, i * width : (i + 1) * width] for i in range(6)]
        lane = lax.broadcasted_iota(jnp.int32, (n, width), 1)
        y = jnp.where(lane < 3 * size_y, lane % size_y, -1000).astype(f32)
        pattern = pick(y - cols[4] + 1.0, cols[:4])
        plain[at, :] = pattern
        own[at, :] = pattern * cols[5]
    keys, zs, bases, goods = [], [], [], []
    for t in range(count):
        at = slice(t * width, (t + 1) * width)
        bx = data[6:7, at].astype(jnp.int32)
        bz = data[8:9, at].astype(jnp.int32)
        good = data[9:10, at] > 0.0
        lane = lax.broadcasted_iota(jnp.int32, (1, width), 1)
        step_in = lane % batch
        across = bx + 2
        side, outer = across % 2, across // 2
        spare = plan.grid_rows + ((plan.size_x + 2) // 2) * plan.outer_rows + 8 * step_in
        base = side * plan.grid_rows + outer * plan.outer_rows + 2 * bz
        bases.append(jnp.where(good, base, spare))
        keys.append(jnp.where(good, side * (plan.outers + 8) + outer, -100 - 10 * step_in))
        zs.append(bz)
        goods.append(jnp.where(good, 1, 0))
    rows = -(-count // 8) * 8
    fill = [jnp.zeros((rows - count, width), jnp.int32)] if rows > count else []
    key, z = jnp.concatenate(keys + fill, axis=0), jnp.concatenate(zs + fill, axis=0)
    base = jnp.concatenate(bases + fill, axis=0)
    lane = lax.broadcasted_iota(jnp.int32, (rows, width), 1) % batch

    def near(a, b, most):
        return (a - b <= most) & (b - a <= most)

    clashes = [
        (lane >= d) & near(key, pltpu.roll(key, d, 1), 1) & near(z, pltpu.roll(z, d, 1), 3)
        for d in range(1, batch)
    ]
    second = clashes[0]
    for clash in clashes[1:]:
        second = second | clash
    second = jnp.where(second, 1, 0)
    bad = jnp.zeros((rows, width), jnp.int32)
    for d, clash in enumerate(clashes):
        both = second * pltpu.roll(second, d + 1, 1)
        bad = jnp.maximum(bad, jnp.where(clash, both, 0))
    places[first : first + rows, :] = base + second * (2 * plan.grid_rows)
    good = jnp.concatenate(goods + fill, axis=0)
    lane = lax.broadcasted_iota(jnp.int32, (rows, width), 1) // GROUP
    state = jnp.zeros((rows, width), jnp.int32)
    for h in range(width // GROUP):
        here = lane == h
        worst = jnp.max(jnp.where(here, bad, 0), axis=1, keepdims=True)
        some = jnp.max(jnp.where(here, good, 0), axis=1, keepdims=True)
        filled = jnp.sum(jnp.where(here, good, 0), axis=1, keepdims=True)
        state = jnp.where(here, some * (1 + worst * filled), state)
    below = plan.tile_rows + first
    places[below : below + rows, :] = state
    below = 2 * plan.tile_rows + first
    places[below : below + rows, :] = base


def place():
    nx, ny = lax.axis_size("gx"), lax.axis_size("gy")
    return nx, ny, lax.axis_index("gx"), lax.axis_index("gy")


def list_slots(plan, bx, by, live):
    f32, bf16 = jnp.float32, jnp.bfloat16
    slots, width = plan.slots, plan.width
    ahead_x = jnp.where(bx >= plan.size_x - 2, live, 0.0)
    back_x = jnp.where(bx < 1, live, 0.0)
    ahead_y = jnp.where(by >= plan.size_y - 2, 1.0, 0.0)
    back_y = jnp.where(by < 1, 1.0, 0.0)
    flags = []
    for step_x, step_y in WAYS:
        flag = {1: ahead_x, -1: back_x, 0: live}[step_x]
        flags.append(flag if step_y == 0 else flag * (ahead_y if step_y > 0 else back_y))
    flag = jnp.concatenate(flags, axis=0)
    lines = 8 * slots
    r, c = (lax.broadcasted_iota(jnp.int32, (width, width), a) for a in range(2))
    upper = jnp.where(r <= c, 1.0, 0.0).astype(bf16)
    r, c = (lax.broadcasted_iota(jnp.int32, (lines, lines), a) for a in range(2))
    before = jnp.where((c < r) & (c // slots == r // slots), 1.0, 0.0).astype(bf16)
    within = jnp.dot(flag.astype(bf16), upper, preferred_element_type=f32)
    count = jnp.broadcast_to(jnp.sum(flag, axis=1, keepdims=True), (lines, width))
    earlier = jnp.dot(before, count.astype(bf16), preferred_element_type=f32)
    slot = jnp.where(flag > 0.0, earlier + within - 1.0, -1.0)
    return slot


def read_group(plan, places, table, spots, plain, sums, found, first, to):
    for j in range(GROUP):
        here = places[2 * plan.tile_rows * plan.width + first + j]
        at = first * HOP + j * HOP
        sums[9 * j : 9 * j + 8, :] = (
            table[pl.ds(here, 8), :] * spots[pl.ds(at, 8), :]
            + table[pl.ds(here + plan.outer_rows, 8), :] * spots[pl.ds(at + 8, 8), :]
        )
    for j in range(0, GROUP, 8):
        row = sums[pl.ds(9 * j, 8, stride=9), :]
        for s in range(1, 8):
            row = row + sums[pl.ds(9 * j + s, 8, stride=9), :]
        row = row * plain[pl.ds(pl.multiple_of(first + j, 8), 8), :]
        found[pl.ds(pl.multiple_of(to + j, 8), 8), :] = row


def component_sums(plan, found, count, out):
    f32, bf16 = jnp.float32, jnp.bfloat16
    width, size_y = plan.width, plan.size_y
    r = lax.broadcasted_iota(jnp.int32, (16, width), 0)
    lane = lax.broadcasted_iota(jnp.int32, (16, width), 1)
    by_part = jnp.where((lane // size_y == r) & (lane < 3 * size_y), 1.0, 0.0).astype(bf16)
    block = 2 * width
    for first in range(0, count, block):
        n = min(block, count - first)
        value = found[first : first + n, :]
        result = None
        for piece in thirds(value):
            part = lax.dot_general(
                by_part, piece.astype(bf16), (((1,), (1,)), ((), ())), preferred_element_type=f32
            )
            result = part if result is None else result + part
        out[:, first : first + n] = result[0:8]


def send_kernel(plan, *refs):
    arguments, tile_count = refs[:5], refs[5]
    (own, plain, spots, places, any_over) = refs[6:11]
    data, one_hot, lists, inbox, corners, got, note, notes, slot_map = refs[11:20]
    send_sem, recv_sem, note_send, note_recv, load_sem = refs[20:25]
    offsets, forces, base_x, base_y, base_z = refs[25:]
    loads = [
        pltpu.make_async_copy(far, near, load_sem.at[i])
        for i, (far, near) in enumerate(zip(arguments, refs[25:]))
    ]
    for load in loads:
        load.start()
    f32, bf16 = jnp.float32, jnp.bfloat16
    slots, width, markers = plan.slots, plan.width, plan.markers
    nx, ny, mx, my = place()
    devices = nx * ny
    me = mx * ny + my

    def other(i):
        to = lax.rem(me + i, devices)
        return to // ny, lax.rem(to, ny)

    barrier = pltpu.get_barrier_semaphore()

    def greet(i, carry):
        pl.semaphore_signal(barrier, inc=1, device_id=other(i), device_id_type=MESH)
        return carry

    lax.fori_loop(1, devices, greet, 0)
    for load in loads:
        load.wait()

    live = jnp.where(lax.broadcasted_iota(jnp.int32, (slots, width), 0) < tile_count[0], 1.0, 0.0)
    bx, by, bz = base_x[...], base_y[...], base_z[...]
    values = [offsets[c] for c in range(3)] + [forces[c] * live for c in range(3)]
    values = values + [bx.astype(f32), by.astype(f32), bz.astype(f32), live]
    data[10:16, :] = jnp.zeros((6, markers), f32)
    for k, value in enumerate(values):
        for t in range(slots):
            data[k : k + 1, t * width : (t + 1) * width] = value[t : t + 1, :]
    slot = list_slots(plan, bx, by, live)
    slot_map[...] = slot
    over = jnp.zeros((slots, width), f32)
    for d in range(8):
        here = slot[d * slots : (d + 1) * slots]
        over = jnp.maximum(over, jnp.where(here >= plan.caps[d], 1.0, 0.0))
    note[...] = jnp.broadcast_to(jnp.max(over), note.shape)
    fill_one_hot(plan, slot_map, one_hot)
    stack = jnp.concatenate(thirds(data[...]), axis=0).astype(bf16)
    found = lax.dot_general(
        stack, one_hot[...], (((1,), (1,)), ((), ())), preferred_element_type=f32
    )
    found = found[0:16] + found[16:32] + found[32:48]
    lane = lax.broadcasted_iota(jnp.int32, (1, plan.listed), 1)
    for row, axis, size in ((6, 0, plan.size_x), (7, 1, plan.size_y)):
        shift = jnp.zeros((1, plan.listed), f32)
        for d in range(8):
            inside = (lane >= plan.starts[d]) & (lane < plan.starts[d] + plan.caps[d])
            shift = jnp.where(inside, float(WAYS[d][axis] * size), shift)
        moved_by = jnp.where(row_mask((16, plan.listed), row), shift * found[9:10], 0.0)
        found = found - moved_by
    lists[...] = found

    pl.semaphore_wait(barrier, devices - 1)

    def word(i):
        return pltpu.make_async_remote_copy(
            src_ref=note,
            dst_ref=notes.at[i],
            send_sem=note_send.at[i],
            recv_sem=note_recv.at[i],
            device_id=other(i),
            device_id_type=MESH,
        )

    copies = []
    for d, (step_x, step_y) in enumerate(WAYS):
        start, size = plan.span(d)
        target = inbox.at[:, pl.ds(start, size)] if d < 4 else corners.at[d - 4]
        copies.append(
            pltpu.make_async_remote_copy(
                src_ref=lists.at[:, pl.ds(start, size)],
                dst_ref=target,
                send_sem=send_sem.at[d],
                recv_sem=recv_sem.at[d],
                device_id=(lax.rem(mx + step_x + nx, nx), lax.rem(my + step_y + ny, ny)),
                device_id_type=MESH,
            )
        )
        copies[-1].start()

    def tell(i, carry):
        word(i).start()
        return carry

    lax.fori_loop(1, devices, tell, 0)
    prepare(plan, data, 0, slots, OWN_BATCH, spots, own, plain, places)
    for copy in copies:
        copy.wait()

    got[:, 0 : plan.faces] = inbox[...]
    lane = lax.broadcasted_iota(jnp.int32, (16, width), 1) // plan.caps[4]
    last = corners[0]
    for i in range(1, 4):
        last = jnp.where(lane == i, corners[i], last)
    got[:, plan.faces :] = last
    prepare(plan, got, slots, plan.tiles - slots, LIST_BATCH, spots, own, plain, places)

    def hear(i, most):
        word(i).wait()
        return jnp.maximum(most, notes[i])

    any_over[0] = jnp.max(lax.fori_loop(1, devices, hear, note[...])).astype(jnp.int32)


def fill_one_hot(plan, slot_map, one_hot):
    for d in range(8):
        rows = plan.caps[d]
        index = lax.broadcasted_iota(jnp.int32, (rows, plan.width), 0).astype(jnp.float32)
        for t in range(plan.slots):
            line = slot_map[d * plan.slots + t : d * plan.slots + t + 1, :]
            hot = jnp.where(index == line, 1.0, 0.0).astype(jnp.bfloat16)
            one_hot[plan.starts[d] : plan.starts[d] + rows, t * plan.width : (t + 1) * plan.width] = hot


def main_kernel(plan, time_step, *refs):
    own, plain, spots, places, tile_count, u_in, density_in, u_out, partial, table = refs[:10]
    grid, found, sums, u_s, density_s, sems = refs[10:]
    f32, bf16 = jnp.float32, jnp.bfloat16
    width, depth, size_y, total = plan.width, plan.depth, plan.size_y, plan.total
    outer_rows, grid_rows = plan.outer_rows, plan.grid_rows
    loads = [
        pltpu.make_async_copy(u_in, u_s, sems.at[0]),
        pltpu.make_async_copy(density_in, density_s, sems.at[1]),
    ]
    for load in loads:
        load.start()
    zero = jnp.zeros((8, width), f32)

    def clear(i, carry):
        for g in range(4):
            at = g * grid_rows + i * outer_rows
            for j in range(0, outer_rows, 8):
                grid[pl.ds(pl.multiple_of(at + j, 8), 8), :] = zero
        return carry

    lax.fori_loop(1, plan.outers - 1, clear, 0)
    for o in (0, 1, plan.outers - 2, plan.outers - 1):
        for g in range(2):
            at = g * grid_rows + o * outer_rows
            table[at : at + outer_rows, :] = jnp.zeros((outer_rows, width), f32)
    found[...] = jnp.zeros((plan.listed, width), f32)

    def spread_group(batch, g, carry):
        first = g * GROUP
        state = places[plan.tile_rows * width + first]

        def windows(j):
            here = places[first + j]
            at = first * HOP + j * HOP
            row = jnp.broadcast_to(own[pl.ds(first + j, 1), :], (8, width))
            one, two = pl.ds(here, 8), pl.ds(here + outer_rows, 8)
            return [
                (one, grid[one, :] + spots[pl.ds(at, 8), :] * row),
                (two, grid[two, :] + spots[pl.ds(at + 8, 8), :] * row),
            ]

        @pl.when(state == 1)
        def _():
            for j0 in range(0, GROUP, batch):
                stores = []
                for j in range(j0, j0 + batch):
                    stores = stores + windows(j)
                for where, value in stores:
                    grid[where, :] = value

        @pl.when(state > 1)
        def _():
            def single(j, c):
                for where, value in windows(j):
                    grid[where, :] = value
                return c

            lax.fori_loop(0, state - 1, single, 0)

        return carry

    live_groups = tile_count[0] * (width // GROUP)
    lists_from, all_groups = plan.markers // GROUP, total // GROUP
    lax.fori_loop(0, live_groups, functools.partial(spread_group, OWN_BATCH), 0)
    lax.fori_loop(lists_from, all_groups, functools.partial(spread_group, LIST_BATCH), 0)

    def fold(i, carry):
        stores = []
        for g in range(4):
            at = g * grid_rows + i * outer_rows
            for to, source, rows in [(2 * depth, 0, 2), (2, 2 * depth + 2, 4)]:
                here = pl.ds(at + to, rows)
                stores.append((here, grid[here, :] + grid[pl.ds(at + source, rows), :]))
        for where, value in stores:
            grid[where, :] = value
        return carry

    lax.fori_loop(1, plan.outers - 1, fold, 0)
    for load in loads:
        load.wait()

    def lines(g, outer, side):
        return pl.ds(g * grid_rows + outer * outer_rows + 2 + side, depth, stride=2)

    def plane(p, homes):
        force = None
        for copy in range(2):
            for g, outer, side in homes:
                part = grid[lines(2 * copy + g, outer, side), :]
                force = part if force is None else force + part
        force = force.T
        scale = time_step / density_s[p]
        pieces = []
        for c in range(3):
            value = u_s[c, p] + force[c * size_y : (c + 1) * size_y] * scale
            u_s[c, p] = value
            pieces.append(value)
        if width > 3 * size_y:
            pieces.append(jnp.zeros((width - 3 * size_y, depth), f32))
        back = jnp.concatenate(pieces, axis=0).T
        for g, outer, side in homes:
            table[lines(g, outer, side), :] = back
            at = g * grid_rows + outer * outer_rows + side
            table[pl.ds(at, 1), :] = back[depth - 1 : depth]
            table[pl.ds(at + 2 * depth + 2, 1), :] = back[0:1]
            table[pl.ds(at + 2 * depth + 4, 1), :] = back[1:2]

    def pair(i, carry):
        for j in range(pairs):
            o = i * pairs + j
            plane(2 * o, [(0, o + 1, 1), (1, o + 1, 0)])
            plane(2 * o + 1, [(0, o + 2, 0), (1, o + 1, 1)])
        return carry

    pairs = divisor(plan.size_x // 2, 2)
    lax.fori_loop(0, plan.size_x // 2 // pairs, pair, 0)
    leave = pltpu.make_async_copy(u_s, u_out, sems.at[2])
    leave.start()

    def read_list(g, carry):
        first = g * GROUP

        @pl.when(places[plan.tile_rows * width + first] > 0)
        def _():
            read_group(plan, places, table, spots, plain, sums, found, first, first - plan.markers)

        return carry

    lax.fori_loop(lists_from, all_groups, read_list, 0)
    component_sums(plan, found, plan.listed, partial)
    leave.wait()


def return_kernel(plan, *refs):
    partial, plain, spots, table, base_x, base_y, places, tile_count, out = refs[:9]
    slot_map, one_hot, found, sums, velocity, inbox, corners, send_sem, recv_sem = refs[9:]
    f32, bf16 = jnp.float32, jnp.bfloat16
    width = plan.width
    nx, ny, mx, my = place()
    barrier = pltpu.get_barrier_semaphore()

    def neighbour(step_x, step_y):
        return (lax.rem(mx + step_x + nx, nx), lax.rem(my + step_y + ny, ny))

    for way in WAYS:
        pl.semaphore_signal(barrier, inc=1, device_id=neighbour(*way), device_id_type=MESH)
    pl.semaphore_wait(barrier, len(WAYS))
    copies = []
    for d, (step_x, step_y) in enumerate(WAYS):
        start, size = plan.span(d)
        target = inbox.at[:, pl.ds(start, size)] if d < 4 else corners.at[d - 4]
        copies.append(
            pltpu.make_async_remote_copy(
                src_ref=partial.at[:, pl.ds(start, size)],
                dst_ref=target,
                send_sem=send_sem.at[d],
                recv_sem=recv_sem.at[d],
                device_id=neighbour(-step_x, -step_y),
                device_id_type=MESH,
            )
        )
        copies[-1].start()

    def read(g, carry):
        first = g * GROUP
        read_group(plan, places, table, spots, plain, sums, found, first, first)
        return carry

    lax.fori_loop(0, plan.markers // GROUP, read, 0)
    component_sums(plan, found, plan.markers, velocity)
    shape = (plan.slots, width)
    live = jnp.where(lax.broadcasted_iota(jnp.int32, shape, 0) < tile_count[0], 1.0, 0.0)
    slot_map[...] = list_slots(plan, base_x[...], base_y[...], live)
    fill_one_hot(plan, slot_map, one_hot)
    for copy in copies:
        copy.wait()
    lane = lax.broadcasted_iota(jnp.int32, (8, width), 1) // plan.caps[4]
    last = corners[0]
    for i in range(1, 4):
        last = jnp.where(lane == i, corners[i], last)
    back = jnp.concatenate([inbox[...], last], axis=1)
    stack = jnp.concatenate(thirds(back) + [jnp.zeros_like(back)], axis=0).astype(bf16)
    extra = jnp.dot(stack, one_hot[...], preferred_element_type=f32)
    extra = extra[0:8] + extra[8:16] + extra[16:24]
    total = velocity[...] + extra
    live = tile_count[0]
    for t in range(plan.slots):
        row = total[:, t * width : (t + 1) * width]
        row = jnp.where(lax.broadcasted_iota(jnp.int32, row.shape, 0) * 0 + t < live, row, 0.0)
        for c in range(3):
            out[c, t : t + 1, :] = row[c : c + 1, :]


def on_device(u_old, density, offsets, forces, base_x, base_y, base_z, tile_count):
    time_step = 0.5
    _, size_x, size_y, depth = u_old.shape
    slots, width = base_x.shape
    plan = Plan(size_x, size_y, depth, slots, width)
    f32, bf16 = jnp.float32, jnp.bfloat16
    devices = lax.axis_size("gx") * lax.axis_size("gy")
    whole, scalars = pl.BlockSpec(memory_space=pltpu.VMEM), pl.BlockSpec(memory_space=pltpu.SMEM)
    far = pl.BlockSpec(memory_space=pl.ANY)
    lines = 8 * slots
    dma = pltpu.SemaphoreType.DMA
    own, plain, spots, places, over = pl.pallas_call(
        functools.partial(send_kernel, plan),
        out_shape=[
            jax.ShapeDtypeStruct((plan.total, width), f32),
            jax.ShapeDtypeStruct((plan.total, width), f32),
            jax.ShapeDtypeStruct((plan.total * HOP, width), f32),
            jax.ShapeDtypeStruct((3 * plan.tile_rows, width), jnp.int32),
            jax.ShapeDtypeStruct((1,), jnp.int32),
        ],
        in_specs=[far] * 5 + [scalars],
        out_specs=[whole] * 4 + [scalars],
        scratch_shapes=[
            pltpu.VMEM((16, plan.markers), f32),
            pltpu.VMEM((plan.listed, plan.markers), bf16),
            pltpu.VMEM((16, plan.listed), f32),
            pltpu.VMEM((16, plan.faces), f32),
            pltpu.VMEM((4, 16, width), f32),
            pltpu.VMEM((16, plan.listed), f32),
            pltpu.VMEM((1, width), f32),
            pltpu.VMEM((devices, 1, width), f32),
            pltpu.VMEM((lines, width), f32),
            dma((8,)),
            dma((8,)),
            dma((devices,)),
            dma((devices,)),
            dma((5,)),
        ]
        + [pltpu.VMEM(offsets.shape, f32)] * 2
        + [pltpu.VMEM(base_x.shape, jnp.int32)] * 3,
        compiler_params=pltpu.CompilerParams(
            vmem_limit_bytes=SEND_LIMIT, collective_id=0, has_side_effects=True
        ),
        name="send",
    )(offsets, forces, base_x, base_y, base_z, tile_count)

    def sparse(*args):
        places_line = places.reshape(-1)
        u_new, partial, table = pl.pallas_call(
            functools.partial(main_kernel, plan, time_step),
            out_shape=[
                jax.ShapeDtypeStruct(u_old.shape, f32),
                jax.ShapeDtypeStruct((8, plan.listed), f32),
                jax.ShapeDtypeStruct((2 * plan.grid_rows, width), f32),
            ],
            in_specs=[whole] * 3 + [scalars] * 2 + [far] * 2,
            out_specs=[far, whole, whole],
            scratch_shapes=[
                pltpu.VMEM((4 * plan.grid_rows, width), f32),
                pltpu.VMEM((plan.listed, width), f32),
                pltpu.VMEM((9 * GROUP, width), f32),
                pltpu.VMEM(u_old.shape, f32),
                pltpu.VMEM(density.shape, f32),
                dma((3,)),
            ],
            compiler_params=pltpu.CompilerParams(vmem_limit_bytes=MAIN_LIMIT),
            name="main",
        )(own, plain, spots, places_line, tile_count, u_old, density)
        out = pl.pallas_call(
            functools.partial(return_kernel, plan),
            out_shape=jax.ShapeDtypeStruct((3, slots, width), f32),
            in_specs=[whole] * 6 + [scalars] * 2,
            out_specs=whole,
            scratch_shapes=[
                pltpu.VMEM((lines, width), f32),
                pltpu.VMEM((plan.listed, plan.markers), bf16),
                pltpu.VMEM((plan.markers, width), f32),
                pltpu.VMEM((9 * GROUP, width), f32),
                pltpu.VMEM((8, plan.markers), f32),
                pltpu.VMEM((8, plan.faces), f32),
                pltpu.VMEM((4, 8, width), f32),
                dma((8,)),
                dma((8,)),
            ],
            compiler_params=pltpu.CompilerParams(
                vmem_limit_bytes=SEND_LIMIT, collective_id=1, has_side_effects=True
            ),
            name="give_back",
        )(partial, plain, spots, table, base_x, base_y, places_line, tile_count)
        return u_new, out

    args = (u_old, density, offsets, forces, base_x, base_y, base_z, tile_count)
    return lax.cond(over[0] > 0, dense_device, sparse, *args)


def solution(mesh):
    in_specs = (
        P(None, "gx", "gy", None),
        P("gx", "gy", None),
        P(None, ("gx", "gy"), None),
        P(None, ("gx", "gy"), None),
        P(("gx", "gy"), None),
        P(("gx", "gy"), None),
        P(("gx", "gy"), None),
        P(("gx", "gy")),
    )
    out_specs = (P(None, "gx", "gy", None), P(None, ("gx", "gy"), None))
    return jax.shard_map(
        on_device, mesh=mesh, in_specs=in_specs, out_specs=out_specs, check_vma=False
    )
```

```python
import functools

import jax
import jax.numpy as jnp
from jax import lax
from jax.experimental import pallas as pl
from jax.experimental.pallas import tpu as pltpu
from jax.sharding import PartitionSpec as P

VMEM_LIMIT = 60 * 1024 * 1024
SEND_LIMIT = 10 * 1024 * 1024
MAIN_LIMIT = 26 * 1024 * 1024


def divisor(count, most):
    return max(d for d in range(1, most + 1) if count % d == 0)


def moved(value, step_x, step_y):
    if step_y == 0:
        n = lax.axis_size("gx")
        return lax.ppermute(value, "gx", [(i, (i + step_x) % n) for i in range(n)])
    if step_x == 0:
        n = lax.axis_size("gy")
        return lax.ppermute(value, "gy", [(i, (i + step_y) % n) for i in range(n)])
    nx, ny = lax.axis_size("gx"), lax.axis_size("gy")
    pairs = [
        (i * ny + j, ((i + step_x) % nx) * ny + (j + step_y) % ny)
        for i in range(nx)
        for j in range(ny)
    ]
    return lax.ppermute(value, ("gx", "gy"), pairs)


def stencil(frac):
    root = jnp.sqrt(1.0 + 4.0 * frac - 4.0 * frac * frac)
    return [
        (3.0 - 2.0 * frac - root) / 8.0,
        (3.0 - 2.0 * frac + root) / 8.0,
        (1.0 + 2.0 * frac + root) / 8.0,
        (1.0 + 2.0 * frac - root) / 8.0,
    ]


def pick(delta, four):
    total = jnp.where(delta == 0, four[0], 0.0)
    for k in range(1, 4):
        total = jnp.where(delta == k, four[k], total)
    return total


def wrapped(delta, length):
    delta = jnp.where(delta < 0, delta + length, delta)
    return jnp.where(delta >= length, delta - length, delta)


def edge_weights(frac, base, rows, size):
    row = lax.broadcasted_iota(jnp.int32, (rows, base.shape[1]), 0)
    cell = jnp.where(row == size + 2, -1, row)
    cell = jnp.where(row > size + 2, -8, cell)
    return pick(cell - base + 1, stencil(frac))


def halves(value):
    high = value.astype(jnp.bfloat16)
    low = (value - high.astype(jnp.float32)).astype(jnp.bfloat16)
    return high, low


def edges(size):
    return (size - 1, size, size + 1), (size + 2, 0, 1)


def spread_kernel(size_x, size_y, feat, base, grid, *refs):
    slabs, (wx_s, wy_s, high_s, low_s) = refs[:8], refs[8:]
    planes, rows, depth = grid.shape[1], grid.shape[2], grid.shape[3]
    markers = feat.shape[1]
    wx_s[...] = edge_weights(feat[0:1, :], base[0:1, :], wx_s.shape[0], size_x)
    wy_s[...] = edge_weights(feat[1:2, :], base[1:2, :], rows, size_y)
    four = stencil(feat[2:3, :])
    column = jnp.concatenate(
        four + [base[2:3, :].astype(jnp.float32)] + [feat[3 + c : 4 + c, :] for c in range(3)], axis=0
    ).T
    cut = 256 if markers % 256 == 0 else 128
    for start in range(0, markers, cut):
        part = column[start : start + cut]
        lane = lax.broadcasted_iota(jnp.int32, (cut, depth), 1)
        delta = wrapped(lane - part[:, 4:5].astype(jnp.int32) + 1, depth)
        wz = pick(delta, [part[:, k : k + 1] for k in range(4)])
        for c in range(3):
            high, low = halves(wz * part[:, 5 + c : 6 + c])
            high_s[start : start + cut, c * depth : (c + 1) * depth] = high
            low_s[start : start + cut, c * depth : (c + 1) * depth] = low
    group = divisor(planes, 8)

    def turn(g, carry):
        first = g * group
        left = jnp.concatenate(
            [wy_s[...] * wx_s[pl.ds(first + j, 1), :] for j in range(group)], axis=0
        )
        high, low = halves(left)
        dot = functools.partial(jnp.dot, preferred_element_type=jnp.float32)
        total = dot(high, high_s[...]) + dot(low, high_s[...]) + dot(high, low_s[...])
        for j in range(group):
            for c in range(3):
                grid[c, first + j] = total[j * rows : (j + 1) * rows, c * depth : (c + 1) * depth]
        return carry

    lax.fori_loop(0, planes // group, turn, 0)
    sides_x, sides_y = edges(size_x), edges(size_y)
    for side in range(2):
        for c in range(3):
            for j, p in enumerate(sides_x[side]):
                slabs[side][c, j] = grid[c, p]
                for other in range(2):
                    for i, r in enumerate(sides_y[other]):
                        slabs[4 + 2 * side + other][c, j, i : i + 1] = grid[c, p, r : r + 1]
            for i, r in enumerate(sides_y[side]):
                for p in range(planes):
                    slabs[2 + side][c, i, p : p + 1] = grid[c, p, r : r + 1]


def read_kernel(size_x, size_y, time_step, *refs):
    feat, base, grid, u_old, density, low_x, high_x, low_y, high_y = refs[:9]
    slabs, (u_new, velocity) = refs[9:17], refs[17:19]
    total, wx_s, wy_s, wz3, table = refs[19:]
    planes, rows, depth = grid.shape[1], grid.shape[2], grid.shape[3]
    markers = feat.shape[1]
    wx_s[...] = edge_weights(feat[0:1, :], base[0:1, :], wx_s.shape[0], size_x)
    wy_s[...] = edge_weights(feat[1:2, :], base[1:2, :], rows, size_y)
    cut = 256 if markers % 256 == 0 else 128
    for start in range(0, markers, cut):
        at = slice(start, start + cut)
        row = lax.broadcasted_iota(jnp.int32, (depth, cut), 0)
        delta = wrapped(row - base[2:3, at] + 1, depth)
        high, low = halves(pick(delta, stencil(feat[2:3, at])))
        wz3[0:depth, at] = high
        wz3[depth : 2 * depth, at] = high
        wz3[2 * depth :, at] = low
    total[...] = grid[...]
    near_x, near_y = edges(size_x)[::-1], edges(size_y)[::-1]
    for side in range(2):
        for c in range(3):
            for j, p in enumerate(near_x[side]):
                total[c, p] = total[c, p] + slabs[side][c, j]
                for other in range(2):
                    for i, r in enumerate(near_y[other]):
                        total[c, p, r : r + 1] = (
                            total[c, p, r : r + 1] + slabs[4 + 2 * side + other][c, j, i : i + 1]
                        )
            for i, r in enumerate(near_y[side]):
                for p in range(planes):
                    total[c, p, r : r + 1] = total[c, p, r : r + 1] + slabs[2 + side][c, i, p : p + 1]
    group = divisor(planes, 6)
    spare = jnp.ones((rows - size_y - 3, depth), jnp.float32)

    def plane_state(k, p):
        if p < size_x:
            main = density[p] if k == 3 else u_old[k, p]
        elif p < size_x + 2:
            main = high_x[k, p - size_x]
        else:
            main = low_x[k, 0]
        edge = [high_y[k, 0, p : p + 1], high_y[k, 1, p : p + 1], low_y[k, 0, p : p + 1], spare]
        return jnp.concatenate([main] + edge, axis=0)

    for g in range(planes // group):
        pieces = []
        for p in range(g * group, (g + 1) * group):
            scale = time_step / plane_state(3, p)
            for c in range(3):
                value = plane_state(c, p) + total[c, p] * scale
                if p < size_x:
                    u_new[c, p] = value[:size_y]
                pieces.append(value)
        high, low = halves(jnp.concatenate(pieces, axis=0))
        table[g, :, 0:depth] = high
        table[g, :, depth : 2 * depth] = low
        table[g, :, 2 * depth :] = high

    def turn(step, carry):
        at = pl.ds(pl.multiple_of(step * cut, cut), cut)
        right = wz3[:, at]
        wy = wy_s[:, at]
        sums = [jnp.zeros((8, cut), jnp.float32) for _ in range(3)]
        for g in range(planes // group):
            found = jnp.dot(table[g], right, preferred_element_type=jnp.float32)
            for j in range(group):
                p = g * group + j
                weight = wy * wx_s[p : p + 1, at]
                for c in range(3):
                    first = (j * 3 + c) * rows
                    product = found[first : first + rows] * weight
                    for r in range(0, rows, 8):
                        sums[c] = sums[c] + product[r : r + 8]
        velocity[:, at] = (
            jnp.concatenate([jnp.sum(s, axis=0, keepdims=True) for s in sums], axis=0) * feat[6:7, at]
        )
        return carry

    lax.fori_loop(0, markers // cut, turn, 0)


def dense_device(u_old, density, offsets, forces, base_x, base_y, base_z, tile_count):
    time_step = 0.5
    _, size_x, size_y, depth = u_old.shape
    slots, width = base_x.shape
    markers = slots * width
    planes = size_x + 3
    rows = -(-(size_y + 3) // 8) * 8
    lines = -(-planes // 8) * 8
    f32, bf16 = jnp.float32, jnp.bfloat16
    live = (lax.broadcasted_iota(jnp.int32, (slots, width), 0) < tile_count[0]).astype(f32)
    feat = jnp.concatenate([offsets, forces * live[None], live[None]], axis=0).reshape(7, markers)
    base = jnp.stack([base_x, base_y, base_z], axis=0).reshape(3, markers)

    up = jnp.concatenate([u_old[:, size_x - 1 :], density[None, size_x - 1 :]], axis=0)
    down = jnp.concatenate([u_old[:, :2], density[None, :2]], axis=0)
    low_x, high_x = moved(up, 1, 0), moved(down, -1, 0)

    def strip(r):
        inner = jnp.concatenate([u_old[:, :, r], density[None, :, r]], axis=0)
        return jnp.concatenate([inner, high_x[:, :, r], low_x[:, :, r]], axis=1)

    low_y = moved(strip(size_y - 1)[:, None], 0, 1)
    high_y = moved(jnp.stack([strip(0), strip(1)], axis=1), 0, -1)

    params = pltpu.CompilerParams(vmem_limit_bytes=VMEM_LIMIT)
    slab_x = jax.ShapeDtypeStruct((3, 3, rows, depth), f32)
    slab_y = jax.ShapeDtypeStruct((3, 3, planes, depth), f32)
    corner = jax.ShapeDtypeStruct((3, 3, 3, depth), f32)
    whole = pl.BlockSpec(memory_space=pltpu.VMEM)
    flops = 6 * planes * rows * 3 * depth * markers
    cost = pl.CostEstimate(flops=flops, transcendentals=0, bytes_accessed=8 * planes * rows * depth)
    grid, *slabs = pl.pallas_call(
        functools.partial(spread_kernel, size_x, size_y),
        out_shape=[jax.ShapeDtypeStruct((3, planes, rows, depth), f32)]
        + [slab_x] * 2
        + [slab_y] * 2
        + [corner] * 4,
        in_specs=[whole] * 2,
        out_specs=[whole] * 9,
        scratch_shapes=[
            pltpu.VMEM((lines, markers), f32),
            pltpu.VMEM((rows, markers), f32),
            pltpu.VMEM((markers, 3 * depth), bf16),
            pltpu.VMEM((markers, 3 * depth), bf16),
        ],
        compiler_params=params,
        cost_estimate=cost,
        name="spread",
    )(feat, base)
    ways = [(1, 0), (-1, 0), (0, 1), (0, -1), (1, 1), (1, -1), (-1, 1), (-1, -1)]
    slabs = [moved(slab, *way) for slab, way in zip(slabs, ways)]
    group = divisor(planes, 6)
    u_new, velocity = pl.pallas_call(
        functools.partial(read_kernel, size_x, size_y, time_step),
        out_shape=[
            jax.ShapeDtypeStruct(u_old.shape, f32),
            jax.ShapeDtypeStruct((3, markers), f32),
        ],
        in_specs=[whole] * 17,
        out_specs=[whole] * 2,
        scratch_shapes=[
            pltpu.VMEM((3, planes, rows, depth), f32),
            pltpu.VMEM((lines, markers), f32),
            pltpu.VMEM((rows, markers), f32),
            pltpu.VMEM((3 * depth, markers), bf16),
            pltpu.VMEM((planes // group, group * 3 * rows, 3 * depth), bf16),
        ],
        compiler_params=params,
        cost_estimate=cost,
        name="read",
    )(feat, base, grid, u_old, density, low_x, high_x, low_y, high_y, *slabs)
    return (u_new, velocity.reshape(3, slots, width))


MESH = pl.DeviceIdType.MESH
WAYS = [(1, 0), (-1, 0), (0, 1), (0, -1), (1, 1), (1, -1), (-1, 1), (-1, -1)]
OWN_BATCH, LIST_BATCH = 8, 8
GROUP, LIST_GROUP = 64, 32
HOP = 17


def thirds(value):
    high = value.astype(jnp.bfloat16).astype(jnp.float32)
    rest = value - high
    middle = rest.astype(jnp.bfloat16).astype(jnp.float32)
    return [high, middle, rest - middle]


class Plan:
    def __init__(self, size_x, size_y, depth, slots, width):
        self.size_x, self.size_y, self.depth = size_x, size_y, depth
        self.slots, self.width = slots, width
        self.markers = slots * width

        def cap(reach, size):
            return -(-2 * reach * self.markers // size // width) * width

        corner = width // 4
        self.caps = [cap(2, size_x), cap(1, size_x), cap(2, size_y), cap(1, size_y)] + [corner] * 4
        self.starts = [sum(self.caps[:d]) for d in range(8)]
        self.listed = sum(self.caps)
        self.faces = self.starts[4]
        self.tiles = slots + self.listed // width
        self.total = self.tiles * width
        self.tile_rows = -(-self.tiles // 8) * 8
        self.outers = (size_x + 2) // 2 + 2
        self.outer_rows = 2 * (depth + 4)
        self.grid_rows = self.outers * self.outer_rows

    def span(self, d):
        if d < 4:
            return self.starts[d], self.caps[d]
        return self.faces, self.width


def row_mask(shape, value):
    return lax.broadcasted_iota(jnp.int32, shape, 0) == value


def prepare(plan, data, first, count, batch, group, spots, own, plain, places):
    width, size_y = plan.width, plan.size_y
    f32, bf16 = jnp.float32, jnp.bfloat16
    k_row = lax.broadcasted_iota(jnp.int32, (32, 6 * width), 0)
    n_lane = lax.broadcasted_iota(jnp.int32, (32, 6 * width), 1)
    kind = k_row % 8
    part, inside = n_lane // width, n_lane % width
    hit = ((kind < 5) & (part == kind)) | ((kind > 4) & (part == 5) & (inside // size_y == kind - 5))
    select = jnp.where(hit & (k_row < 24), 1.0, 0.0).astype(bf16)
    k_row = lax.broadcasted_iota(jnp.int32, (32, 8 * width), 0)
    n_lane = lax.broadcasted_iota(jnp.int32, (32, 8 * width), 1)
    hit = (k_row % 8 == n_lane // width) & (k_row < 24)
    spread_out = jnp.where(hit, 1.0, 0.0).astype(bf16)
    step = 4
    for t0 in range(0, count, step):
        n = min(step, count - t0) * width
        d = data[:, t0 * width : t0 * width + n]
        at = slice((first + t0) * width, (first + t0) * width + n)
        rows = lax.broadcasted_iota(jnp.int32, (8, n), 0)
        w = stencil(jnp.where(rows < 3, d[0:8], 0.5))
        factors = jnp.concatenate([v[2:3] for v in w] + [v[0:1] for v in w], axis=0)
        stack = jnp.concatenate(thirds(factors) + [jnp.zeros((8, n), f32)], axis=0)
        left = stack.T.astype(bf16)
        base = (first + t0) * width * HOP
        x = [
            jnp.dot(left, spread_out[:, i * width : (i + 2) * width], preferred_element_type=f32)
            for i in (4, 6)
        ]
        x = [x[i // 2][:, (i % 2) * width : (i % 2 + 1) * width] for i in range(4)]
        for i in range(0, 4, 2):
            z = jnp.dot(left, spread_out[:, i * width : (i + 2) * width], preferred_element_type=f32)
            for j in range(2):
                for h in range(2):
                    for side in range(2):
                        row = base + 8 * h + 2 * (i + j) + side
                        value = z[:, j * width : (j + 1) * width] * x[2 * h + side]
                        spots[pl.ds(row, n, stride=HOP), :] = value
        block = jnp.concatenate([v[1:2] for v in w] + [d[7:8], d[3:6]], axis=0)
        stack = jnp.concatenate(thirds(block) + [jnp.zeros((8, n), f32)], axis=0).astype(bf16)
        wide = lax.dot_general(
            stack, select, (((0,), (0,)), ((), ())), preferred_element_type=f32
        )
        cols = [wide[:, i * width : (i + 1) * width] for i in range(6)]
        lane = lax.broadcasted_iota(jnp.int32, (n, width), 1)
        y = jnp.where(lane < 3 * size_y, lane % size_y, -1000).astype(f32)
        pattern = pick(y - cols[4] + 1.0, cols[:4])
        plain[at, :] = pattern
        own[at, :] = pattern * cols[5]
    keys, zs, bases, goods = [], [], [], []
    for t in range(count):
        at = slice(t * width, (t + 1) * width)
        bx = data[6:7, at].astype(jnp.int32)
        bz = data[8:9, at].astype(jnp.int32)
        good = data[9:10, at] > 0.0
        lane = lax.broadcasted_iota(jnp.int32, (1, width), 1)
        step_in = lane % batch
        across = bx + 2
        side, outer = across % 2, across // 2
        spare = plan.grid_rows + ((plan.size_x + 2) // 2) * plan.outer_rows + 8 * step_in
        base = side * plan.grid_rows + outer * plan.outer_rows + 2 * bz
        bases.append(jnp.where(good, base, spare))
        keys.append(jnp.where(good, side * (plan.outers + 8) + outer, -100 - 10 * step_in))
        zs.append(bz)
        goods.append(jnp.where(good, 1, 0))
    rows = -(-count // 8) * 8
    fill = [jnp.zeros((rows - count, width), jnp.int32)] if rows > count else []
    key, z = jnp.concatenate(keys + fill, axis=0), jnp.concatenate(zs + fill, axis=0)
    base = jnp.concatenate(bases + fill, axis=0)
    lane = lax.broadcasted_iota(jnp.int32, (rows, width), 1) % batch

    def near(a, b, most):
        return (a - b <= most) & (b - a <= most)

    clashes = [
        (lane >= d) & near(key, pltpu.roll(key, d, 1), 1) & near(z, pltpu.roll(z, d, 1), 3)
        for d in range(1, batch)
    ]
    second = clashes[0]
    for clash in clashes[1:]:
        second = second | clash
    second = jnp.where(second, 1, 0)
    bad = jnp.zeros((rows, width), jnp.int32)
    for d, clash in enumerate(clashes):
        both = second * pltpu.roll(second, d + 1, 1)
        bad = jnp.maximum(bad, jnp.where(clash, both, 0))
    places[first : first + rows, :] = base + second * (2 * plan.grid_rows)
    good = jnp.concatenate(goods + fill, axis=0)
    lane = lax.broadcasted_iota(jnp.int32, (rows, width), 1) // group
    state = jnp.zeros((rows, width), jnp.int32)
    for h in range(width // group):
        here = lane == h
        worst = jnp.max(jnp.where(here, bad, 0), axis=1, keepdims=True)
        some = jnp.max(jnp.where(here, good, 0), axis=1, keepdims=True)
        filled = jnp.sum(jnp.where(here, good, 0), axis=1, keepdims=True)
        state = jnp.where(here, some * (1 + worst * filled), state)
    below = plan.tile_rows + first
    places[below : below + rows, :] = state
    below = 2 * plan.tile_rows + first
    places[below : below + rows, :] = base


def place():
    nx, ny = lax.axis_size("gx"), lax.axis_size("gy")
    return nx, ny, lax.axis_index("gx"), lax.axis_index("gy")


def list_slots(plan, bx, by, live):
    f32, bf16 = jnp.float32, jnp.bfloat16
    slots, width = plan.slots, plan.width
    ahead_x = jnp.where(bx >= plan.size_x - 2, live, 0.0)
    back_x = jnp.where(bx < 1, live, 0.0)
    ahead_y = jnp.where(by >= plan.size_y - 2, 1.0, 0.0)
    back_y = jnp.where(by < 1, 1.0, 0.0)
    flags = []
    for step_x, step_y in WAYS:
        flag = {1: ahead_x, -1: back_x, 0: live}[step_x]
        flags.append(flag if step_y == 0 else flag * (ahead_y if step_y > 0 else back_y))
    flag = jnp.concatenate(flags, axis=0)
    lines = 8 * slots
    r, c = (lax.broadcasted_iota(jnp.int32, (width, width), a) for a in range(2))
    upper = jnp.where(r <= c, 1.0, 0.0).astype(bf16)
    r, c = (lax.broadcasted_iota(jnp.int32, (lines, lines), a) for a in range(2))
    before = jnp.where((c < r) & (c // slots == r // slots), 1.0, 0.0).astype(bf16)
    within = jnp.dot(flag.astype(bf16), upper, preferred_element_type=f32)
    count = jnp.broadcast_to(jnp.sum(flag, axis=1, keepdims=True), (lines, width))
    earlier = jnp.dot(before, count.astype(bf16), preferred_element_type=f32)
    slot = jnp.where(flag > 0.0, earlier + within - 1.0, -1.0)
    return slot


def read_group(plan, group, places, table, spots, plain, sums, found, first, to):
    for j in range(group):
        here = places[2 * plan.tile_rows * plan.width + first + j]
        at = first * HOP + j * HOP
        sums[9 * j : 9 * j + 8, :] = (
            table[pl.ds(here, 8), :] * spots[pl.ds(at, 8), :]
            + table[pl.ds(here + plan.outer_rows, 8), :] * spots[pl.ds(at + 8, 8), :]
        )
    for j in range(0, group, 8):
        row = sums[pl.ds(9 * j, 8, stride=9), :]
        for s in range(1, 8):
            row = row + sums[pl.ds(9 * j + s, 8, stride=9), :]
        row = row * plain[pl.ds(pl.multiple_of(first + j, 8), 8), :]
        found[pl.ds(pl.multiple_of(to + j, 8), 8), :] = row


def component_sums(plan, found, count, out):
    f32, bf16 = jnp.float32, jnp.bfloat16
    width, size_y = plan.width, plan.size_y
    r = lax.broadcasted_iota(jnp.int32, (16, width), 0)
    lane = lax.broadcasted_iota(jnp.int32, (16, width), 1)
    by_part = jnp.where((lane // size_y == r) & (lane < 3 * size_y), 1.0, 0.0).astype(bf16)
    block = 2 * width
    for first in range(0, count, block):
        n = min(block, count - first)
        value = found[first : first + n, :]
        result = None
        for piece in thirds(value):
            part = lax.dot_general(
                by_part, piece.astype(bf16), (((1,), (1,)), ((), ())), preferred_element_type=f32
            )
            result = part if result is None else result + part
        out[:, first : first + n] = result[0:8]


def send_kernel(plan, *refs):
    arguments, tile_count = refs[:5], refs[5]
    (own, plain, spots, places, any_over) = refs[6:11]
    data, one_hot, lists, inbox, corners, got, note, notes, slot_map = refs[11:20]
    send_sem, recv_sem, note_send, note_recv, load_sem = refs[20:25]
    offsets, forces, base_x, base_y, base_z = refs[25:]
    loads = [
        pltpu.make_async_copy(far, near, load_sem.at[i])
        for i, (far, near) in enumerate(zip(arguments, refs[25:]))
    ]
    for load in loads:
        load.start()
    f32, bf16 = jnp.float32, jnp.bfloat16
    slots, width, markers = plan.slots, plan.width, plan.markers
    nx, ny, mx, my = place()
    devices = nx * ny
    me = mx * ny + my

    def other(i):
        to = lax.rem(me + i, devices)
        return to // ny, lax.rem(to, ny)

    barrier = pltpu.get_barrier_semaphore()

    def greet(i, carry):
        pl.semaphore_signal(barrier, inc=1, device_id=other(i), device_id_type=MESH)
        return carry

    lax.fori_loop(1, devices, greet, 0)
    for load in loads:
        load.wait()

    live = jnp.where(lax.broadcasted_iota(jnp.int32, (slots, width), 0) < tile_count[0], 1.0, 0.0)
    bx, by, bz = base_x[...], base_y[...], base_z[...]
    values = [offsets[c] for c in range(3)] + [forces[c] * live for c in range(3)]
    values = values + [bx.astype(f32), by.astype(f32), bz.astype(f32), live]
    data[10:16, :] = jnp.zeros((6, markers), f32)
    for k, value in enumerate(values):
        for t in range(slots):
            data[k : k + 1, t * width : (t + 1) * width] = value[t : t + 1, :]
    slot = list_slots(plan, bx, by, live)
    slot_map[...] = slot
    over = jnp.zeros((slots, width), f32)
    for d in range(8):
        here = slot[d * slots : (d + 1) * slots]
        over = jnp.maximum(over, jnp.where(here >= plan.caps[d], 1.0, 0.0))
    note[...] = jnp.broadcast_to(jnp.max(over), note.shape)
    fill_one_hot(plan, slot_map, one_hot)
    stack = jnp.concatenate(thirds(data[...]), axis=0).astype(bf16)
    found = lax.dot_general(
        stack, one_hot[...], (((1,), (1,)), ((), ())), preferred_element_type=f32
    )
    found = found[0:16] + found[16:32] + found[32:48]
    lane = lax.broadcasted_iota(jnp.int32, (1, plan.listed), 1)
    for row, axis, size in ((6, 0, plan.size_x), (7, 1, plan.size_y)):
        shift = jnp.zeros((1, plan.listed), f32)
        for d in range(8):
            inside = (lane >= plan.starts[d]) & (lane < plan.starts[d] + plan.caps[d])
            shift = jnp.where(inside, float(WAYS[d][axis] * size), shift)
        moved_by = jnp.where(row_mask((16, plan.listed), row), shift * found[9:10], 0.0)
        found = found - moved_by
    lists[...] = found

    pl.semaphore_wait(barrier, devices - 1)

    def word(i):
        return pltpu.make_async_remote_copy(
            src_ref=note,
            dst_ref=notes.at[i],
            send_sem=note_send.at[i],
            recv_sem=note_recv.at[i],
            device_id=other(i),
            device_id_type=MESH,
        )

    copies = []
    for d, (step_x, step_y) in enumerate(WAYS):
        start, size = plan.span(d)
        target = inbox.at[:, pl.ds(start, size)] if d < 4 else corners.at[d - 4]
        copies.append(
            pltpu.make_async_remote_copy(
                src_ref=lists.at[:, pl.ds(start, size)],
                dst_ref=target,
                send_sem=send_sem.at[d],
                recv_sem=recv_sem.at[d],
                device_id=(lax.rem(mx + step_x + nx, nx), lax.rem(my + step_y + ny, ny)),
                device_id_type=MESH,
            )
        )
        copies[-1].start()

    def tell(i, carry):
        word(i).start()
        return carry

    lax.fori_loop(1, devices, tell, 0)
    prepare(plan, data, 0, slots, OWN_BATCH, GROUP, spots, own, plain, places)
    for copy in copies:
        copy.wait()

    got[:, 0 : plan.faces] = inbox[...]
    lane = lax.broadcasted_iota(jnp.int32, (16, width), 1) // plan.caps[4]
    last = corners[0]
    for i in range(1, 4):
        last = jnp.where(lane == i, corners[i], last)
    got[:, plan.faces :] = last
    prepare(plan, got, slots, plan.tiles - slots, LIST_BATCH, LIST_GROUP, spots, own, plain, places)

    def hear(i, most):
        word(i).wait()
        return jnp.maximum(most, notes[i])

    any_over[0] = jnp.max(lax.fori_loop(1, devices, hear, note[...])).astype(jnp.int32)


def fill_one_hot(plan, slot_map, one_hot):
    for d in range(8):
        rows = plan.caps[d]
        index = lax.broadcasted_iota(jnp.int32, (rows, plan.width), 0).astype(jnp.float32)
        for t in range(plan.slots):
            line = slot_map[d * plan.slots + t : d * plan.slots + t + 1, :]
            hot = jnp.where(index == line, 1.0, 0.0).astype(jnp.bfloat16)
            one_hot[plan.starts[d] : plan.starts[d] + rows, t * plan.width : (t + 1) * plan.width] = hot


def main_kernel(plan, time_step, *refs):
    own, plain, spots, places, tile_count, u_in, density_in, u_out, partial, table = refs[:10]
    grid, found, sums, u_s, density_s, sems = refs[10:]
    f32, bf16 = jnp.float32, jnp.bfloat16
    width, depth, size_y, total = plan.width, plan.depth, plan.size_y, plan.total
    outer_rows, grid_rows = plan.outer_rows, plan.grid_rows
    loads = [
        pltpu.make_async_copy(u_in, u_s, sems.at[0]),
        pltpu.make_async_copy(density_in, density_s, sems.at[1]),
    ]
    for load in loads:
        load.start()
    zero = jnp.zeros((8, width), f32)

    def clear(i, carry):
        for g in range(4):
            at = g * grid_rows + i * outer_rows
            for j in range(0, outer_rows, 8):
                grid[pl.ds(pl.multiple_of(at + j, 8), 8), :] = zero
        return carry

    lax.fori_loop(1, plan.outers - 1, clear, 0)
    for o in (0, 1, plan.outers - 2, plan.outers - 1):
        for g in range(2):
            at = g * grid_rows + o * outer_rows
            table[at : at + outer_rows, :] = jnp.zeros((outer_rows, width), f32)
    found[...] = jnp.zeros((plan.listed, width), f32)

    def spread_group(batch, group, g, carry):
        first = g * group
        state = places[plan.tile_rows * width + first]

        def windows(j):
            here = places[first + j]
            at = first * HOP + j * HOP
            row = jnp.broadcast_to(own[pl.ds(first + j, 1), :], (8, width))
            one, two = pl.ds(here, 8), pl.ds(here + outer_rows, 8)
            return [
                (one, grid[one, :] + spots[pl.ds(at, 8), :] * row),
                (two, grid[two, :] + spots[pl.ds(at + 8, 8), :] * row),
            ]

        @pl.when(state == 1)
        def _():
            for j0 in range(0, group, batch):
                stores = []
                for j in range(j0, j0 + batch):
                    stores = stores + windows(j)
                for where, value in stores:
                    grid[where, :] = value

        @pl.when(state > 1)
        def _():
            def single(j, c):
                for where, value in windows(j):
                    grid[where, :] = value
                return c

            lax.fori_loop(0, state - 1, single, 0)

        return carry

    live_groups = tile_count[0] * (width // GROUP)
    lists_from, all_groups = plan.markers // LIST_GROUP, total // LIST_GROUP
    lax.fori_loop(0, live_groups, functools.partial(spread_group, OWN_BATCH, GROUP), 0)
    lax.fori_loop(lists_from, all_groups, functools.partial(spread_group, LIST_BATCH, LIST_GROUP), 0)

    def fold(i, carry):
        stores = []
        for g in range(4):
            at = g * grid_rows + i * outer_rows
            for to, source, rows in [(2 * depth, 0, 2), (2, 2 * depth + 2, 4)]:
                here = pl.ds(at + to, rows)
                stores.append((here, grid[here, :] + grid[pl.ds(at + source, rows), :]))
        for where, value in stores:
            grid[where, :] = value
        return carry

    lax.fori_loop(1, plan.outers - 1, fold, 0)
    for load in loads:
        load.wait()

    def lines(g, outer, side):
        return pl.ds(g * grid_rows + outer * outer_rows + 2 + side, depth, stride=2)

    def plane(p, homes):
        force = None
        for copy in range(2):
            for g, outer, side in homes:
                part = grid[lines(2 * copy + g, outer, side), :]
                force = part if force is None else force + part
        force = force.T
        scale = time_step / density_s[p]
        pieces = []
        for c in range(3):
            value = u_s[c, p] + force[c * size_y : (c + 1) * size_y] * scale
            u_s[c, p] = value
            pieces.append(value)
        if width > 3 * size_y:
            pieces.append(jnp.zeros((width - 3 * size_y, depth), f32))
        back = jnp.concatenate(pieces, axis=0).T
        for g, outer, side in homes:
            table[lines(g, outer, side), :] = back
            at = g * grid_rows + outer * outer_rows + side
            table[pl.ds(at, 1), :] = back[depth - 1 : depth]
            table[pl.ds(at + 2 * depth + 2, 1), :] = back[0:1]
            table[pl.ds(at + 2 * depth + 4, 1), :] = back[1:2]

    def pair(i, carry):
        for j in range(pairs):
            o = i * pairs + j
            plane(2 * o, [(0, o + 1, 1), (1, o + 1, 0)])
            plane(2 * o + 1, [(0, o + 2, 0), (1, o + 1, 1)])
        return carry

    pairs = divisor(plan.size_x // 2, 2)
    lax.fori_loop(0, plan.size_x // 2 // pairs, pair, 0)
    leave = pltpu.make_async_copy(u_s, u_out, sems.at[2])
    leave.start()

    def read_list(g, carry):
        first = g * LIST_GROUP

        @pl.when(places[plan.tile_rows * width + first] > 0)
        def _():
            read_group(
                plan, LIST_GROUP, places, table, spots, plain, sums, found, first, first - plan.markers
            )

        return carry

    lax.fori_loop(lists_from, all_groups, read_list, 0)
    component_sums(plan, found, plan.listed, partial)
    leave.wait()


def return_kernel(plan, *refs):
    partial, plain, spots, table, base_x, base_y, places, tile_count, out = refs[:9]
    slot_map, one_hot, found, sums, velocity, inbox, corners, send_sem, recv_sem = refs[9:]
    f32, bf16 = jnp.float32, jnp.bfloat16
    width = plan.width
    nx, ny, mx, my = place()
    barrier = pltpu.get_barrier_semaphore()

    def neighbour(step_x, step_y):
        return (lax.rem(mx + step_x + nx, nx), lax.rem(my + step_y + ny, ny))

    for way in WAYS:
        pl.semaphore_signal(barrier, inc=1, device_id=neighbour(*way), device_id_type=MESH)
    pl.semaphore_wait(barrier, len(WAYS))
    copies = []
    for d, (step_x, step_y) in enumerate(WAYS):
        start, size = plan.span(d)
        target = inbox.at[:, pl.ds(start, size)] if d < 4 else corners.at[d - 4]
        copies.append(
            pltpu.make_async_remote_copy(
                src_ref=partial.at[:, pl.ds(start, size)],
                dst_ref=target,
                send_sem=send_sem.at[d],
                recv_sem=recv_sem.at[d],
                device_id=neighbour(-step_x, -step_y),
                device_id_type=MESH,
            )
        )
        copies[-1].start()

    def read(g, carry):
        first = g * GROUP
        read_group(plan, GROUP, places, table, spots, plain, sums, found, first, first)
        return carry

    lax.fori_loop(0, plan.markers // GROUP, read, 0)
    component_sums(plan, found, plan.markers, velocity)
    shape = (plan.slots, width)
    live = jnp.where(lax.broadcasted_iota(jnp.int32, shape, 0) < tile_count[0], 1.0, 0.0)
    slot_map[...] = list_slots(plan, base_x[...], base_y[...], live)
    fill_one_hot(plan, slot_map, one_hot)
    for copy in copies:
        copy.wait()
    lane = lax.broadcasted_iota(jnp.int32, (8, width), 1) // plan.caps[4]
    last = corners[0]
    for i in range(1, 4):
        last = jnp.where(lane == i, corners[i], last)
    back = jnp.concatenate([inbox[...], last], axis=1)
    stack = jnp.concatenate(thirds(back) + [jnp.zeros_like(back)], axis=0).astype(bf16)
    extra = jnp.dot(stack, one_hot[...], preferred_element_type=f32)
    extra = extra[0:8] + extra[8:16] + extra[16:24]
    total = velocity[...] + extra
    live = tile_count[0]
    for t in range(plan.slots):
        row = total[:, t * width : (t + 1) * width]
        row = jnp.where(lax.broadcasted_iota(jnp.int32, row.shape, 0) * 0 + t < live, row, 0.0)
        for c in range(3):
            out[c, t : t + 1, :] = row[c : c + 1, :]


def on_device(u_old, density, offsets, forces, base_x, base_y, base_z, tile_count):
    time_step = 0.5
    _, size_x, size_y, depth = u_old.shape
    slots, width = base_x.shape
    plan = Plan(size_x, size_y, depth, slots, width)
    f32, bf16 = jnp.float32, jnp.bfloat16
    devices = lax.axis_size("gx") * lax.axis_size("gy")
    whole, scalars = pl.BlockSpec(memory_space=pltpu.VMEM), pl.BlockSpec(memory_space=pltpu.SMEM)
    far = pl.BlockSpec(memory_space=pl.ANY)
    lines = 8 * slots
    dma = pltpu.SemaphoreType.DMA
    own, plain, spots, places, over = pl.pallas_call(
        functools.partial(send_kernel, plan),
        out_shape=[
            jax.ShapeDtypeStruct((plan.total, width), f32),
            jax.ShapeDtypeStruct((plan.total, width), f32),
            jax.ShapeDtypeStruct((plan.total * HOP, width), f32),
            jax.ShapeDtypeStruct((3 * plan.tile_rows, width), jnp.int32),
            jax.ShapeDtypeStruct((1,), jnp.int32),
        ],
        in_specs=[far] * 5 + [scalars],
        out_specs=[whole] * 4 + [scalars],
        scratch_shapes=[
            pltpu.VMEM((16, plan.markers), f32),
            pltpu.VMEM((plan.listed, plan.markers), bf16),
            pltpu.VMEM((16, plan.listed), f32),
            pltpu.VMEM((16, plan.faces), f32),
            pltpu.VMEM((4, 16, width), f32),
            pltpu.VMEM((16, plan.listed), f32),
            pltpu.VMEM((1, width), f32),
            pltpu.VMEM((devices, 1, width), f32),
            pltpu.VMEM((lines, width), f32),
            dma((8,)),
            dma((8,)),
            dma((devices,)),
            dma((devices,)),
            dma((5,)),
        ]
        + [pltpu.VMEM(offsets.shape, f32)] * 2
        + [pltpu.VMEM(base_x.shape, jnp.int32)] * 3,
        compiler_params=pltpu.CompilerParams(
            vmem_limit_bytes=SEND_LIMIT, collective_id=0, has_side_effects=True
        ),
        name="send",
    )(offsets, forces, base_x, base_y, base_z, tile_count)

    def sparse(*args):
        places_line = places.reshape(-1)
        u_new, partial, table = pl.pallas_call(
            functools.partial(main_kernel, plan, time_step),
            out_shape=[
                jax.ShapeDtypeStruct(u_old.shape, f32),
                jax.ShapeDtypeStruct((8, plan.listed), f32),
                jax.ShapeDtypeStruct((2 * plan.grid_rows, width), f32),
            ],
            in_specs=[whole] * 3 + [scalars] * 2 + [far] * 2,
            out_specs=[far, whole, whole],
            scratch_shapes=[
                pltpu.VMEM((4 * plan.grid_rows, width), f32),
                pltpu.VMEM((plan.listed, width), f32),
                pltpu.VMEM((9 * GROUP, width), f32),
                pltpu.VMEM(u_old.shape, f32),
                pltpu.VMEM(density.shape, f32),
                dma((3,)),
            ],
            compiler_params=pltpu.CompilerParams(vmem_limit_bytes=MAIN_LIMIT),
            name="main",
        )(own, plain, spots, places_line, tile_count, u_old, density)
        out = pl.pallas_call(
            functools.partial(return_kernel, plan),
            out_shape=jax.ShapeDtypeStruct((3, slots, width), f32),
            in_specs=[whole] * 6 + [scalars] * 2,
            out_specs=whole,
            scratch_shapes=[
                pltpu.VMEM((lines, width), f32),
                pltpu.VMEM((plan.listed, plan.markers), bf16),
                pltpu.VMEM((plan.markers, width), f32),
                pltpu.VMEM((9 * GROUP, width), f32),
                pltpu.VMEM((8, plan.markers), f32),
                pltpu.VMEM((8, plan.faces), f32),
                pltpu.VMEM((4, 8, width), f32),
                dma((8,)),
                dma((8,)),
            ],
            compiler_params=pltpu.CompilerParams(
                vmem_limit_bytes=SEND_LIMIT, collective_id=1, has_side_effects=True
            ),
            name="give_back",
        )(partial, plain, spots, table, base_x, base_y, places_line, tile_count)
        return u_new, out

    args = (u_old, density, offsets, forces, base_x, base_y, base_z, tile_count)
    return lax.cond(over[0] > 0, dense_device, sparse, *args)


def solution(mesh):
    in_specs = (
        P(None, "gx", "gy", None),
        P("gx", "gy", None),
        P(None, ("gx", "gy"), None),
        P(None, ("gx", "gy"), None),
        P(("gx", "gy"), None),
        P(("gx", "gy"), None),
        P(("gx", "gy"), None),
        P(("gx", "gy")),
    )
    out_specs = (P(None, "gx", "gy", None), P(None, ("gx", "gy"), None))
    return jax.shard_map(
        on_device, mesh=mesh, in_specs=in_specs, out_specs=out_specs, check_vma=False
    )
```
